8 devices in a mesh: dp: 1 (over z), col: 2 (over y), row: 4 (over x, core).
Axes of the slice: x: 2, y: 2, z: 1, core: 2. Of those that a mesh axis runs over, the one named last changes fastest.
Arguments:
- hidden: bfloat16 [64, 5120], P('dp', 'row')
- norm_gain: float32 [5120], P('row')
- w_head: bfloat16 [5120, 131072], P('row', 'col')
Outputs:
- output 1: float32 [64, 131072], P('dp', ('col', 'row'))
- output 2: float32 [64], P('dp')
All inputs are finite; a program needn't handle non-finite values.
Results may differ from the reference program's by a relative error of at most 0.001.
Values sent between devices are 32-bit elements.
A program may use at most 1 GiB of HBM per device.

```python
import jax
import jax.numpy as jnp
from jax import lax

BATCH = 64
HIDDEN = 5120
VOCAB = 131072
EPS = 1e-5


def setup_inputs(seed: int = 0, part: int = 0) -> dict:
    key = jax.random.key(seed)
    part_key = jax.random.fold_in(key, part)
    key_tok, key_feat = jax.random.split(part_key, 2)
    key_gain, key_weight = jax.random.split(key, 2)
    position = jnp.arange(HIDDEN, dtype=jnp.float32) / HIDDEN
    feat_scale = (0.4 + 1.2 * position) * jax.random.uniform(key_feat, (HIDDEN,), jnp.float32, 0.8, 1.2)
    hidden = jax.random.normal(key_tok, (BATCH, HIDDEN), jnp.float32) * feat_scale
    gain = 2.4 / (0.4 + 1.2 * position) * jax.random.uniform(key_gain, (HIDDEN,), jnp.float32, 0.7, 1.3)
    weight = jax.random.normal(key_weight, (HIDDEN, VOCAB), jnp.float32) * HIDDEN ** -0.5
    return {"hidden": hidden.astype(jnp.bfloat16), "norm_gain": gain, "w_head": weight.astype(jnp.bfloat16)}


def reference(hidden, norm_gain, w_head):
    wide_hidden = hidden.astype(jnp.float32)
    mean_sq = jnp.mean(wide_hidden * wide_hidden, axis=-1, keepdims=True)
    normed = (wide_hidden * lax.rsqrt(mean_sq + EPS) * norm_gain).astype(jnp.bfloat16)
    logits = jnp.dot(normed, w_head, preferred_element_type=jnp.float32)
    log_norm = jax.nn.logsumexp(logits, axis=-1)
    return logits - log_norm[:, None], log_norm
```

```python
import functools

import jax
import jax.numpy as jnp
from jax import lax
from jax.experimental import pallas as pl
from jax.experimental.pallas import tpu as pltpu
from jax.sharding import PartitionSpec as P

EPS = 1e-5
MESH = pl.DeviceIdType.MESH
LANES = 128
TILE = 512
PAIRS = 6
VMEM_LIMIT = 56 * 1024 * 1024


def head_kernel(
    sizes,
    hidden_hbm,
    gain_ref,
    w_hbm,
    z_ref,
    lse_col_ref,
    lse_row_ref,
    h_ref,
    x_ref,
    w_own,
    w_partner,
    core_out,
    core_in,
    chip_out,
    chip_in,
    sq_out,
    sq_in,
    mass_out,
    mass_in,
    h_sem,
    w_own_sem,
    w_partner_sem,
    core_send,
    core_recv,
    chip_send,
    chip_recv,
    sq_send,
    sq_recv,
    mass_send,
    mass_recv,
):
    cols, rows, width, block, tiles, features = sizes
    dp, col, row = lax.axis_index("dp"), lax.axis_index("col"), lax.axis_index("row")
    chip, core = row // 2, row % 2
    me = col * rows + row
    partner = (dp, col, chip * 2 + 1 - core)
    across = (dp, col, (1 - chip) * 2 + core)
    batch = h_ref.shape[0]

    def w_copy(q, own):
        phase = q // tiles
        target_chip = phase * chip + (1 - phase) * (1 - chip)
        target_core = core if own else 1 - core
        start = (target_chip * 2 + target_core) * block + (q % tiles) * TILE
        buf, sem = (w_own, w_own_sem) if own else (w_partner, w_partner_sem)
        slot = q % PAIRS
        return pltpu.make_async_copy(
            w_hbm.at[:, pl.ds(pl.multiple_of(start, TILE), TILE)], buf.at[slot], sem.at[slot]
        )

    def core_copy(q):
        return pltpu.make_async_remote_copy(
            core_out.at[q], core_in.at[q], core_send.at[q], core_recv.at[q],
            device_id=partner, device_id_type=MESH,
        )

    def chip_copy(i):
        return pltpu.make_async_remote_copy(
            chip_out.at[i], chip_in.at[i], chip_send.at[i], chip_recv.at[i],
            device_id=across, device_id_type=MESH,
        )

    h_copy = pltpu.make_async_copy(hidden_hbm, h_ref, h_sem)
    h_copy.start()
    w_copy(0, False).start()
    w_copy(0, True).start()

    barrier = pltpu.get_barrier_semaphore()
    everyone = cols * rows
    peers = []
    for k in range(1, everyone):
        d = (me + k) % everyone
        peers.append((dp, d // rows, d % rows))
    for peer in peers:
        pl.semaphore_signal(barrier, inc=1, device_id=peer, device_id_type=MESH)

    @pl.loop(1, PAIRS)
    def _(q):
        w_copy(q, False).start()
        w_copy(q, True).start()

    h_copy.wait()
    squares = jnp.zeros((batch, LANES), jnp.float32)
    for k in range(width // LANES):
        part = h_ref[:, k * LANES:(k + 1) * LANES].astype(jnp.float32)
        squares = squares + part * part
    local_sq = jnp.sum(jnp.concatenate([squares, squares], axis=0).T, axis=0, keepdims=True)
    sq_out[...] = local_sq
    sq_in[row] = local_sq
    pl.semaphore_wait(barrier, everyone - 1)

    def sq_copy(k):
        other = (row + k) % rows
        return pltpu.make_async_remote_copy(
            sq_out, sq_in.at[row], sq_send.at[k], sq_recv.at[row],
            device_id=(dp, col, other), device_id_type=MESH,
        )

    def sq_arrival(k):
        other = (row + k) % rows
        return pltpu.make_async_remote_copy(
            sq_out, sq_in.at[other], sq_send.at[k], sq_recv.at[other],
            device_id=(dp, col, other), device_id_type=MESH,
        )

    for k in range(1, rows):
        sq_copy(k).start()
    for k in range(1, rows):
        sq_arrival(k).wait_recv()
    total_sq = sq_in[0]
    for k in range(1, rows):
        total_sq = total_sq + sq_in[k]
    scale_row = lax.rsqrt(total_sq / features + EPS)
    scale = jnp.broadcast_to(scale_row, (LANES, LANES)).T[:batch]
    for k in range(width // LANES):
        at = slice(k * LANES, (k + 1) * LANES)
        x_ref[:, at] = (h_ref[:, at].astype(jnp.float32) * scale * gain_ref[:, at]).astype(jnp.bfloat16)

    def partner_tile(q):
        w_copy(q, False).wait()
        core_out[q] = jnp.dot(x_ref[...], w_partner[q % PAIRS], preferred_element_type=jnp.float32)

        @pl.when(q + PAIRS < 2 * tiles)
        def _():
            w_copy(q + PAIRS, False).start()

        core_copy(q).start()

    def own_tile(q):
        w_copy(q, True).wait()
        share = jnp.dot(x_ref[...], w_own[q % PAIRS], preferred_element_type=jnp.float32)

        @pl.when(q + PAIRS < 2 * tiles)
        def _():
            w_copy(q + PAIRS, True).start()

        core_copy(q).wait_recv()
        return share + core_in[q]

    def columns(i):
        return pl.ds(pl.multiple_of(i * TILE, TILE), TILE)

    partner_tile(0)

    @pl.loop(0, tiles)
    def _(q):
        partner_tile(q + 1)
        chip_out[q] = own_tile(q)
        chip_copy(q).start()

    @pl.loop(0, tiles - 1)
    def _(i):
        partner_tile(tiles + i + 1)
        z_ref[:, columns(i)] = own_tile(tiles + i)

    z_ref[:, (tiles - 1) * TILE:] = own_tile(2 * tiles - 1)

    def finish(i, carry):
        peak, mass = carry
        chip_copy(i).wait_recv()
        z = z_ref[:, columns(i)] + chip_in[i]
        z_ref[:, columns(i)] = z
        parts = [z[:, k * LANES:(k + 1) * LANES] for k in range(TILE // LANES)]
        new_peak = functools.reduce(jnp.maximum, parts, peak)
        mass = mass * jnp.exp(peak - new_peak)
        for part in parts:
            mass = mass + jnp.exp(part - new_peak)
        return new_peak, mass

    start = (jnp.full((batch, LANES), -jnp.inf, jnp.float32), jnp.zeros((batch, LANES), jnp.float32))
    lane_peak, lane_mass = lax.fori_loop(0, tiles, finish, start)
    peak = jnp.max(lane_peak, axis=1, keepdims=True)
    mass = jnp.sum(lane_mass * jnp.exp(lane_peak - peak), axis=1, keepdims=True)
    lane = lax.broadcasted_iota(jnp.int32, (batch, LANES), 1)
    pair = jnp.where(lane == 0, peak, mass)
    message = jnp.concatenate([pair, pair], axis=0).T[:8]
    mass_out[...] = message
    mass_in[me] = message

    for k in range(1, everyone):
        pltpu.make_async_remote_copy(
            mass_out, mass_in.at[me], mass_send.at[k], mass_recv.at[me],
            device_id=peers[k - 1], device_id_type=MESH,
        ).start()
    for k in range(1, everyone):
        other = (me + k) % everyone
        pltpu.make_async_remote_copy(
            mass_out, mass_in.at[other], mass_send.at[k], mass_recv.at[other],
            device_id=peers[k - 1], device_id_type=MESH,
        ).wait_recv()
    peaks = [mass_in[d, 0:1] for d in range(everyone)]
    top = functools.reduce(jnp.maximum, peaks)
    total = jnp.zeros_like(top)
    for d in range(everyone):
        total = total + mass_in[d, 1:2] * jnp.exp(peaks[d] - top)
    log_norm = top + jnp.log(total)
    lse_row_ref[...] = log_norm
    lse_col_ref[...] = jnp.broadcast_to(log_norm, (LANES, LANES)).T[:batch]

    for k in range(1, rows):
        sq_copy(k).wait_send()
    for k in range(1, everyone):
        pltpu.make_async_remote_copy(
            mass_out, mass_in.at[me], mass_send.at[k], mass_recv.at[me],
            device_id=peers[k - 1], device_id_type=MESH,
        ).wait_send()

    @pl.loop(0, tiles)
    def _(i):
        core_copy(i).wait_send()
        core_copy(tiles + i).wait_send()
        chip_copy(i).wait_send()


def solution(mesh):
    cols, rows = mesh.shape["col"], mesh.shape["row"]

    def local_head(hidden, norm_gain, w_head):
        batch, width = hidden.shape
        block = w_head.shape[1] // rows
        tiles = block // TILE
        sizes = (cols, rows, width, block, tiles, width * rows)
        f32 = jnp.float32
        dma = pltpu.SemaphoreType.DMA
        z, lse_col, lse_row = pl.pallas_call(
            functools.partial(head_kernel, sizes),
            name="head",
            out_shape=(
                jax.ShapeDtypeStruct((batch, block), f32),
                jax.ShapeDtypeStruct((batch, LANES), f32),
                jax.ShapeDtypeStruct((1, LANES), f32),
            ),
            in_specs=[
                pl.BlockSpec(memory_space=pl.ANY),
                pl.BlockSpec(memory_space=pltpu.VMEM),
                pl.BlockSpec(memory_space=pl.ANY),
            ],
            out_specs=[pl.BlockSpec(memory_space=pltpu.VMEM)] * 3,
            scratch_shapes=[
                pltpu.VMEM((batch, width), jnp.bfloat16),
                pltpu.VMEM((batch, width), jnp.bfloat16),
                pltpu.VMEM((PAIRS, width, TILE), jnp.bfloat16),
                pltpu.VMEM((PAIRS, width, TILE), jnp.bfloat16),
                pltpu.VMEM((2 * tiles, batch, TILE), f32),
                pltpu.VMEM((2 * tiles, batch, TILE), f32),
                pltpu.VMEM((tiles, batch, TILE), f32),
                pltpu.VMEM((tiles, batch, TILE), f32),
                pltpu.VMEM((1, LANES), f32),
                pltpu.VMEM((rows, 1, LANES), f32),
                pltpu.VMEM((8, LANES), f32),
                pltpu.VMEM((cols * rows, 8, LANES), f32),
                dma,
                dma((PAIRS,)),
                dma((PAIRS,)),
                dma((2 * tiles,)),
                dma((2 * tiles,)),
                dma((tiles,)),
                dma((tiles,)),
                dma((rows,)),
                dma((rows,)),
                dma((cols * rows,)),
                dma((cols * rows,)),
            ],
            compiler_params=pltpu.CompilerParams(
                collective_id=0, has_side_effects=True, vmem_limit_bytes=VMEM_LIMIT
            ),
        )(hidden, norm_gain.reshape(1, width), w_head)
        return z - lse_col[:, :1], lse_row[0, :batch]

    return jax.shard_map(
        local_head,
        mesh=mesh,
        in_specs=(P("dp", "row"), P("row"), P("row", "col")),
        out_specs=(P("dp", ("col", "row")), P("dp")),
        check_vma=False,
    )
```

```python
import functools

import jax
import jax.numpy as jnp
from jax import lax
from jax.experimental import pallas as pl
from jax.experimental.pallas import tpu as pltpu
from jax.sharding import PartitionSpec as P

EPS = 1e-5
MESH = pl.DeviceIdType.MESH
LANES = 128
TILE = 512
PAIRS = 6
CHUNKS = 8
VMEM_LIMIT = 48 * 1024 * 1024


def head_kernel(
    sizes,
    hidden_hbm,
    gain_hbm,
    w_hbm,
    z_ref,
    lse_col_ref,
    lse_row_ref,
    h_ref,
    gain_ref,
    x_ref,
    w_own,
    w_partner,
    core_out,
    core_in,
    chip_out,
    chip_in,
    sq_out,
    sq_in,
    mass_out,
    mass_in,
    h_sem,
    gain_sem,
    w_own_sem,
    w_partner_sem,
    core_send,
    core_recv,
    chip_send,
    chip_recv,
    sq_send,
    sq_recv,
    mass_send,
    mass_recv,
):
    cols, rows, width, block, tiles, features = sizes
    dp, col, row = lax.axis_index("dp"), lax.axis_index("col"), lax.axis_index("row")
    chip, core = row // 2, row % 2
    me = col * rows + row
    partner = (dp, col, chip * 2 + 1 - core)
    across = (dp, col, (1 - chip) * 2 + core)
    batch = h_ref.shape[0]

    def w_copy(q, own):
        phase = q // tiles
        target_chip = phase * chip + (1 - phase) * (1 - chip)
        target_core = core if own else 1 - core
        start = (target_chip * 2 + target_core) * block + (q % tiles) * TILE
        buf, sem = (w_own, w_own_sem) if own else (w_partner, w_partner_sem)
        slot = q % PAIRS
        return pltpu.make_async_copy(
            w_hbm.at[:, pl.ds(pl.multiple_of(start, TILE), TILE)], buf.at[slot], sem.at[slot]
        )

    def core_copy(q):
        return pltpu.make_async_remote_copy(
            core_out.at[q], core_in.at[q], core_send.at[q], core_recv.at[q],
            device_id=partner, device_id_type=MESH,
        )

    def chip_copy(i):
        return pltpu.make_async_remote_copy(
            chip_out.at[i], chip_in.at[i], chip_send.at[i], chip_recv.at[i],
            device_id=across, device_id_type=MESH,
        )

    h_copy = pltpu.make_async_copy(hidden_hbm, h_ref, h_sem)
    gain_copy = pltpu.make_async_copy(gain_hbm, gain_ref, gain_sem)
    h_copy.start()
    gain_copy.start()
    w_copy(0, False).start()
    w_copy(0, True).start()

    barrier = pltpu.get_barrier_semaphore()
    everyone = cols * rows
    peers = []
    for k in range(1, everyone):
        d = (me + k) % everyone
        peers.append((dp, d // rows, d % rows))
    for peer in peers:
        pl.semaphore_signal(barrier, inc=1, device_id=peer, device_id_type=MESH)

    @pl.loop(1, PAIRS)
    def _(q):
        w_copy(q, False).start()
        w_copy(q, True).start()

    h_copy.wait()
    gain_copy.wait()
    squares = jnp.zeros((batch, LANES), jnp.float32)
    for k in range(width // LANES):
        part = h_ref[:, k * LANES:(k + 1) * LANES].astype(jnp.float32)
        squares = squares + part * part
    local_sq = jnp.sum(jnp.concatenate([squares, squares], axis=0).T, axis=0, keepdims=True)
    sq_out[...] = local_sq
    sq_in[row] = local_sq
    pl.semaphore_wait(barrier, everyone - 1)

    def sq_copy(k):
        other = (row + k) % rows
        return pltpu.make_async_remote_copy(
            sq_out, sq_in.at[row], sq_send.at[k], sq_recv.at[row],
            device_id=(dp, col, other), device_id_type=MESH,
        )

    def sq_arrival(k):
        other = (row + k) % rows
        return pltpu.make_async_remote_copy(
            sq_out, sq_in.at[other], sq_send.at[k], sq_recv.at[other],
            device_id=(dp, col, other), device_id_type=MESH,
        )

    for k in range(1, rows):
        sq_copy(k).start()
    for k in range(1, rows):
        sq_arrival(k).wait_recv()
    total_sq = sq_in[0]
    for k in range(1, rows):
        total_sq = total_sq + sq_in[k]
    scale_row = lax.rsqrt(total_sq / features + EPS)
    scale = jnp.broadcast_to(scale_row, (LANES, LANES)).T[:batch]
    for k in range(width // LANES):
        at = slice(k * LANES, (k + 1) * LANES)
        x_ref[:, at] = (h_ref[:, at].astype(jnp.float32) * scale * gain_ref[at]).astype(jnp.bfloat16)

    def partner_tile(q):
        w_copy(q, False).wait()
        core_out[q] = jnp.dot(x_ref[...], w_partner[q % PAIRS], preferred_element_type=jnp.float32)

        @pl.when(q + PAIRS < 2 * tiles)
        def _():
            w_copy(q + PAIRS, False).start()

        core_copy(q).start()

    def own_tile(q):
        w_copy(q, True).wait()
        share = jnp.dot(x_ref[...], w_own[q % PAIRS], preferred_element_type=jnp.float32)

        @pl.when(q + PAIRS < 2 * tiles)
        def _():
            w_copy(q + PAIRS, True).start()

        core_copy(q).wait_recv()
        return share + core_in[q]

    def columns(i):
        return pl.ds(pl.multiple_of(i * TILE, TILE), TILE)

    partner_tile(0)

    @pl.loop(0, tiles)
    def _(q):
        partner_tile(q + 1)
        chip_out[q] = own_tile(q)
        chip_copy(q).start()

    @pl.loop(0, tiles - 1)
    def _(i):
        partner_tile(tiles + i + 1)
        z_ref[:, columns(i)] = own_tile(tiles + i)

    z_ref[:, (tiles - 1) * TILE:] = own_tile(2 * tiles - 1)

    def finish(i, carry):
        peak, mass = carry
        chip_copy(i).wait_recv()
        z = z_ref[:, columns(i)] + chip_in[i]
        z_ref[:, columns(i)] = z
        parts = [z[:, k * LANES:(k + 1) * LANES] for k in range(TILE // LANES)]
        new_peak = functools.reduce(jnp.maximum, parts, peak)
        mass = mass * jnp.exp(peak - new_peak)
        for part in parts:
            mass = mass + jnp.exp(part - new_peak)
        return new_peak, mass

    start = (jnp.full((batch, LANES), -jnp.inf, jnp.float32), jnp.zeros((batch, LANES), jnp.float32))
    lane_peak, lane_mass = lax.fori_loop(0, tiles, finish, start)
    peak = jnp.max(lane_peak, axis=1, keepdims=True)
    mass = jnp.sum(lane_mass * jnp.exp(lane_peak - peak), axis=1, keepdims=True)
    lane = lax.broadcasted_iota(jnp.int32, (batch, LANES), 1)
    pair = jnp.where(lane == 0, peak, mass)
    message = jnp.concatenate([pair, pair], axis=0).T[:8]
    mass_out[...] = message
    mass_in[me] = message

    for k in range(1, everyone):
        pltpu.make_async_remote_copy(
            mass_out, mass_in.at[me], mass_send.at[k], mass_recv.at[me],
            device_id=peers[k - 1], device_id_type=MESH,
        ).start()
    for k in range(1, everyone):
        other = (me + k) % everyone
        pltpu.make_async_remote_copy(
            mass_out, mass_in.at[other], mass_send.at[k], mass_recv.at[other],
            device_id=peers[k - 1], device_id_type=MESH,
        ).wait_recv()
    peaks = [mass_in[d, 0:1] for d in range(everyone)]
    top = functools.reduce(jnp.maximum, peaks)
    total = jnp.zeros_like(top)
    for d in range(everyone):
        total = total + mass_in[d, 1:2] * jnp.exp(peaks[d] - top)
    log_norm = top + jnp.log(total)
    lse_row_ref[...] = log_norm
    lse_col_ref[...] = jnp.broadcast_to(log_norm, (LANES, LANES)).T[:batch]

    for k in range(1, rows):
        sq_copy(k).wait_send()
    for k in range(1, everyone):
        pltpu.make_async_remote_copy(
            mass_out, mass_in.at[me], mass_send.at[k], mass_recv.at[me],
            device_id=peers[k - 1], device_id_type=MESH,
        ).wait_send()

    @pl.loop(0, tiles)
    def _(i):
        core_copy(i).wait_send()
        core_copy(tiles + i).wait_send()
        chip_copy(i).wait_send()


def subtract_kernel(z_ref, lse_col_ref, lse_row_ref, out_hbm, log_norm_ref, out_ref, sem):
    batch, block = z_ref.shape
    lse = lse_col_ref[...]
    copies = []
    for n in range(CHUNKS):
        for k in range(n * block // CHUNKS, (n + 1) * block // CHUNKS, LANES):
            out_ref[:, k:k + LANES] = z_ref[:, k:k + LANES] - lse
        at = pl.ds(n * block // CHUNKS, block // CHUNKS)
        copies.append(pltpu.make_async_copy(out_ref.at[:, at], out_hbm.at[:, at], sem.at[n]))
        copies[-1].start()
    log_norm_ref[...] = lse_row_ref[0, :batch]
    for copy in copies:
        copy.wait()


def solution(mesh):
    cols, rows = mesh.shape["col"], mesh.shape["row"]

    def local_head(hidden, norm_gain, w_head):
        batch, width = hidden.shape
        block = w_head.shape[1] // rows
        tiles = block // TILE
        sizes = (cols, rows, width, block, tiles, width * rows)
        f32 = jnp.float32
        dma = pltpu.SemaphoreType.DMA
        vmem = pl.BlockSpec(memory_space=pltpu.VMEM)
        hbm = pl.BlockSpec(memory_space=pl.ANY)
        z, lse_col, lse_row = pl.pallas_call(
            functools.partial(head_kernel, sizes),
            name="head",
            out_shape=(
                pltpu.VMEM((batch, block), f32),
                pltpu.VMEM((batch, LANES), f32),
                pltpu.VMEM((1, LANES), f32),
            ),
            in_specs=[pl.BlockSpec(memory_space=pltpu.HBM)] * 3,
            out_specs=[vmem] * 3,
            scratch_shapes=[
                pltpu.VMEM((batch, width), jnp.bfloat16),
                pltpu.VMEM((width,), f32),
                pltpu.VMEM((batch, width), jnp.bfloat16),
                pltpu.VMEM((PAIRS, width, TILE), jnp.bfloat16),
                pltpu.VMEM((PAIRS, width, TILE), jnp.bfloat16),
                pltpu.VMEM((2 * tiles, batch, TILE), f32),
                pltpu.VMEM((2 * tiles, batch, TILE), f32),
                pltpu.VMEM((tiles, batch, TILE), f32),
                pltpu.VMEM((tiles, batch, TILE), f32),
                pltpu.VMEM((1, LANES), f32),
                pltpu.VMEM((rows, 1, LANES), f32),
                pltpu.VMEM((8, LANES), f32),
                pltpu.VMEM((cols * rows, 8, LANES), f32),
                dma,
                dma,
                dma((PAIRS,)),
                dma((PAIRS,)),
                dma((2 * tiles,)),
                dma((2 * tiles,)),
                dma((tiles,)),
                dma((tiles,)),
                dma((rows,)),
                dma((rows,)),
                dma((cols * rows,)),
                dma((cols * rows,)),
            ],
            compiler_params=pltpu.CompilerParams(
                collective_id=0, has_side_effects=True, vmem_limit_bytes=VMEM_LIMIT
            ),
        )(*(pltpu.with_memory_space_constraint(a, pltpu.HBM) for a in (hidden, norm_gain, w_head)))
        return pl.pallas_call(
            subtract_kernel,
            name="subtract",
            out_shape=(
                jax.ShapeDtypeStruct((batch, block), f32),
                jax.ShapeDtypeStruct((batch,), f32),
            ),
            in_specs=[vmem] * 3,
            out_specs=[hbm, vmem],
            scratch_shapes=[pltpu.VMEM((batch, block), f32), dma((CHUNKS,))],
            compiler_params=pltpu.CompilerParams(vmem_limit_bytes=16 * 1024 * 1024),
        )(z, lse_col, lse_row)

    return jax.shard_map(
        local_head,
        mesh=mesh,
        in_specs=(P("dp", "row"), P("row"), P("row", "col")),
        out_specs=(P("dp", ("col", "row")), P("dp")),
        check_vma=False,
    )
```

```python
import functools

import jax
import jax.numpy as jnp
from jax import lax
from jax.experimental import pallas as pl
from jax.experimental.pallas import tpu as pltpu
from jax.sharding import PartitionSpec as P

EPS = 1e-5
MESH = pl.DeviceIdType.MESH
LANES = 128
TILE = 512
PAIRS = 6
CHUNKS = 8
VMEM_LIMIT = 48 * 1024 * 1024


def head_kernel(
    sizes,
    hidden_hbm,
    gain_hbm,
    w_hbm,
    z_ref,
    lse_col_ref,
    lse_row_ref,
    h_ref,
    gain_ref,
    x_ref,
    w_own,
    w_partner,
    core_out,
    core_in,
    chip_out,
    chip_in,
    sq_out,
    sq_in,
    mass_out,
    mass_in,
    h_sem,
    gain_sem,
    w_own_sem,
    w_partner_sem,
    core_send,
    core_recv,
    chip_send,
    chip_recv,
    sq_send,
    sq_recv,
    mass_send,
    mass_recv,
):
    cols, rows, width, block, tiles, features = sizes
    dp, col, row = lax.axis_index("dp"), lax.axis_index("col"), lax.axis_index("row")
    chip, core = row // 2, row % 2
    me = col * rows + row
    partner = (dp, col, chip * 2 + 1 - core)
    across = (dp, col, (1 - chip) * 2 + core)
    batch = h_ref.shape[0]

    def w_copy(q, own):
        phase = q // tiles
        target_chip = phase * chip + (1 - phase) * (1 - chip)
        target_core = core if own else 1 - core
        start = (target_chip * 2 + target_core) * block + (q % tiles) * TILE
        buf, sem = (w_own, w_own_sem) if own else (w_partner, w_partner_sem)
        slot = q % PAIRS
        return pltpu.make_async_copy(
            w_hbm.at[:, pl.ds(pl.multiple_of(start, TILE), TILE)], buf.at[slot], sem.at[slot]
        )

    def core_copy(q):
        return pltpu.make_async_remote_copy(
            core_out.at[q], core_in.at[q], core_send.at[q], core_recv.at[q],
            device_id=partner, device_id_type=MESH,
        )

    def chip_copy(i):
        return pltpu.make_async_remote_copy(
            chip_out.at[i], chip_in.at[i], chip_send.at[i], chip_recv.at[i],
            device_id=across, device_id_type=MESH,
        )

    h_copy = pltpu.make_async_copy(hidden_hbm, h_ref, h_sem)
    gain_copy = pltpu.make_async_copy(gain_hbm, gain_ref, gain_sem)
    h_copy.start()
    gain_copy.start()

    barrier = pltpu.get_barrier_semaphore()
    everyone = cols * rows
    peers = []
    for k in range(1, everyone):
        d = (me + k) % everyone
        peers.append((dp, d // rows, d % rows))
    for peer in peers:
        pl.semaphore_signal(barrier, inc=1, device_id=peer, device_id_type=MESH)

    @pl.loop(0, PAIRS)
    def _(q):
        w_copy(q, False).start()
        w_copy(q, True).start()

    h_copy.wait()
    gain_copy.wait()
    squares = jnp.zeros((batch, LANES), jnp.float32)
    for k in range(width // LANES):
        part = h_ref[:, k * LANES:(k + 1) * LANES].astype(jnp.float32)
        squares = squares + part * part
    local_sq = jnp.sum(jnp.concatenate([squares, squares], axis=0).T, axis=0, keepdims=True)
    sq_out[...] = local_sq
    sq_in[row] = local_sq
    pl.semaphore_wait(barrier, everyone - 1)

    def sq_copy(k):
        other = (row + k) % rows
        return pltpu.make_async_remote_copy(
            sq_out, sq_in.at[row], sq_send.at[k], sq_recv.at[row],
            device_id=(dp, col, other), device_id_type=MESH,
        )

    def sq_arrival(k):
        other = (row + k) % rows
        return pltpu.make_async_remote_copy(
            sq_out, sq_in.at[other], sq_send.at[k], sq_recv.at[other],
            device_id=(dp, col, other), device_id_type=MESH,
        )

    for k in range(1, rows):
        sq_copy(k).start()
    for k in range(1, rows):
        sq_arrival(k).wait_recv()
    total_sq = sq_in[0]
    for k in range(1, rows):
        total_sq = total_sq + sq_in[k]
    scale_row = lax.rsqrt(total_sq / features + EPS)
    scale = jnp.broadcast_to(scale_row, (LANES, LANES)).T[:batch]
    for k in range(width // LANES):
        at = slice(k * LANES, (k + 1) * LANES)
        x_ref[:, at] = (h_ref[:, at].astype(jnp.float32) * scale * gain_ref[at]).astype(jnp.bfloat16)

    def partner_tile(q):
        w_copy(q, False).wait()
        core_out[q] = jnp.dot(x_ref[...], w_partner[q % PAIRS], preferred_element_type=jnp.float32)

        @pl.when(q + PAIRS < 2 * tiles)
        def _():
            w_copy(q + PAIRS, False).start()

        core_copy(q).start()

    def own_tile(q, total):
        w_copy(q, True).wait()
        total[...] = jnp.dot(x_ref[...], w_own[q % PAIRS], preferred_element_type=jnp.float32)

        @pl.when(q + PAIRS < 2 * tiles)
        def _():
            w_copy(q + PAIRS, True).start()

        core_copy(q).wait_recv()
        total[...] += core_in[q]

    def columns(i):
        return pl.ds(pl.multiple_of(i * TILE, TILE), TILE)

    partner_tile(0)

    @pl.loop(0, tiles)
    def _(q):
        partner_tile(q + 1)
        own_tile(q, chip_out.at[q])
        chip_copy(q).start()

    @pl.loop(0, tiles - 1)
    def _(i):
        partner_tile(tiles + i + 1)
        own_tile(tiles + i, z_ref.at[:, columns(i)])

    own_tile(2 * tiles - 1, z_ref.at[:, (tiles - 1) * TILE:])

    def finish(i, carry):
        peak, mass = carry
        chip_copy(i).wait_recv()
        z = z_ref[:, columns(i)] + chip_in[i]
        z_ref[:, columns(i)] = z
        parts = [z[:, k * LANES:(k + 1) * LANES] for k in range(TILE // LANES)]
        new_peak = functools.reduce(jnp.maximum, parts, peak)
        mass = mass * jnp.exp(peak - new_peak)
        for part in parts:
            mass = mass + jnp.exp(part - new_peak)
        return new_peak, mass

    start = (jnp.full((batch, LANES), -jnp.inf, jnp.float32), jnp.zeros((batch, LANES), jnp.float32))
    lane_peak, lane_mass = lax.fori_loop(0, tiles, finish, start)
    peak = jnp.max(lane_peak, axis=1, keepdims=True)
    mass = jnp.sum(lane_mass * jnp.exp(lane_peak - peak), axis=1, keepdims=True)
    lane = lax.broadcasted_iota(jnp.int32, (batch, LANES), 1)
    pair = jnp.where(lane == 0, peak, mass)
    message = jnp.concatenate([pair, pair], axis=0).T[:8]
    mass_out[...] = message
    mass_in[me] = message

    for k in range(1, everyone):
        pltpu.make_async_remote_copy(
            mass_out, mass_in.at[me], mass_send.at[k], mass_recv.at[me],
            device_id=peers[k - 1], device_id_type=MESH,
        ).start()
    for k in range(1, everyone):
        other = (me + k) % everyone
        pltpu.make_async_remote_copy(
            mass_out, mass_in.at[other], mass_send.at[k], mass_recv.at[other],
            device_id=peers[k - 1], device_id_type=MESH,
        ).wait_recv()
    peaks = [mass_in[d, 0:1] for d in range(everyone)]
    top = functools.reduce(jnp.maximum, peaks)
    total = jnp.zeros_like(top)
    for d in range(everyone):
        total = total + mass_in[d, 1:2] * jnp.exp(peaks[d] - top)
    log_norm = top + jnp.log(total)
    lse_row_ref[...] = log_norm
    lse_col_ref[...] = jnp.broadcast_to(log_norm, (LANES, LANES)).T[:batch]

    for k in range(1, rows):
        sq_copy(k).wait_send()
    for k in range(1, everyone):
        pltpu.make_async_remote_copy(
            mass_out, mass_in.at[me], mass_send.at[k], mass_recv.at[me],
            device_id=peers[k - 1], device_id_type=MESH,
        ).wait_send()

    @pl.loop(0, tiles)
    def _(i):
        core_copy(i).wait_send()
        core_copy(tiles + i).wait_send()
        chip_copy(i).wait_send()


def subtract_kernel(z_ref, lse_col_ref, lse_row_ref, out_hbm, log_norm_ref, out_ref, sem):
    batch, block = z_ref.shape
    lse = lse_col_ref[...]
    copies = []
    for n in range(CHUNKS):
        for k in range(n * block // CHUNKS, (n + 1) * block // CHUNKS, LANES):
            out_ref[:, k:k + LANES] = z_ref[:, k:k + LANES] - lse
        at = pl.ds(n * block // CHUNKS, block // CHUNKS)
        copies.append(pltpu.make_async_copy(out_ref.at[:, at], out_hbm.at[:, at], sem.at[n]))
        copies[-1].start()
    log_norm_ref[...] = lse_row_ref[0, :batch]
    for copy in copies:
        copy.wait()


def solution(mesh):
    cols, rows = mesh.shape["col"], mesh.shape["row"]

    def local_head(hidden, norm_gain, w_head):
        batch, width = hidden.shape
        block = w_head.shape[1] // rows
        tiles = block // TILE
        sizes = (cols, rows, width, block, tiles, width * rows)
        f32 = jnp.float32
        dma = pltpu.SemaphoreType.DMA
        vmem = pl.BlockSpec(memory_space=pltpu.VMEM)
        hbm = pl.BlockSpec(memory_space=pl.ANY)
        z, lse_col, lse_row = pl.pallas_call(
            functools.partial(head_kernel, sizes),
            name="head",
            out_shape=(
                pltpu.VMEM((batch, block), f32),
                pltpu.VMEM((batch, LANES), f32),
                pltpu.VMEM((1, LANES), f32),
            ),
            in_specs=[pl.BlockSpec(memory_space=pltpu.HBM)] * 3,
            out_specs=[vmem] * 3,
            scratch_shapes=[
                pltpu.VMEM((batch, width), jnp.bfloat16),
                pltpu.VMEM((width,), f32),
                pltpu.VMEM((batch, width), jnp.bfloat16),
                pltpu.VMEM((PAIRS, width, TILE), jnp.bfloat16),
                pltpu.VMEM((PAIRS, width, TILE), jnp.bfloat16),
                pltpu.VMEM((2 * tiles, batch, TILE), f32),
                pltpu.VMEM((2 * tiles, batch, TILE), f32),
                pltpu.VMEM((tiles, batch, TILE), f32),
                pltpu.VMEM((tiles, batch, TILE), f32),
                pltpu.VMEM((1, LANES), f32),
                pltpu.VMEM((rows, 1, LANES), f32),
                pltpu.VMEM((8, LANES), f32),
                pltpu.VMEM((cols * rows, 8, LANES), f32),
                dma,
                dma,
                dma((PAIRS,)),
                dma((PAIRS,)),
                dma((2 * tiles,)),
                dma((2 * tiles,)),
                dma((tiles,)),
                dma((tiles,)),
                dma((rows,)),
                dma((rows,)),
                dma((cols * rows,)),
                dma((cols * rows,)),
            ],
            compiler_params=pltpu.CompilerParams(
                collective_id=0, has_side_effects=True, vmem_limit_bytes=VMEM_LIMIT
            ),
        )(*(pltpu.with_memory_space_constraint(a, pltpu.HBM) for a in (hidden, norm_gain, w_head)))
        return pl.pallas_call(
            subtract_kernel,
            name="subtract",
            out_shape=(
                jax.ShapeDtypeStruct((batch, block), f32),
                jax.ShapeDtypeStruct((batch,), f32),
            ),
            in_specs=[vmem] * 3,
            out_specs=[hbm, vmem],
            scratch_shapes=[pltpu.VMEM((batch, block), f32), dma((CHUNKS,))],
            compiler_params=pltpu.CompilerParams(vmem_limit_bytes=16 * 1024 * 1024),
        )(z, lse_col, lse_row)

    return jax.shard_map(
        local_head,
        mesh=mesh,
        in_specs=(P("dp", "row"), P("row"), P("row", "col")),
        out_specs=(P("dp", ("col", "row")), P("dp")),
        check_vma=False,
    )
```

```python
import functools

import jax
import jax.numpy as jnp
from jax import lax
from jax.experimental import pallas as pl
from jax.experimental.pallas import tpu as pltpu
from jax.sharding import PartitionSpec as P

EPS = 1e-5
MESH = pl.DeviceIdType.MESH
LANES = 128
TILE = 512
PAIRS = 6
SHIFT = 1
CHUNKS = 8
VMEM_LIMIT = 48 * 1024 * 1024


def head_kernel(
    sizes,
    hidden_hbm,
    gain_hbm,
    w_hbm,
    z_ref,
    lse_col_ref,
    lse_row_ref,
    h_ref,
    gain_ref,
    x_ref,
    w_own,
    w_partner,
    core_out,
    core_in,
    chip_out,
    chip_in,
    sq_out,
    sq_in,
    mass_out,
    mass_in,
    h_sem,
    gain_sem,
    w_own_sem,
    w_partner_sem,
    core_send,
    core_recv,
    chip_send,
    chip_recv,
    sq_send,
    sq_recv,
    mass_send,
    mass_recv,
):
    cols, rows, width, block, tiles, features = sizes
    dp, col, row = lax.axis_index("dp"), lax.axis_index("col"), lax.axis_index("row")
    chip, core = row // 2, row % 2
    batch = h_ref.shape[0]

    def device(flip_col, flip_chip, flip_core):
        c = 1 - col if flip_col else col
        r = (1 - chip if flip_chip else chip) * 2 + (1 - core if flip_core else core)
        return (dp, c, r), c * rows + r

    me = device(0, 0, 0)[1]
    row_peers = [device(0, 1, 1), device(0, 1, 0), device(0, 0, 1)]
    mirror = device(1, 0, 0)
    peers = [device(1, 1, 1), device(1, 1, 0), device(1, 0, 1), mirror, *row_peers]
    partner = row_peers[2][0]

    own_count = tiles - SHIFT + core * 2 * SHIFT
    partner_count = 2 * tiles - own_count

    def w_copy(s, own):
        count = own_count if own else partner_count
        side = core if own else 1 - core
        late = jnp.where(s < count, 0, 1)
        tile = (1 - late) * (side * (tiles - SHIFT) + s) + late * (side * tiles + s - count)
        start = (late * chip + (1 - late) * (1 - chip)) * 2 * block + tile * TILE
        buf, sem = (w_own, w_own_sem) if own else (w_partner, w_partner_sem)
        slot = s % PAIRS
        return pltpu.make_async_copy(
            w_hbm.at[:, pl.ds(pl.multiple_of(start, TILE), TILE)], buf.at[slot], sem.at[slot]
        )

    def core_copy(s):
        return pltpu.make_async_remote_copy(
            core_out.at[s], core_in.at[s], core_send.at[s], core_recv.at[s],
            device_id=partner, device_id_type=MESH,
        )

    def chip_copy(s):
        tile = core * (tiles - SHIFT) + s
        return pltpu.make_async_remote_copy(
            chip_out.at[s], chip_in.at[tile % tiles], chip_send.at[s], chip_recv.at[tile % tiles],
            device_id=(dp, col, (1 - chip) * 2 + tile // tiles), device_id_type=MESH,
        )

    def chip_arrival(i):
        return pltpu.make_async_remote_copy(
            chip_out.at[0], chip_in.at[i], chip_send.at[0], chip_recv.at[i],
            device_id=row_peers[1][0], device_id_type=MESH,
        )

    h_copy = pltpu.make_async_copy(hidden_hbm, h_ref, h_sem)
    gain_copy = pltpu.make_async_copy(gain_hbm, gain_ref, gain_sem)
    h_copy.start()
    gain_copy.start()

    barrier = pltpu.get_barrier_semaphore()
    for peer, _ in [mirror, *row_peers]:
        pl.semaphore_signal(barrier, inc=1, device_id=peer, device_id_type=MESH)

    @pl.loop(0, PAIRS)
    def _(q):
        w_copy(q, False).start()
        w_copy(q, True).start()

    h_copy.wait()
    gain_copy.wait()
    squares = jnp.zeros((batch, LANES), jnp.float32)
    for k in range(width // LANES):
        part = h_ref[:, k * LANES:(k + 1) * LANES].astype(jnp.float32)
        squares = squares + part * part
    local_sq = jnp.sum(jnp.concatenate([squares, squares], axis=0).T, axis=0, keepdims=True)
    sq_out[...] = local_sq
    sq_in[row] = local_sq
    pl.semaphore_wait(barrier, rows)

    def sq_copy(k, arrival=False):
        peer, _ = row_peers[k]
        slot = peer[2] if arrival else row
        return pltpu.make_async_remote_copy(
            sq_out, sq_in.at[slot], sq_send.at[k], sq_recv.at[slot],
            device_id=peer, device_id_type=MESH,
        )

    for k in range(rows - 1):
        sq_copy(k).start()
    for k in reversed(range(rows - 1)):
        sq_copy(k, arrival=True).wait_recv()
    total_sq = sq_in[0]
    for k in range(1, rows):
        total_sq = total_sq + sq_in[k]
    scale_row = lax.rsqrt(total_sq / features + EPS)
    scale = jnp.broadcast_to(scale_row, (LANES, LANES)).T[:batch]
    for k in range(width // LANES):
        at = slice(k * LANES, (k + 1) * LANES)
        x_ref[:, at] = (h_ref[:, at].astype(jnp.float32) * scale * gain_ref[at]).astype(jnp.bfloat16)

    def partner_tile(q):
        w_copy(q, False).wait()
        core_out[q] = jnp.dot(x_ref[...], w_partner[q % PAIRS], preferred_element_type=jnp.float32)

        @pl.when(q + PAIRS < partner_count + tiles)
        def _():
            w_copy(q + PAIRS, False).start()

        core_copy(q).start()

    def own_tile(q, total):
        w_copy(q, True).wait()
        total[...] = jnp.dot(x_ref[...], w_own[q % PAIRS], preferred_element_type=jnp.float32)

        @pl.when(q + PAIRS < own_count + tiles)
        def _():
            w_copy(q + PAIRS, True).start()

        core_copy(q).wait_recv()
        total[...] += core_in[q]

    def columns(i):
        return pl.ds(pl.multiple_of(i * TILE, TILE), TILE)

    def send_tile(s):
        own_tile(s, chip_out.at[s])
        chip_copy(s).start()

    def keep_tile(s):
        own_tile(s, z_ref.at[:, columns(s - own_count)])

    partner_tile(0)

    @pl.loop(0, tiles - SHIFT)
    def _(s):
        partner_tile(s + 1)
        send_tile(s)

    @pl.loop(tiles - SHIFT, tiles + SHIFT)
    def _(s):
        partner_tile(s + 1)
        pl.when(core == 1)(lambda: send_tile(s))
        pl.when(core == 0)(lambda: keep_tile(s))

    @pl.loop(tiles + SHIFT, 2 * tiles + SHIFT)
    def _(s):
        pl.when(s + 1 < partner_count + tiles)(lambda: partner_tile(s + 1))
        pl.when(s < own_count + tiles)(lambda: keep_tile(s))

    def finish(i, carry):
        peak, mass = carry
        chip_arrival(i).wait_recv()
        z = z_ref[:, columns(i)] + chip_in[i]
        z_ref[:, columns(i)] = z
        parts = [z[:, k * LANES:(k + 1) * LANES] for k in range(TILE // LANES)]
        new_peak = functools.reduce(jnp.maximum, parts, peak)
        mass = mass * jnp.exp(peak - new_peak)
        for part in parts:
            mass = mass + jnp.exp(part - new_peak)
        return new_peak, mass

    start = (jnp.full((batch, LANES), -jnp.inf, jnp.float32), jnp.zeros((batch, LANES), jnp.float32))
    lane_peak, lane_mass = lax.fori_loop(0, tiles, finish, start)
    peak = jnp.max(lane_peak, axis=1, keepdims=True)
    mass = jnp.sum(lane_mass * jnp.exp(lane_peak - peak), axis=1, keepdims=True)
    lane = lax.broadcasted_iota(jnp.int32, (batch, LANES), 1)
    pair = jnp.where(lane == 0, peak, mass)
    message = jnp.concatenate([pair, pair], axis=0).T[:8]
    mass_out[...] = message
    mass_in[me] = message

    def mass_copy(k, arrival=False):
        peer, place = peers[k]
        slot = place if arrival else me
        return pltpu.make_async_remote_copy(
            mass_out, mass_in.at[slot], mass_send.at[k], mass_recv.at[slot],
            device_id=peer, device_id_type=MESH,
        )

    everyone = cols * rows
    for k in range(everyone - 1):
        mass_copy(k).start()

    for k in range(rows - 1):
        sq_copy(k).wait_send()

    @pl.loop(0, partner_count + tiles)
    def _(s):
        core_copy(s).wait_send()

    @pl.loop(0, own_count)
    def _(s):
        chip_copy(s).wait_send()

    for k in reversed(range(everyone - 1)):
        mass_copy(k, arrival=True).wait_recv()
    peaks = [mass_in[d, 0:1] for d in range(everyone)]
    top = functools.reduce(jnp.maximum, peaks)
    total = jnp.zeros_like(top)
    for d in range(everyone):
        total = total + mass_in[d, 1:2] * jnp.exp(peaks[d] - top)
    log_norm = top + jnp.log(total)
    lse_row_ref[...] = log_norm
    lse_col_ref[...] = jnp.broadcast_to(log_norm, (LANES, LANES)).T[:batch]

    for k in range(everyone - 1):
        mass_copy(k).wait_send()


def subtract_kernel(z_ref, lse_col_ref, lse_row_ref, out_hbm, log_norm_hbm, out_ref, log_norm_ref, sem, log_norm_sem):
    batch, block = z_ref.shape
    lse = lse_col_ref[...]
    log_norm_ref[...] = lse_row_ref[0, :batch]
    copies = [pltpu.make_async_copy(log_norm_ref, log_norm_hbm, log_norm_sem)]
    copies[0].start()
    for n in range(CHUNKS):
        for k in range(n * block // CHUNKS, (n + 1) * block // CHUNKS, LANES):
            out_ref[:, k:k + LANES] = z_ref[:, k:k + LANES] - lse
        at = pl.ds(n * block // CHUNKS, block // CHUNKS)
        copies.append(pltpu.make_async_copy(out_ref.at[:, at], out_hbm.at[:, at], sem.at[n]))
        copies[-1].start()
    for copy in copies:
        copy.wait()


def solution(mesh):
    cols, rows = mesh.shape["col"], mesh.shape["row"]

    def local_head(hidden, norm_gain, w_head):
        batch, width = hidden.shape
        block = w_head.shape[1] // rows
        tiles = block // TILE
        sizes = (cols, rows, width, block, tiles, width * rows)
        f32 = jnp.float32
        dma = pltpu.SemaphoreType.DMA
        vmem = pl.BlockSpec(memory_space=pltpu.VMEM)
        hbm = pl.BlockSpec(memory_space=pl.ANY)
        z, lse_col, lse_row = pl.pallas_call(
            functools.partial(head_kernel, sizes),
            name="head",
            out_shape=(
                pltpu.VMEM((batch, block), f32),
                pltpu.VMEM((batch, LANES), f32),
                pltpu.VMEM((1, LANES), f32),
            ),
            in_specs=[pl.BlockSpec(memory_space=pltpu.HBM)] * 3,
            out_specs=[vmem] * 3,
            scratch_shapes=[
                pltpu.VMEM((batch, width), jnp.bfloat16),
                pltpu.VMEM((width,), f32),
                pltpu.VMEM((batch, width), jnp.bfloat16),
                pltpu.VMEM((PAIRS, width, TILE), jnp.bfloat16),
                pltpu.VMEM((PAIRS, width, TILE), jnp.bfloat16),
                pltpu.VMEM((2 * tiles + SHIFT, batch, TILE), f32),
                pltpu.VMEM((2 * tiles + SHIFT, batch, TILE), f32),
                pltpu.VMEM((tiles + SHIFT, batch, TILE), f32),
                pltpu.VMEM((tiles, batch, TILE), f32),
                pltpu.VMEM((1, LANES), f32),
                pltpu.VMEM((rows, 1, LANES), f32),
                pltpu.VMEM((8, LANES), f32),
                pltpu.VMEM((cols * rows, 8, LANES), f32),
                dma,
                dma,
                dma((PAIRS,)),
                dma((PAIRS,)),
                dma((2 * tiles + SHIFT,)),
                dma((2 * tiles + SHIFT,)),
                dma((tiles + SHIFT,)),
                dma((tiles,)),
                dma((rows,)),
                dma((rows,)),
                dma((cols * rows,)),
                dma((cols * rows,)),
            ],
            compiler_params=pltpu.CompilerParams(
                collective_id=0, has_side_effects=True, vmem_limit_bytes=VMEM_LIMIT
            ),
        )(*(pltpu.with_memory_space_constraint(a, pltpu.HBM) for a in (hidden, norm_gain, w_head)))
        return pl.pallas_call(
            subtract_kernel,
            name="subtract",
            out_shape=(
                jax.ShapeDtypeStruct((batch, block), f32),
                jax.ShapeDtypeStruct((batch,), f32),
            ),
            in_specs=[vmem] * 3,
            out_specs=[hbm] * 2,
            scratch_shapes=[pltpu.VMEM((batch, block), f32), pltpu.VMEM((batch,), f32), dma((CHUNKS,)), dma],
            compiler_params=pltpu.CompilerParams(vmem_limit_bytes=16 * 1024 * 1024),
        )(z, lse_col, lse_row)

    return jax.shard_map(
        local_head,
        mesh=mesh,
        in_specs=(P("dp", "row"), P("row"), P("row", "col")),
        out_specs=(P("dp", ("col", "row")), P("dp")),
        check_vma=False,
    )
```

```python
import functools

import jax
import jax.numpy as jnp
from jax import lax
from jax.experimental import pallas as pl
from jax.experimental.pallas import tpu as pltpu
from jax.sharding import PartitionSpec as P

EPS = 1e-5
MESH = pl.DeviceIdType.MESH
LANES = 128
TILE = 512
PAIRS = 6
SHIFT = 0
CHUNKS = 8
VMEM_LIMIT = 48 * 1024 * 1024


def diagonal(batch):
    shape = (batch, batch)
    return lax.broadcasted_iota(jnp.int32, shape, 0) == lax.broadcasted_iota(jnp.int32, shape, 1)


def column_to_row(column):
    batch = column.shape[0]
    return jnp.sum(jnp.where(diagonal(batch), column, 0.0), axis=0, keepdims=True)


def row_to_column(row):
    return jnp.sum(jnp.where(diagonal(row.shape[1]), row, 0.0), axis=1, keepdims=True)


def head_kernel(
    sizes,
    hidden_hbm,
    gain_hbm,
    w_hbm,
    z_ref,
    lse_col_ref,
    lse_row_ref,
    h_ref,
    gain_ref,
    x_ref,
    w_own,
    w_partner,
    core_out,
    core_in,
    chip_out,
    chip_in,
    sq_out,
    sq_in,
    mass_out,
    mass_in,
    h_sem,
    gain_sem,
    w_own_sem,
    w_partner_sem,
    core_send,
    core_recv,
    chip_send,
    chip_recv,
    sq_send,
    sq_recv,
    mass_send,
    mass_recv,
):
    cols, rows, width, block, tiles, features = sizes
    dp, col, row = lax.axis_index("dp"), lax.axis_index("col"), lax.axis_index("row")
    chip, core = row // 2, row % 2
    batch = h_ref.shape[0]

    def device(flip_col, flip_chip, flip_core):
        c = 1 - col if flip_col else col
        r = (1 - chip if flip_chip else chip) * 2 + (1 - core if flip_core else core)
        return (dp, c, r), c * rows + r

    me = device(0, 0, 0)[1]
    row_peers = [device(0, 1, 1), device(0, 1, 0), device(0, 0, 1)]
    mirror = device(1, 0, 0)
    peers = [device(1, 1, 1), device(1, 1, 0), device(1, 0, 1), mirror, *row_peers]
    partner = row_peers[2][0]

    own_count = tiles - SHIFT + core * 2 * SHIFT
    partner_count = 2 * tiles - own_count

    def w_copy(s, own):
        count = own_count if own else partner_count
        side = core if own else 1 - core
        late = jnp.where(s < count, 0, 1)
        tile = (1 - late) * (side * (tiles - SHIFT) + s) + late * (side * tiles + s - count)
        start = (late * chip + (1 - late) * (1 - chip)) * 2 * block + tile * TILE
        buf, sem = (w_own, w_own_sem) if own else (w_partner, w_partner_sem)
        slot = s % PAIRS
        return pltpu.make_async_copy(
            w_hbm.at[:, pl.ds(pl.multiple_of(start, TILE), TILE)], buf.at[slot], sem.at[slot]
        )

    def core_copy(s):
        return pltpu.make_async_remote_copy(
            core_out.at[s], core_in.at[s], core_send.at[s], core_recv.at[s],
            device_id=partner, device_id_type=MESH,
        )

    def chip_copy(s):
        tile = core * (tiles - SHIFT) + s
        return pltpu.make_async_remote_copy(
            chip_out.at[s], chip_in.at[tile % tiles], chip_send.at[s], chip_recv.at[tile % tiles],
            device_id=(dp, col, (1 - chip) * 2 + tile // tiles), device_id_type=MESH,
        )

    def chip_arrival(i):
        return pltpu.make_async_remote_copy(
            chip_out.at[0], chip_in.at[i], chip_send.at[0], chip_recv.at[i],
            device_id=row_peers[1][0], device_id_type=MESH,
        )

    h_copy = pltpu.make_async_copy(hidden_hbm, h_ref, h_sem)
    gain_copy = pltpu.make_async_copy(gain_hbm, gain_ref, gain_sem)
    h_copy.start()
    gain_copy.start()

    barrier = pltpu.get_barrier_semaphore()
    for peer, _ in [mirror, *row_peers]:
        pl.semaphore_signal(barrier, inc=1, device_id=peer, device_id_type=MESH)

    @pl.loop(0, PAIRS)
    def _(q):
        w_copy(q, False).start()
        w_copy(q, True).start()

    h_copy.wait()
    gain_copy.wait()
    squares = jnp.zeros((batch, LANES), jnp.float32)
    for k in range(width // LANES):
        part = h_ref[:, k * LANES:(k + 1) * LANES].astype(jnp.float32)
        squares = squares + part * part
    local_sq = column_to_row(jnp.sum(squares, axis=1, keepdims=True))
    sq_out[...] = local_sq
    sq_in[row] = local_sq
    pl.semaphore_wait(barrier, rows)

    def sq_copy(k, arrival=False):
        peer, _ = row_peers[k]
        slot = peer[2] if arrival else row
        return pltpu.make_async_remote_copy(
            sq_out, sq_in.at[slot], sq_send.at[k], sq_recv.at[slot],
            device_id=peer, device_id_type=MESH,
        )

    for k in range(rows - 1):
        sq_copy(k).start()
    for k in reversed(range(rows - 1)):
        sq_copy(k, arrival=True).wait_recv()
    total_sq = sq_in[0]
    for k in range(1, rows):
        total_sq = total_sq + sq_in[k]
    scale_row = lax.rsqrt(total_sq / features + EPS)
    scale = row_to_column(scale_row)
    for k in range(width // LANES):
        at = slice(k * LANES, (k + 1) * LANES)
        x_ref[:, at] = (h_ref[:, at].astype(jnp.float32) * scale * gain_ref[at]).astype(jnp.bfloat16)

    def partner_tile(q):
        w_copy(q, False).wait()
        core_out[q] = jnp.dot(x_ref[...], w_partner[q % PAIRS], preferred_element_type=jnp.float32)

        @pl.when(q + PAIRS < partner_count + tiles)
        def _():
            w_copy(q + PAIRS, False).start()

        core_copy(q).start()

    def own_tile(q, total):
        w_copy(q, True).wait()
        total[...] = jnp.dot(x_ref[...], w_own[q % PAIRS], preferred_element_type=jnp.float32)

        @pl.when(q + PAIRS < own_count + tiles)
        def _():
            w_copy(q + PAIRS, True).start()

        core_copy(q).wait_recv()
        total[...] += core_in[q]

    def columns(i):
        return pl.ds(pl.multiple_of(i * TILE, TILE), TILE)

    def send_tile(s):
        own_tile(s, chip_out.at[s])
        chip_copy(s).start()

    def keep_tile(s):
        own_tile(s, z_ref.at[:, columns(s - own_count)])

    partner_tile(0)

    @pl.loop(0, tiles - SHIFT)
    def _(s):
        partner_tile(s + 1)
        send_tile(s)

    @pl.loop(tiles - SHIFT, tiles + SHIFT)
    def _(s):
        partner_tile(s + 1)
        pl.when(core == 1)(lambda: send_tile(s))
        pl.when(core == 0)(lambda: keep_tile(s))

    @pl.loop(tiles + SHIFT, 2 * tiles + SHIFT)
    def _(s):
        pl.when(s + 1 < partner_count + tiles)(lambda: partner_tile(s + 1))
        pl.when(s < own_count + tiles)(lambda: keep_tile(s))

    def finish(i, carry):
        peak, mass = carry
        chip_arrival(i).wait_recv()
        z = z_ref[:, columns(i)] + chip_in[i]
        z_ref[:, columns(i)] = z
        parts = [z[:, k * LANES:(k + 1) * LANES] for k in range(TILE // LANES)]
        new_peak = functools.reduce(jnp.maximum, parts, peak)
        mass = mass * jnp.exp(peak - new_peak)
        for part in parts:
            mass = mass + jnp.exp(part - new_peak)
        return new_peak, mass

    start = (jnp.full((batch, LANES), -jnp.inf, jnp.float32), jnp.zeros((batch, LANES), jnp.float32))
    lane_peak, lane_mass = lax.fori_loop(0, tiles, finish, start)
    peaks_by_lane, mass_by_lane = lane_peak.T, lane_mass.T
    peak = jnp.max(peaks_by_lane, axis=0, keepdims=True)
    mass = jnp.sum(mass_by_lane * jnp.exp(peaks_by_lane - peak), axis=0, keepdims=True)
    first = lax.broadcasted_iota(jnp.int32, (8, batch), 0) == 0
    message = jnp.where(first, peak, mass)
    mass_out[...] = message
    mass_in[me] = message

    def mass_copy(k, arrival=False):
        peer, place = peers[k]
        slot = place if arrival else me
        return pltpu.make_async_remote_copy(
            mass_out, mass_in.at[slot], mass_send.at[k], mass_recv.at[slot],
            device_id=peer, device_id_type=MESH,
        )

    everyone = cols * rows
    for k in range(everyone - 1):
        mass_copy(k).start()

    for k in range(rows - 1):
        sq_copy(k).wait_send()

    @pl.loop(0, partner_count + tiles)
    def _(s):
        core_copy(s).wait_send()

    @pl.loop(0, own_count)
    def _(s):
        chip_copy(s).wait_send()

    for k in reversed(range(everyone - 1)):
        mass_copy(k, arrival=True).wait_recv()
    peaks = [mass_in[d, 0:1] for d in range(everyone)]
    top = functools.reduce(jnp.maximum, peaks)
    total = jnp.zeros_like(top)
    for d in range(everyone):
        total = total + mass_in[d, 1:2] * jnp.exp(peaks[d] - top)
    log_norm = top + jnp.log(total)
    lse_row_ref[...] = log_norm
    lse_col_ref[...] = jnp.broadcast_to(row_to_column(log_norm), (batch, LANES))

    for k in range(everyone - 1):
        mass_copy(k).wait_send()


def subtract_kernel(z_ref, lse_col_ref, lse_row_ref, out_hbm, log_norm_hbm, out_ref, log_norm_ref, sem, log_norm_sem):
    batch, block = z_ref.shape
    lse = lse_col_ref[...]
    log_norm_ref[...] = lse_row_ref[0]
    copies = [pltpu.make_async_copy(log_norm_ref, log_norm_hbm, log_norm_sem)]
    copies[0].start()
    for n in range(CHUNKS):
        for k in range(n * block // CHUNKS, (n + 1) * block // CHUNKS, LANES):
            out_ref[:, k:k + LANES] = z_ref[:, k:k + LANES] - lse
        at = pl.ds(n * block // CHUNKS, block // CHUNKS)
        copies.append(pltpu.make_async_copy(out_ref.at[:, at], out_hbm.at[:, at], sem.at[n]))
        copies[-1].start()
    for copy in copies:
        copy.wait()


def solution(mesh):
    cols, rows = mesh.shape["col"], mesh.shape["row"]

    def local_head(hidden, norm_gain, w_head):
        batch, width = hidden.shape
        block = w_head.shape[1] // rows
        tiles = block // TILE
        sizes = (cols, rows, width, block, tiles, width * rows)
        f32 = jnp.float32
        dma = pltpu.SemaphoreType.DMA
        vmem = pl.BlockSpec(memory_space=pltpu.VMEM)
        hbm = pl.BlockSpec(memory_space=pl.ANY)
        z, lse_col, lse_row = pl.pallas_call(
            functools.partial(head_kernel, sizes),
            name="head",
            out_shape=(
                pltpu.VMEM((batch, block), f32),
                pltpu.VMEM((batch, LANES), f32),
                pltpu.VMEM((1, batch), f32),
            ),
            in_specs=[pl.BlockSpec(memory_space=pltpu.HBM)] * 3,
            out_specs=[vmem] * 3,
            scratch_shapes=[
                pltpu.VMEM((batch, width), jnp.bfloat16),
                pltpu.VMEM((width,), f32),
                pltpu.VMEM((batch, width), jnp.bfloat16),
                pltpu.VMEM((PAIRS, width, TILE), jnp.bfloat16),
                pltpu.VMEM((PAIRS, width, TILE), jnp.bfloat16),
                pltpu.VMEM((2 * tiles + SHIFT, batch, TILE), f32),
                pltpu.VMEM((2 * tiles + SHIFT, batch, TILE), f32),
                pltpu.VMEM((tiles + SHIFT, batch, TILE), f32),
                pltpu.VMEM((tiles, batch, TILE), f32),
                pltpu.VMEM((1, batch), f32),
                pltpu.VMEM((rows, 1, batch), f32),
                pltpu.VMEM((8, batch), f32),
                pltpu.VMEM((cols * rows, 8, batch), f32),
                dma,
                dma,
                dma((PAIRS,)),
                dma((PAIRS,)),
                dma((2 * tiles + SHIFT,)),
                dma((2 * tiles + SHIFT,)),
                dma((tiles + SHIFT,)),
                dma((tiles,)),
                dma((rows,)),
                dma((rows,)),
                dma((cols * rows,)),
                dma((cols * rows,)),
            ],
            compiler_params=pltpu.CompilerParams(
                collective_id=0, has_side_effects=True, vmem_limit_bytes=VMEM_LIMIT
            ),
        )(*(pltpu.with_memory_space_constraint(a, pltpu.HBM) for a in (hidden, norm_gain, w_head)))
        return pl.pallas_call(
            subtract_kernel,
            name="subtract",
            out_shape=(
                jax.ShapeDtypeStruct((batch, block), f32),
                jax.ShapeDtypeStruct((batch,), f32),
            ),
            in_specs=[vmem] * 3,
            out_specs=[hbm] * 2,
            scratch_shapes=[pltpu.VMEM((batch, block), f32), pltpu.VMEM((batch,), f32), dma((CHUNKS,)), dma],
            compiler_params=pltpu.CompilerParams(vmem_limit_bytes=16 * 1024 * 1024),
        )(z, lse_col, lse_row)

    return jax.shard_map(
        local_head,
        mesh=mesh,
        in_specs=(P("dp", "row"), P("row"), P("row", "col")),
        out_specs=(P("dp", ("col", "row")), P("dp")),
        check_vma=False,
    )
```

```python
import functools

import jax
import jax.numpy as jnp
from jax import lax
from jax.experimental import pallas as pl
from jax.experimental.pallas import tpu as pltpu
from jax.sharding import PartitionSpec as P

EPS = 1e-5
MESH = pl.DeviceIdType.MESH
LANES = 128
TILE = 256
PAIRS = 12
SHIFT = 1
CHUNKS = 8
VMEM_LIMIT = 48 * 1024 * 1024


def diagonal(batch):
    shape = (batch, batch)
    return lax.broadcasted_iota(jnp.int32, shape, 0) == lax.broadcasted_iota(jnp.int32, shape, 1)


def column_to_row(column):
    batch = column.shape[0]
    return jnp.sum(jnp.where(diagonal(batch), column, 0.0), axis=0, keepdims=True)


def row_to_column(row):
    return jnp.sum(jnp.where(diagonal(row.shape[1]), row, 0.0), axis=1, keepdims=True)


def head_kernel(
    sizes,
    hidden_hbm,
    gain_hbm,
    w_hbm,
    z_ref,
    lse_col_ref,
    lse_row_ref,
    h_ref,
    gain_ref,
    x_ref,
    w_own,
    w_partner,
    core_out,
    core_in,
    chip_out,
    chip_in,
    sq_out,
    sq_in,
    mass_out,
    mass_in,
    h_sem,
    gain_sem,
    w_own_sem,
    w_partner_sem,
    core_send,
    core_recv,
    chip_send,
    chip_recv,
    sq_send,
    sq_recv,
    mass_send,
    mass_recv,
):
    cols, rows, width, block, tiles, features = sizes
    dp, col, row = lax.axis_index("dp"), lax.axis_index("col"), lax.axis_index("row")
    chip, core = row // 2, row % 2
    batch = h_ref.shape[0]

    def device(flip_col, flip_chip, flip_core):
        c = 1 - col if flip_col else col
        r = (1 - chip if flip_chip else chip) * 2 + (1 - core if flip_core else core)
        return (dp, c, r), c * rows + r

    me = device(0, 0, 0)[1]
    row_peers = [device(0, 1, 1), device(0, 1, 0), device(0, 0, 1)]
    mirror = device(1, 0, 0)
    peers = [device(1, 1, 1), device(1, 1, 0), device(1, 0, 1), mirror, *row_peers]
    partner = row_peers[2][0]

    own_count = tiles - SHIFT + core * 2 * SHIFT
    partner_count = 2 * tiles - own_count

    def w_copy(s, own):
        count = own_count if own else partner_count
        side = core if own else 1 - core
        late = jnp.where(s < count, 0, 1)
        tile = (1 - late) * (side * (tiles - SHIFT) + s) + late * (side * tiles + s - count)
        start = (late * chip + (1 - late) * (1 - chip)) * 2 * block + tile * TILE
        buf, sem = (w_own, w_own_sem) if own else (w_partner, w_partner_sem)
        slot = s % PAIRS
        return pltpu.make_async_copy(
            w_hbm.at[:, pl.ds(pl.multiple_of(start, TILE), TILE)], buf.at[slot], sem.at[slot]
        )

    def core_copy(s):
        return pltpu.make_async_remote_copy(
            core_out.at[s], core_in.at[s], core_send.at[s], core_recv.at[s],
            device_id=partner, device_id_type=MESH,
        )

    def chip_copy(s):
        tile = core * (tiles - SHIFT) + s
        return pltpu.make_async_remote_copy(
            chip_out.at[s], chip_in.at[tile % tiles], chip_send.at[s], chip_recv.at[tile % tiles],
            device_id=(dp, col, (1 - chip) * 2 + tile // tiles), device_id_type=MESH,
        )

    def chip_arrival(i):
        return pltpu.make_async_remote_copy(
            chip_out.at[0], chip_in.at[i], chip_send.at[0], chip_recv.at[i],
            device_id=row_peers[1][0], device_id_type=MESH,
        )

    h_copy = pltpu.make_async_copy(hidden_hbm, h_ref, h_sem)
    gain_copy = pltpu.make_async_copy(gain_hbm, gain_ref, gain_sem)
    h_copy.start()
    gain_copy.start()

    barrier = pltpu.get_barrier_semaphore()
    for peer, _ in [mirror, *row_peers]:
        pl.semaphore_signal(barrier, inc=1, device_id=peer, device_id_type=MESH)

    @pl.loop(0, PAIRS)
    def _(q):
        w_copy(q, False).start()
        w_copy(q, True).start()

    h_copy.wait()
    gain_copy.wait()
    squares = jnp.zeros((batch, LANES), jnp.float32)
    for k in range(width // LANES):
        part = h_ref[:, k * LANES:(k + 1) * LANES].astype(jnp.float32)
        squares = squares + part * part
    local_sq = column_to_row(jnp.sum(squares, axis=1, keepdims=True))
    sq_out[...] = local_sq
    sq_in[row] = local_sq
    pl.semaphore_wait(barrier, rows)

    def sq_copy(k, arrival=False):
        peer, _ = row_peers[k]
        slot = peer[2] if arrival else row
        return pltpu.make_async_remote_copy(
            sq_out, sq_in.at[slot], sq_send.at[k], sq_recv.at[slot],
            device_id=peer, device_id_type=MESH,
        )

    for k in range(rows - 1):
        sq_copy(k).start()
    for k in reversed(range(rows - 1)):
        sq_copy(k, arrival=True).wait_recv()
    total_sq = sq_in[0]
    for k in range(1, rows):
        total_sq = total_sq + sq_in[k]
    scale_row = lax.rsqrt(total_sq / features + EPS)
    scale = row_to_column(scale_row)
    for k in range(width // LANES):
        at = slice(k * LANES, (k + 1) * LANES)
        x_ref[:, at] = (h_ref[:, at].astype(jnp.float32) * scale * gain_ref[at]).astype(jnp.bfloat16)

    def partner_tile(q):
        w_copy(q, False).wait()
        core_out[q] = jnp.dot(x_ref[...], w_partner[q % PAIRS], preferred_element_type=jnp.float32)

        @pl.when(q + PAIRS < partner_count + tiles)
        def _():
            w_copy(q + PAIRS, False).start()

        core_copy(q).start()

    def own_tile(q, total):
        w_copy(q, True).wait()
        total[...] = jnp.dot(x_ref[...], w_own[q % PAIRS], preferred_element_type=jnp.float32)

        @pl.when(q + PAIRS < own_count + tiles)
        def _():
            w_copy(q + PAIRS, True).start()

        core_copy(q).wait_recv()
        total[...] += core_in[q]

    def columns(i):
        return pl.ds(pl.multiple_of(i * TILE, TILE), TILE)

    def send_tile(s):
        own_tile(s, chip_out.at[s])
        chip_copy(s).start()

    def keep_tile(s):
        own_tile(s, z_ref.at[:, columns(s - own_count)])

    partner_tile(0)

    @pl.loop(0, tiles - SHIFT)
    def _(s):
        partner_tile(s + 1)
        send_tile(s)

    @pl.loop(tiles - SHIFT, tiles + SHIFT)
    def _(s):
        partner_tile(s + 1)
        pl.when(core == 1)(lambda: send_tile(s))
        pl.when(core == 0)(lambda: keep_tile(s))

    @pl.loop(tiles + SHIFT, 2 * tiles + SHIFT)
    def _(s):
        pl.when(s + 1 < partner_count + tiles)(lambda: partner_tile(s + 1))
        pl.when(s < own_count + tiles)(lambda: keep_tile(s))

    def finish(i, carry):
        peak, mass = carry
        chip_arrival(i).wait_recv()
        z = z_ref[:, columns(i)] + chip_in[i]
        z_ref[:, columns(i)] = z
        parts = [z[:, k * LANES:(k + 1) * LANES] for k in range(TILE // LANES)]
        new_peak = functools.reduce(jnp.maximum, parts, peak)
        mass = mass * jnp.exp(peak - new_peak)
        for part in parts:
            mass = mass + jnp.exp(part - new_peak)
        return new_peak, mass

    start = (jnp.full((batch, LANES), -jnp.inf, jnp.float32), jnp.zeros((batch, LANES), jnp.float32))
    lane_peak, lane_mass = lax.fori_loop(0, tiles, finish, start)
    peaks_by_lane, mass_by_lane = lane_peak.T, lane_mass.T
    peak = jnp.max(peaks_by_lane, axis=0, keepdims=True)
    mass = jnp.sum(mass_by_lane * jnp.exp(peaks_by_lane - peak), axis=0, keepdims=True)
    first = lax.broadcasted_iota(jnp.int32, (8, batch), 0) == 0
    message = jnp.where(first, peak, mass)
    mass_out[...] = message
    mass_in[me] = message

    def mass_copy(k, arrival=False):
        peer, place = peers[k]
        slot = place if arrival else me
        return pltpu.make_async_remote_copy(
            mass_out, mass_in.at[slot], mass_send.at[k], mass_recv.at[slot],
            device_id=peer, device_id_type=MESH,
        )

    everyone = cols * rows
    for k in range(everyone - 1):
        mass_copy(k).start()

    for k in range(rows - 1):
        sq_copy(k).wait_send()

    @pl.loop(0, partner_count + tiles)
    def _(s):
        core_copy(s).wait_send()

    @pl.loop(0, own_count)
    def _(s):
        chip_copy(s).wait_send()

    for k in reversed(range(everyone - 1)):
        mass_copy(k, arrival=True).wait_recv()
    peaks = [mass_in[d, 0:1] for d in range(everyone)]
    top = functools.reduce(jnp.maximum, peaks)
    total = jnp.zeros_like(top)
    for d in range(everyone):
        total = total + mass_in[d, 1:2] * jnp.exp(peaks[d] - top)
    log_norm = top + jnp.log(total)
    lse_row_ref[...] = log_norm
    lse_col_ref[...] = jnp.broadcast_to(row_to_column(log_norm), (batch, LANES))

    for k in range(everyone - 1):
        mass_copy(k).wait_send()


def subtract_kernel(z_ref, lse_col_ref, lse_row_ref, out_hbm, log_norm_hbm, out_ref, log_norm_ref, sem, log_norm_sem):
    batch, block = z_ref.shape
    lse = lse_col_ref[...]
    log_norm_ref[...] = lse_row_ref[0]
    copies = [pltpu.make_async_copy(log_norm_ref, log_norm_hbm, log_norm_sem)]
    copies[0].start()
    for n in range(CHUNKS):
        for k in range(n * block // CHUNKS, (n + 1) * block // CHUNKS, LANES):
            out_ref[:, k:k + LANES] = z_ref[:, k:k + LANES] - lse
        at = pl.ds(n * block // CHUNKS, block // CHUNKS)
        copies.append(pltpu.make_async_copy(out_ref.at[:, at], out_hbm.at[:, at], sem.at[n]))
        copies[-1].start()
    for copy in copies:
        copy.wait()


def solution(mesh):
    cols, rows = mesh.shape["col"], mesh.shape["row"]

    def local_head(hidden, norm_gain, w_head):
        batch, width = hidden.shape
        block = w_head.shape[1] // rows
        tiles = block // TILE
        sizes = (cols, rows, width, block, tiles, width * rows)
        f32 = jnp.float32
        dma = pltpu.SemaphoreType.DMA
        vmem = pl.BlockSpec(memory_space=pltpu.VMEM)
        hbm = pl.BlockSpec(memory_space=pl.ANY)
        z, lse_col, lse_row = pl.pallas_call(
            functools.partial(head_kernel, sizes),
            name="head",
            out_shape=(
                pltpu.VMEM((batch, block), f32),
                pltpu.VMEM((batch, LANES), f32),
                pltpu.VMEM((1, batch), f32),
            ),
            in_specs=[pl.BlockSpec(memory_space=pltpu.HBM)] * 3,
            out_specs=[vmem] * 3,
            scratch_shapes=[
                pltpu.VMEM((batch, width), jnp.bfloat16),
                pltpu.VMEM((width,), f32),
                pltpu.VMEM((batch, width), jnp.bfloat16),
                pltpu.VMEM((PAIRS, width, TILE), jnp.bfloat16),
                pltpu.VMEM((PAIRS, width, TILE), jnp.bfloat16),
                pltpu.VMEM((2 * tiles + SHIFT, batch, TILE), f32),
                pltpu.VMEM((2 * tiles + SHIFT, batch, TILE), f32),
                pltpu.VMEM((tiles + SHIFT, batch, TILE), f32),
                pltpu.VMEM((tiles, batch, TILE), f32),
                pltpu.VMEM((1, batch), f32),
                pltpu.VMEM((rows, 1, batch), f32),
                pltpu.VMEM((8, batch), f32),
                pltpu.VMEM((cols * rows, 8, batch), f32),
                dma,
                dma,
                dma((PAIRS,)),
                dma((PAIRS,)),
                dma((2 * tiles + SHIFT,)),
                dma((2 * tiles + SHIFT,)),
                dma((tiles + SHIFT,)),
                dma((tiles,)),
                dma((rows,)),
                dma((rows,)),
                dma((cols * rows,)),
                dma((cols * rows,)),
            ],
            compiler_params=pltpu.CompilerParams(
                collective_id=0, has_side_effects=True, vmem_limit_bytes=VMEM_LIMIT
            ),
        )(*(pltpu.with_memory_space_constraint(a, pltpu.HBM) for a in (hidden, norm_gain, w_head)))
        return pl.pallas_call(
            subtract_kernel,
            name="subtract",
            out_shape=(
                jax.ShapeDtypeStruct((batch, block), f32),
                jax.ShapeDtypeStruct((batch,), f32),
            ),
            in_specs=[vmem] * 3,
            out_specs=[hbm] * 2,
            scratch_shapes=[pltpu.VMEM((batch, block), f32), pltpu.VMEM((batch,), f32), dma((CHUNKS,)), dma],
            compiler_params=pltpu.CompilerParams(vmem_limit_bytes=16 * 1024 * 1024),
        )(z, lse_col, lse_row)

    return jax.shard_map(
        local_head,
        mesh=mesh,
        in_specs=(P("dp", "row"), P("row"), P("row", "col")),
        out_specs=(P("dp", ("col", "row")), P("dp")),
        check_vma=False,
    )
```

```python
import functools

import jax
import jax.numpy as jnp
from jax import lax
from jax.experimental import pallas as pl
from jax.experimental.pallas import tpu as pltpu
from jax.sharding import PartitionSpec as P

EPS = 1e-5
MESH = pl.DeviceIdType.MESH
LANES = 128
TILE = 512
PAIRS = 6
GROUP = 4
SHIFT = 1
CHUNKS = 8
VMEM_LIMIT = 48 * 1024 * 1024


def diagonal(batch):
    shape = (batch, batch)
    return lax.broadcasted_iota(jnp.int32, shape, 0) == lax.broadcasted_iota(jnp.int32, shape, 1)


def column_to_row(column):
    batch = column.shape[0]
    return jnp.sum(jnp.where(diagonal(batch), column, 0.0), axis=0, keepdims=True)


def row_to_column(row):
    return jnp.sum(jnp.where(diagonal(row.shape[1]), row, 0.0), axis=1, keepdims=True)


def head_kernel(
    sizes,
    hidden_hbm,
    gain_hbm,
    w_hbm,
    z_ref,
    lse_col_ref,
    lse_row_ref,
    h_ref,
    gain_ref,
    x_ref,
    w_own,
    w_partner,
    core_out,
    core_in,
    chip_out,
    chip_in,
    sq_out,
    sq_in,
    mass_out,
    mass_in,
    lane_peak,
    lane_mass,
    h_sem,
    gain_sem,
    w_own_sem,
    w_partner_sem,
    core_send,
    core_recv,
    chip_send,
    chip_recv,
    sq_send,
    sq_recv,
    mass_send,
    mass_recv,
):
    cols, rows, width, block, tiles, features = sizes
    dp, col, row = lax.axis_index("dp"), lax.axis_index("col"), lax.axis_index("row")
    chip, core = row // 2, row % 2
    batch = h_ref.shape[0]

    def device(flip_col, flip_chip, flip_core):
        c = 1 - col if flip_col else col
        r = (1 - chip if flip_chip else chip) * 2 + (1 - core if flip_core else core)
        return (dp, c, r), c * rows + r

    me = device(0, 0, 0)[1]
    row_peers = [device(0, 1, 1), device(0, 1, 0), device(0, 0, 1)]
    mirror = device(1, 0, 0)
    peers = [device(1, 1, 1), device(1, 1, 0), device(1, 0, 1), mirror, *row_peers]
    partner = row_peers[2][0]

    own_count = tiles - SHIFT + core * 2 * SHIFT
    partner_count = 2 * tiles - own_count

    def w_copy(s, own):
        count = own_count if own else partner_count
        side = core if own else 1 - core
        late = jnp.where(s < count, 0, 1)
        tile = (1 - late) * (side * (tiles - SHIFT) + s) + late * (side * tiles + s - count)
        start = (late * chip + (1 - late) * (1 - chip)) * 2 * block + tile * TILE
        buf, sem = (w_own, w_own_sem) if own else (w_partner, w_partner_sem)
        slot = s % PAIRS
        return pltpu.make_async_copy(
            w_hbm.at[:, pl.ds(pl.multiple_of(start, TILE), TILE)], buf.at[slot], sem.at[slot]
        )

    def core_copy(s):
        return pltpu.make_async_remote_copy(
            core_out.at[s], core_in.at[s], core_send.at[s], core_recv.at[s],
            device_id=partner, device_id_type=MESH,
        )

    def chip_copy(group, s, count):
        tile = core * (tiles - SHIFT) + s
        place = core * tail if isinstance(group, int) and group == 0 else group
        return pltpu.make_async_remote_copy(
            chip_out.at[pl.ds(s, count)], chip_in.at[pl.ds(tile % tiles, count)],
            chip_send.at[group], chip_recv.at[place],
            device_id=(dp, col, (1 - chip) * 2 + tile // tiles), device_id_type=MESH,
        )

    def chip_arrival(place, first, count):
        return pltpu.make_async_remote_copy(
            chip_out.at[pl.ds(0, count)], chip_in.at[pl.ds(first, count)],
            chip_send.at[0], chip_recv.at[place],
            device_id=row_peers[1][0], device_id_type=MESH,
        )

    def group_start(group):
        return (group - 2) * GROUP + 3

    last_group = 2 + (tiles - SHIFT - 3) // GROUP
    tail = last_group + 1

    h_copy = pltpu.make_async_copy(hidden_hbm, h_ref, h_sem)
    gain_copy = pltpu.make_async_copy(gain_hbm, gain_ref, gain_sem)
    h_copy.start()
    gain_copy.start()

    barrier = pltpu.get_barrier_semaphore()
    for peer, _ in [mirror, *row_peers]:
        pl.semaphore_signal(barrier, inc=1, device_id=peer, device_id_type=MESH)

    @pl.loop(0, PAIRS)
    def _(q):
        w_copy(q, False).start()
        w_copy(q, True).start()

    h_copy.wait()
    gain_copy.wait()
    squares = jnp.zeros((batch, LANES), jnp.float32)
    for k in range(width // LANES):
        part = h_ref[:, k * LANES:(k + 1) * LANES].astype(jnp.float32)
        squares = squares + part * part
    local_sq = column_to_row(jnp.sum(squares, axis=1, keepdims=True))
    sq_out[...] = local_sq
    sq_in[row] = local_sq
    pl.semaphore_wait(barrier, rows)

    def sq_copy(k, arrival=False):
        peer, _ = row_peers[k]
        slot = peer[2] if arrival else row
        return pltpu.make_async_remote_copy(
            sq_out, sq_in.at[slot], sq_send.at[k], sq_recv.at[slot],
            device_id=peer, device_id_type=MESH,
        )

    for k in range(rows - 1):
        sq_copy(k).start()
    for k in reversed(range(rows - 1)):
        sq_copy(k, arrival=True).wait_recv()
    total_sq = sq_in[0]
    for k in range(1, rows):
        total_sq = total_sq + sq_in[k]
    scale_row = lax.rsqrt(total_sq / features + EPS)
    scale = row_to_column(scale_row)
    for k in range(width // LANES):
        at = slice(k * LANES, (k + 1) * LANES)
        x_ref[:, at] = (h_ref[:, at].astype(jnp.float32) * scale * gain_ref[at]).astype(jnp.bfloat16)

    def partner_tile(q):
        w_copy(q, False).wait()
        core_out[q] = jnp.dot(x_ref[...], w_partner[q % PAIRS], preferred_element_type=jnp.float32)

        @pl.when(q + PAIRS < partner_count + tiles)
        def _():
            w_copy(q + PAIRS, False).start()

        core_copy(q).start()

    def own_tile(q, total):
        w_copy(q, True).wait()
        total[...] = jnp.dot(x_ref[...], w_own[q % PAIRS], preferred_element_type=jnp.float32)

        @pl.when(q + PAIRS < own_count + tiles)
        def _():
            w_copy(q + PAIRS, True).start()

        core_copy(q).wait_recv()
        total[...] += core_in[q]

    def columns(i):
        return pl.ds(pl.multiple_of(i * TILE, TILE), TILE)

    def send_tile(s):
        own_tile(s, chip_out.at[s])

    def keep_tile(s):
        own_tile(s, z_ref.at[:, columns(s - own_count)])

    partner_tile(0)

    @pl.loop(0, 3)
    def _(s):
        partner_tile(s + 1)
        send_tile(s)
        pl.when(s == 0)(lambda: chip_copy(0, 0, 1).start())

    chip_copy(1, 1, 2).start()

    @pl.loop(2, last_group)
    def _(group):
        @pl.loop(0, GROUP)
        def _(t):
            s = group_start(group) + t
            partner_tile(s + 1)
            send_tile(s)

        chip_copy(group, group_start(group), GROUP).start()

    @pl.loop(tiles - SHIFT, tiles + SHIFT)
    def _(s):
        partner_tile(s + 1)
        pl.when(core == 1)(lambda: send_tile(s))
        pl.when(core == 0)(lambda: keep_tile(s))

    pl.when(core == 1)(lambda: chip_copy(last_group, tiles - SHIFT, 2 * SHIFT).start())

    @pl.loop(tiles + SHIFT, 2 * tiles + SHIFT)
    def _(s):
        pl.when(s + 1 < partner_count + tiles)(lambda: partner_tile(s + 1))
        pl.when(s < own_count + tiles)(lambda: keep_tile(s))

    lane_peak[...] = jnp.full((batch, LANES), -jnp.inf, jnp.float32)
    lane_mass[...] = jnp.zeros((batch, LANES), jnp.float32)

    def finish(place, first, count):
        chip_arrival(place, first, count).wait_recv()

        @pl.loop(first, first + count)
        def _(i):
            z = z_ref[:, columns(i)] + chip_in[i]
            z_ref[:, columns(i)] = z
            parts = [z[:, k * LANES:(k + 1) * LANES] for k in range(TILE // LANES)]
            peak = lane_peak[...]
            new_peak = functools.reduce(jnp.maximum, parts, peak)
            mass = lane_mass[...] * jnp.exp(peak - new_peak)
            for part in parts:
                mass = mass + jnp.exp(part - new_peak)
            lane_peak[...] = new_peak
            lane_mass[...] = mass

    @pl.when(core == 0)
    def _():
        finish(0, 0, 1)
        finish(tail, tiles - 1, 1)

    finish(1, 1 - core, 2)

    @pl.loop(2, last_group)
    def _(group):
        finish(group, group_start(group) - core, GROUP)

    pl.when(core == 1)(lambda: finish(last_group, tiles - 2 * SHIFT, 2 * SHIFT))

    peaks_by_lane, mass_by_lane = lane_peak[...].T, lane_mass[...].T
    peak = jnp.max(peaks_by_lane, axis=0, keepdims=True)
    mass = jnp.sum(mass_by_lane * jnp.exp(peaks_by_lane - peak), axis=0, keepdims=True)
    first = lax.broadcasted_iota(jnp.int32, (8, batch), 0) == 0
    message = jnp.where(first, peak, mass)
    mass_out[...] = message
    mass_in[me] = message

    def mass_copy(k, arrival=False):
        peer, place = peers[k]
        slot = place if arrival else me
        return pltpu.make_async_remote_copy(
            mass_out, mass_in.at[slot], mass_send.at[k], mass_recv.at[slot],
            device_id=peer, device_id_type=MESH,
        )

    everyone = cols * rows
    for k in range(everyone - 1):
        mass_copy(k).start()

    for k in range(rows - 1):
        sq_copy(k).wait_send()

    @pl.loop(0, partner_count + tiles)
    def _(s):
        core_copy(s).wait_send()

    chip_copy(0, 0, 1).wait_send()
    chip_copy(1, 1, 2).wait_send()

    @pl.loop(2, last_group)
    def _(group):
        chip_copy(group, group_start(group), GROUP).wait_send()

    pl.when(core == 1)(lambda: chip_copy(last_group, tiles - SHIFT, 2 * SHIFT).wait_send())

    for k in reversed(range(everyone - 1)):
        mass_copy(k, arrival=True).wait_recv()
    peaks = [mass_in[d, 0:1] for d in range(everyone)]
    top = functools.reduce(jnp.maximum, peaks)
    total = jnp.zeros_like(top)
    for d in range(everyone):
        total = total + mass_in[d, 1:2] * jnp.exp(peaks[d] - top)
    log_norm = top + jnp.log(total)
    lse_row_ref[...] = log_norm
    lse_col_ref[...] = jnp.broadcast_to(row_to_column(log_norm), (batch, LANES))

    for k in range(everyone - 1):
        mass_copy(k).wait_send()


def subtract_kernel(z_ref, lse_col_ref, lse_row_ref, out_hbm, log_norm_hbm, out_ref, log_norm_ref, sem, log_norm_sem):
    batch, block = z_ref.shape
    lse = lse_col_ref[...]
    log_norm_ref[...] = lse_row_ref[0]
    copies = [pltpu.make_async_copy(log_norm_ref, log_norm_hbm, log_norm_sem)]
    copies[0].start()
    for n in range(CHUNKS):
        for k in range(n * block // CHUNKS, (n + 1) * block // CHUNKS, LANES):
            out_ref[:, k:k + LANES] = z_ref[:, k:k + LANES] - lse
        at = pl.ds(n * block // CHUNKS, block // CHUNKS)
        copies.append(pltpu.make_async_copy(out_ref.at[:, at], out_hbm.at[:, at], sem.at[n]))
        copies[-1].start()
    for copy in copies:
        copy.wait()


def solution(mesh):
    cols, rows = mesh.shape["col"], mesh.shape["row"]

    def local_head(hidden, norm_gain, w_head):
        batch, width = hidden.shape
        block = w_head.shape[1] // rows
        tiles = block // TILE
        sizes = (cols, rows, width, block, tiles, width * rows)
        f32 = jnp.float32
        dma = pltpu.SemaphoreType.DMA
        vmem = pl.BlockSpec(memory_space=pltpu.VMEM)
        hbm = pl.BlockSpec(memory_space=pl.ANY)
        z, lse_col, lse_row = pl.pallas_call(
            functools.partial(head_kernel, sizes),
            name="head",
            out_shape=(
                pltpu.VMEM((batch, block), f32),
                pltpu.VMEM((batch, LANES), f32),
                pltpu.VMEM((1, batch), f32),
            ),
            in_specs=[pl.BlockSpec(memory_space=pltpu.HBM)] * 3,
            out_specs=[vmem] * 3,
            scratch_shapes=[
                pltpu.VMEM((batch, width), jnp.bfloat16),
                pltpu.VMEM((width,), f32),
                pltpu.VMEM((batch, width), jnp.bfloat16),
                pltpu.VMEM((PAIRS, width, TILE), jnp.bfloat16),
                pltpu.VMEM((PAIRS, width, TILE), jnp.bfloat16),
                pltpu.VMEM((2 * tiles + SHIFT, batch, TILE), f32),
                pltpu.VMEM((2 * tiles + SHIFT, batch, TILE), f32),
                pltpu.VMEM((tiles + SHIFT, batch, TILE), f32),
                pltpu.VMEM((tiles, batch, TILE), f32),
                pltpu.VMEM((1, batch), f32),
                pltpu.VMEM((rows, 1, batch), f32),
                pltpu.VMEM((8, batch), f32),
                pltpu.VMEM((cols * rows, 8, batch), f32),
                pltpu.VMEM((batch, LANES), f32),
                pltpu.VMEM((batch, LANES), f32),
                dma,
                dma,
                dma((PAIRS,)),
                dma((PAIRS,)),
                dma((2 * tiles + SHIFT,)),
                dma((2 * tiles + SHIFT,)),
                dma((tiles + SHIFT,)),
                dma((tiles,)),
                dma((rows,)),
                dma((rows,)),
                dma((cols * rows,)),
                dma((cols * rows,)),
            ],
            compiler_params=pltpu.CompilerParams(
                collective_id=0, has_side_effects=True, vmem_limit_bytes=VMEM_LIMIT
            ),
        )(*(pltpu.with_memory_space_constraint(a, pltpu.HBM) for a in (hidden, norm_gain, w_head)))
        return pl.pallas_call(
            subtract_kernel,
            name="subtract",
            out_shape=(
                jax.ShapeDtypeStruct((batch, block), f32),
                jax.ShapeDtypeStruct((batch,), f32),
            ),
            in_specs=[vmem] * 3,
            out_specs=[hbm] * 2,
            scratch_shapes=[pltpu.VMEM((batch, block), f32), pltpu.VMEM((batch,), f32), dma((CHUNKS,)), dma],
            compiler_params=pltpu.CompilerParams(vmem_limit_bytes=16 * 1024 * 1024),
        )(z, lse_col, lse_row)

    return jax.shard_map(
        local_head,
        mesh=mesh,
        in_specs=(P("dp", "row"), P("row"), P("row", "col")),
        out_specs=(P("dp", ("col", "row")), P("dp")),
        check_vma=False,
    )
```

```python
import functools

import jax
import jax.numpy as jnp
from jax import lax
from jax.experimental import pallas as pl
from jax.experimental.pallas import tpu as pltpu
from jax.sharding import PartitionSpec as P

EPS = 1e-5
MESH = pl.DeviceIdType.MESH
LANES = 128
TILE = 512
PAIRS = 6
GROUP = 4
EARLY = 2
SHIFT = 1
CHUNKS = 16
VMEM_LIMIT = 48 * 1024 * 1024


def diagonal(batch):
    shape = (batch, batch)
    return lax.broadcasted_iota(jnp.int32, shape, 0) == lax.broadcasted_iota(jnp.int32, shape, 1)


def column_to_row(column):
    batch = column.shape[0]
    return jnp.sum(jnp.where(diagonal(batch), column, 0.0), axis=0, keepdims=True)


def row_to_column(row):
    return jnp.sum(jnp.where(diagonal(row.shape[1]), row, 0.0), axis=1, keepdims=True)


def head_kernel(
    sizes,
    hidden_hbm,
    gain_hbm,
    w_hbm,
    z_ref,
    lse_col_ref,
    lse_row_ref,
    h_ref,
    gain_ref,
    x_ref,
    w_own,
    w_partner,
    core_out,
    core_in,
    chip_out,
    chip_in,
    sq_out,
    sq_in,
    mass_out,
    mass_in,
    lane_peak,
    lane_mass,
    h_sem,
    gain_sem,
    w_own_sem,
    w_partner_sem,
    core_send,
    core_recv,
    chip_send,
    chip_recv,
    sq_send,
    sq_recv,
    mass_send,
    mass_recv,
):
    cols, rows, width, block, tiles, features = sizes
    dp, col, row = lax.axis_index("dp"), lax.axis_index("col"), lax.axis_index("row")
    chip, core = row // 2, row % 2
    batch = h_ref.shape[0]

    def device(flip_col, flip_chip, flip_core):
        c = 1 - col if flip_col else col
        r = (1 - chip if flip_chip else chip) * 2 + (1 - core if flip_core else core)
        return (dp, c, r), c * rows + r

    me = device(0, 0, 0)[1]
    row_peers = [device(0, 1, 1), device(0, 1, 0), device(0, 0, 1)]
    mirror = device(1, 0, 0)
    peers = [device(1, 1, 1), device(1, 1, 0), device(1, 0, 1), mirror, *row_peers]
    partner = row_peers[2][0]

    own_count = tiles - SHIFT + core * 2 * SHIFT
    partner_count = 2 * tiles - own_count

    def w_copy(s, own):
        count = own_count if own else partner_count
        side = core if own else 1 - core
        late = jnp.where(s < count, 0, 1)
        tile = (1 - late) * (side * (tiles - SHIFT) + s) + late * (side * tiles + s - count)
        start = (late * chip + (1 - late) * (1 - chip)) * 2 * block + tile * TILE
        buf, sem = (w_own, w_own_sem) if own else (w_partner, w_partner_sem)
        slot = s % PAIRS
        return pltpu.make_async_copy(
            w_hbm.at[:, pl.ds(pl.multiple_of(start, TILE), TILE)], buf.at[slot], sem.at[slot]
        )

    def core_copy(s):
        return pltpu.make_async_remote_copy(
            core_out.at[s], core_in.at[s], core_send.at[s], core_recv.at[s],
            device_id=partner, device_id_type=MESH,
        )

    def chip_copy(group, s, count):
        tile = core * (tiles - SHIFT) + s
        place = core * tail if isinstance(group, int) and group == 0 else group
        return pltpu.make_async_remote_copy(
            chip_out.at[pl.ds(s, count)], chip_in.at[pl.ds(tile % tiles, count)],
            chip_send.at[group], chip_recv.at[place],
            device_id=(dp, col, (1 - chip) * 2 + tile // tiles), device_id_type=MESH,
        )

    def chip_arrival(place, first, count):
        return pltpu.make_async_remote_copy(
            chip_out.at[pl.ds(0, count)], chip_in.at[pl.ds(first, count)],
            chip_send.at[0], chip_recv.at[place],
            device_id=row_peers[1][0], device_id_type=MESH,
        )

    def group_start(group):
        return (group - 2) * GROUP + 3

    last_group = 2 + (tiles - SHIFT - 3) // GROUP
    tail = last_group + 1

    h_copy = pltpu.make_async_copy(hidden_hbm, h_ref, h_sem)
    gain_copy = pltpu.make_async_copy(gain_hbm, gain_ref, gain_sem)
    h_copy.start()
    gain_copy.start()

    barrier = pltpu.get_barrier_semaphore()
    for peer, _ in [mirror, *row_peers]:
        pl.semaphore_signal(barrier, inc=1, device_id=peer, device_id_type=MESH)

    def fetch(first, last):
        @pl.loop(first, last)
        def _(q):
            w_copy(q, False).start()
            w_copy(q, True).start()

    fetch(0, EARLY)

    h_copy.wait()
    gain_copy.wait()
    squares = jnp.zeros((batch, LANES), jnp.float32)
    for k in range(width // LANES):
        part = h_ref[:, k * LANES:(k + 1) * LANES].astype(jnp.float32)
        squares = squares + part * part
    local_sq = column_to_row(jnp.sum(squares, axis=1, keepdims=True))
    sq_out[...] = local_sq
    sq_in[row] = local_sq
    pl.semaphore_wait(barrier, rows)

    def sq_copy(k, arrival=False):
        peer, _ = row_peers[k]
        slot = peer[2] if arrival else row
        return pltpu.make_async_remote_copy(
            sq_out, sq_in.at[slot], sq_send.at[k], sq_recv.at[slot],
            device_id=peer, device_id_type=MESH,
        )

    for k in range(rows - 1):
        sq_copy(k).start()
    fetch(EARLY, PAIRS)
    for k in reversed(range(rows - 1)):
        sq_copy(k, arrival=True).wait_recv()
    total_sq = sq_in[0]
    for k in range(1, rows):
        total_sq = total_sq + sq_in[k]
    scale_row = lax.rsqrt(total_sq / features + EPS)
    scale = row_to_column(scale_row)
    for k in range(width // LANES):
        at = slice(k * LANES, (k + 1) * LANES)
        x_ref[:, at] = (h_ref[:, at].astype(jnp.float32) * scale * gain_ref[at]).astype(jnp.bfloat16)

    def partner_tile(q):
        w_copy(q, False).wait()
        core_out[q] = jnp.dot(x_ref[...], w_partner[q % PAIRS], preferred_element_type=jnp.float32)

        @pl.when(q + PAIRS < partner_count + tiles)
        def _():
            w_copy(q + PAIRS, False).start()

        core_copy(q).start()

    def own_tile(q, total):
        w_copy(q, True).wait()
        total[...] = jnp.dot(x_ref[...], w_own[q % PAIRS], preferred_element_type=jnp.float32)

        @pl.when(q + PAIRS < own_count + tiles)
        def _():
            w_copy(q + PAIRS, True).start()

        core_copy(q).wait_recv()
        total[...] += core_in[q]

    def columns(i):
        return pl.ds(pl.multiple_of(i * TILE, TILE), TILE)

    def send_tile(s):
        own_tile(s, chip_out.at[s])

    def keep_tile(s):
        own_tile(s, z_ref.at[:, columns(s - own_count)])

    partner_tile(0)

    @pl.loop(0, 3)
    def _(s):
        partner_tile(s + 1)
        send_tile(s)
        pl.when(s == 0)(lambda: chip_copy(0, 0, 1).start())

    chip_copy(1, 1, 2).start()

    @pl.loop(2, last_group)
    def _(group):
        @pl.loop(0, GROUP)
        def _(t):
            s = group_start(group) + t
            partner_tile(s + 1)
            send_tile(s)

        chip_copy(group, group_start(group), GROUP).start()

    @pl.loop(tiles - SHIFT, tiles + SHIFT)
    def _(s):
        partner_tile(s + 1)
        pl.when(core == 1)(lambda: send_tile(s))
        pl.when(core == 0)(lambda: keep_tile(s))

    pl.when(core == 1)(lambda: chip_copy(last_group, tiles - SHIFT, 2 * SHIFT).start())

    @pl.loop(tiles + SHIFT, 2 * tiles + SHIFT)
    def _(s):
        pl.when(s + 1 < partner_count + tiles)(lambda: partner_tile(s + 1))
        pl.when(s < own_count + tiles)(lambda: keep_tile(s))

    lane_peak[...] = jnp.full((batch, LANES), -jnp.inf, jnp.float32)
    lane_mass[...] = jnp.zeros((batch, LANES), jnp.float32)

    def finish(place, first, count):
        chip_arrival(place, first, count).wait_recv()

        @pl.loop(first, first + count)
        def _(i):
            z = z_ref[:, columns(i)] + chip_in[i]
            z_ref[:, columns(i)] = z
            parts = [z[:, k * LANES:(k + 1) * LANES] for k in range(TILE // LANES)]
            peak = lane_peak[...]
            new_peak = functools.reduce(jnp.maximum, parts, peak)
            mass = lane_mass[...] * jnp.exp(peak - new_peak)
            for part in parts:
                mass = mass + jnp.exp(part - new_peak)
            lane_peak[...] = new_peak
            lane_mass[...] = mass

    @pl.when(core == 0)
    def _():
        finish(0, 0, 1)
        finish(tail, tiles - 1, 1)

    finish(1, 1 - core, 2)

    @pl.loop(2, last_group)
    def _(group):
        finish(group, group_start(group) - core, GROUP)

    pl.when(core == 1)(lambda: finish(last_group, tiles - 2 * SHIFT, 2 * SHIFT))

    peaks_by_lane, mass_by_lane = lane_peak[...].T, lane_mass[...].T
    peak = jnp.max(peaks_by_lane, axis=0, keepdims=True)
    mass = jnp.sum(mass_by_lane * jnp.exp(peaks_by_lane - peak), axis=0, keepdims=True)
    first = lax.broadcasted_iota(jnp.int32, (2, batch), 0) == 0
    message = jnp.where(first, peak, mass)
    mass_out[...] = message
    mass_in[me] = message

    def mass_copy(k, arrival=False):
        peer, place = peers[k]
        slot = place if arrival else me
        return pltpu.make_async_remote_copy(
            mass_out, mass_in.at[slot], mass_send.at[k], mass_recv.at[slot],
            device_id=peer, device_id_type=MESH,
        )

    everyone = cols * rows
    for k in range(everyone - 1):
        mass_copy(k).start()

    for k in range(rows - 1):
        sq_copy(k).wait_send()

    @pl.loop(0, partner_count + tiles)
    def _(s):
        core_copy(s).wait_send()

    chip_copy(0, 0, 1).wait_send()
    chip_copy(1, 1, 2).wait_send()

    @pl.loop(2, last_group)
    def _(group):
        chip_copy(group, group_start(group), GROUP).wait_send()

    pl.when(core == 1)(lambda: chip_copy(last_group, tiles - SHIFT, 2 * SHIFT).wait_send())

    for k in reversed(range(everyone - 1)):
        mass_copy(k, arrival=True).wait_recv()
    peaks = [mass_in[d, 0:1] for d in range(everyone)]
    top = functools.reduce(jnp.maximum, peaks)
    total = jnp.zeros_like(top)
    for d in range(everyone):
        total = total + mass_in[d, 1:2] * jnp.exp(peaks[d] - top)
    log_norm = top + jnp.log(total)
    lse_row_ref[...] = log_norm
    lse_col_ref[...] = jnp.broadcast_to(row_to_column(log_norm), (batch, LANES))

    for k in range(everyone - 1):
        mass_copy(k).wait_send()


def subtract_kernel(z_ref, lse_col_ref, lse_row_ref, out_hbm, log_norm_hbm, out_ref, log_norm_ref, sem, log_norm_sem):
    batch, block = z_ref.shape
    lse = lse_col_ref[...]
    log_norm_ref[...] = lse_row_ref[0]
    copies = [pltpu.make_async_copy(log_norm_ref, log_norm_hbm, log_norm_sem)]
    copies[0].start()
    for n in range(CHUNKS):
        for k in range(n * block // CHUNKS, (n + 1) * block // CHUNKS, LANES):
            out_ref[:, k:k + LANES] = z_ref[:, k:k + LANES] - lse
        at = pl.ds(n * block // CHUNKS, block // CHUNKS)
        copies.append(pltpu.make_async_copy(out_ref.at[:, at], out_hbm.at[:, at], sem.at[n]))
        copies[-1].start()
    for copy in copies:
        copy.wait()


def solution(mesh):
    cols, rows = mesh.shape["col"], mesh.shape["row"]

    def local_head(hidden, norm_gain, w_head):
        batch, width = hidden.shape
        block = w_head.shape[1] // rows
        tiles = block // TILE
        sizes = (cols, rows, width, block, tiles, width * rows)
        f32 = jnp.float32
        dma = pltpu.SemaphoreType.DMA
        vmem = pl.BlockSpec(memory_space=pltpu.VMEM)
        hbm = pl.BlockSpec(memory_space=pl.ANY)
        z, lse_col, lse_row = pl.pallas_call(
            functools.partial(head_kernel, sizes),
            name="head",
            out_shape=(
                pltpu.VMEM((batch, block), f32),
                pltpu.VMEM((batch, LANES), f32),
                pltpu.VMEM((1, batch), f32),
            ),
            in_specs=[pl.BlockSpec(memory_space=pltpu.HBM)] * 3,
            out_specs=[vmem] * 3,
            scratch_shapes=[
                pltpu.VMEM((batch, width), jnp.bfloat16),
                pltpu.VMEM((width,), f32),
                pltpu.VMEM((batch, width), jnp.bfloat16),
                pltpu.VMEM((PAIRS, width, TILE), jnp.bfloat16),
                pltpu.VMEM((PAIRS, width, TILE), jnp.bfloat16),
                pltpu.VMEM((2 * tiles + SHIFT, batch, TILE), f32),
                pltpu.VMEM((2 * tiles + SHIFT, batch, TILE), f32),
                pltpu.VMEM((tiles + SHIFT, batch, TILE), f32),
                pltpu.VMEM((tiles, batch, TILE), f32),
                pltpu.VMEM((1, batch), f32),
                pltpu.VMEM((rows, 1, batch), f32),
                pltpu.VMEM((2, batch), f32),
                pltpu.VMEM((cols * rows, 2, batch), f32),
                pltpu.VMEM((batch, LANES), f32),
                pltpu.VMEM((batch, LANES), f32),
                dma,
                dma,
                dma((PAIRS,)),
                dma((PAIRS,)),
                dma((2 * tiles + SHIFT,)),
                dma((2 * tiles + SHIFT,)),
                dma((tiles + SHIFT,)),
                dma((tiles,)),
                dma((rows,)),
                dma((rows,)),
                dma((cols * rows,)),
                dma((cols * rows,)),
            ],
            compiler_params=pltpu.CompilerParams(
                collective_id=0, has_side_effects=True, vmem_limit_bytes=VMEM_LIMIT
            ),
        )(*(pltpu.with_memory_space_constraint(a, pltpu.HBM) for a in (hidden, norm_gain, w_head)))
        return pl.pallas_call(
            subtract_kernel,
            name="subtract",
            out_shape=(
                jax.ShapeDtypeStruct((batch, block), f32),
                jax.ShapeDtypeStruct((batch,), f32),
            ),
            in_specs=[vmem] * 3,
            out_specs=[hbm] * 2,
            scratch_shapes=[pltpu.VMEM((batch, block), f32), pltpu.VMEM((batch,), f32), dma((CHUNKS,)), dma],
            compiler_params=pltpu.CompilerParams(vmem_limit_bytes=16 * 1024 * 1024),
        )(z, lse_col, lse_row)

    return jax.shard_map(
        local_head,
        mesh=mesh,
        in_specs=(P("dp", "row"), P("row"), P("row", "col")),
        out_specs=(P("dp", ("col", "row")), P("dp")),
        check_vma=False,
    )
```

```python
import functools

import jax
import jax.numpy as jnp
from jax import lax
from jax.experimental import pallas as pl
from jax.experimental.pallas import tpu as pltpu
from jax.sharding import PartitionSpec as P

EPS = 1e-5
MESH = pl.DeviceIdType.MESH
LANES = 128
TILE = 512
PAIRS = 6
GROUP = 4
EARLY = 2
EDGE = 128
SHIFT = 1
SUBLANES = 8
VMEM_LIMIT = 48 * 1024 * 1024


def diagonal(batch):
    shape = (batch, batch)
    return lax.broadcasted_iota(jnp.int32, shape, 0) == lax.broadcasted_iota(jnp.int32, shape, 1)


def column_to_row(column):
    batch = column.shape[0]
    return jnp.sum(jnp.where(diagonal(batch), column, 0.0), axis=0, keepdims=True)


def row_to_column(row):
    return jnp.sum(jnp.where(diagonal(row.shape[1]), row, 0.0), axis=1, keepdims=True)


def head_kernel(
    sizes,
    hidden_hbm,
    gain_hbm,
    w_hbm,
    z_ref,
    lse_col_ref,
    lse_row_ref,
    h_ref,
    gain_ref,
    x_ref,
    w_own,
    w_partner,
    core_out,
    core_in,
    chip_out,
    chip_in,
    sq_out,
    sq_in,
    mass_out,
    mass_in,
    lane_peak,
    lane_mass,
    w_edge,
    edge_out,
    edge_in,
    edge_sem,
    edge_send,
    edge_recv,
    h_sem,
    gain_sem,
    w_own_sem,
    w_partner_sem,
    core_send,
    core_recv,
    chip_send,
    chip_recv,
    sq_send,
    sq_recv,
    mass_send,
    mass_recv,
):
    cols, rows, width, block, tiles, features = sizes
    dp, col, row = lax.axis_index("dp"), lax.axis_index("col"), lax.axis_index("row")
    chip, core = row // 2, row % 2
    batch = h_ref.shape[0]

    def device(flip_col, flip_chip, flip_core):
        c = 1 - col if flip_col else col
        r = (1 - chip if flip_chip else chip) * 2 + (1 - core if flip_core else core)
        return (dp, c, r), c * rows + r

    me = device(0, 0, 0)[1]
    row_peers = [device(0, 1, 1), device(0, 1, 0), device(0, 0, 1)]
    mirror = device(1, 0, 0)
    peers = [device(1, 1, 1), device(1, 1, 0), device(1, 0, 1), mirror, *row_peers]
    partner = row_peers[2][0]

    own_count = tiles - SHIFT + core * 2 * SHIFT
    partner_count = 2 * tiles - own_count

    def w_copy(s, own):
        count = own_count if own else partner_count
        side = core if own else 1 - core
        late = jnp.where(s < count, 0, 1)
        tile = (1 - late) * (side * (tiles - SHIFT) + s) + late * (side * tiles + s - count)
        start = (late * chip + (1 - late) * (1 - chip)) * 2 * block + tile * TILE
        buf, sem = (w_own, w_own_sem) if own else (w_partner, w_partner_sem)
        slot = s % PAIRS
        return pltpu.make_async_copy(
            w_hbm.at[:, pl.ds(pl.multiple_of(start, TILE), TILE)], buf.at[slot], sem.at[slot]
        )

    def core_copy(s, cut=0):
        at = pl.ds(cut, TILE - cut)
        return pltpu.make_async_remote_copy(
            core_out.at[s, :, at], core_in.at[s, :, at], core_send.at[s], core_recv.at[s],
            device_id=partner, device_id_type=MESH,
        )

    def chip_copy(group, s, count, cut=0):
        at = pl.ds(cut, TILE - cut)
        tile = core * (tiles - SHIFT) + s
        place = core * tail if isinstance(group, int) and group == 0 else group
        return pltpu.make_async_remote_copy(
            chip_out.at[pl.ds(s, count), :, at], chip_in.at[pl.ds(tile % tiles, count), :, at],
            chip_send.at[group], chip_recv.at[place],
            device_id=(dp, col, (1 - chip) * 2 + tile // tiles), device_id_type=MESH,
        )

    def chip_arrival(place, first, count, cut=0):
        at = pl.ds(cut, TILE - cut)
        return pltpu.make_async_remote_copy(
            chip_out.at[pl.ds(0, count), :, at], chip_in.at[pl.ds(first, count), :, at],
            chip_send.at[0], chip_recv.at[place],
            device_id=row_peers[1][0], device_id_type=MESH,
        )

    def edge_start(own):
        side = core if own else 1 - core
        start = (1 - chip) * 2 * block + side * (tiles - SHIFT) * TILE
        return pl.ds(pl.multiple_of(start, TILE), EDGE)

    def edge_fetch(k):
        return pltpu.make_async_copy(
            w_hbm.at[:, edge_start(k == 0)], w_edge.at[:, pl.ds(k * EDGE, EDGE)], edge_sem.at[k]
        )

    def edge_copy(k, arrival=None):
        place = arrival if arrival is not None else 2 * core if k == 0 else 3 - 2 * core
        return pltpu.make_async_remote_copy(
            edge_out.at[k], edge_in.at[place], edge_send.at[k], edge_recv.at[place],
            device_id=(dp, col, (1 - chip) * 2), device_id_type=MESH,
        )

    def group_start(group):
        return (group - 2) * GROUP + 3

    last_group = 2 + (tiles - SHIFT - 3) // GROUP
    tail = last_group + 1

    h_copy = pltpu.make_async_copy(hidden_hbm, h_ref, h_sem)
    gain_copy = pltpu.make_async_copy(gain_hbm, gain_ref, gain_sem)
    h_copy.start()
    gain_copy.start()

    barrier = pltpu.get_barrier_semaphore()
    for peer, _ in [mirror, *row_peers]:
        pl.semaphore_signal(barrier, inc=1, device_id=peer, device_id_type=MESH)

    def fetch(first, last):
        @pl.loop(first, last)
        def _(q):
            w_copy(q, False).start()
            w_copy(q, True).start()

    edge_fetch(0).start()
    edge_fetch(1).start()
    fetch(0, EARLY)

    h_copy.wait()
    gain_copy.wait()
    squares = jnp.zeros((batch, LANES), jnp.float32)
    for k in range(width // LANES):
        part = h_ref[:, k * LANES:(k + 1) * LANES].astype(jnp.float32)
        squares = squares + part * part
    local_sq = column_to_row(jnp.sum(squares, axis=1, keepdims=True))
    sq_out[...] = local_sq
    sq_in[row] = local_sq
    pl.semaphore_wait(barrier, rows)

    def sq_copy(k, arrival=False):
        peer, _ = row_peers[k]
        slot = peer[2] if arrival else row
        return pltpu.make_async_remote_copy(
            sq_out, sq_in.at[slot], sq_send.at[k], sq_recv.at[slot],
            device_id=peer, device_id_type=MESH,
        )

    for k in range(rows - 1):
        sq_copy(k).start()
    fetch(EARLY, PAIRS)
    for k in reversed(range(rows - 1)):
        sq_copy(k, arrival=True).wait_recv()
    total_sq = sq_in[0]
    for k in range(1, rows):
        total_sq = total_sq + sq_in[k]
    scale_row = lax.rsqrt(total_sq / features + EPS)
    scale = row_to_column(scale_row)
    for k in range(width // LANES):
        at = slice(k * LANES, (k + 1) * LANES)
        x_ref[:, at] = (h_ref[:, at].astype(jnp.float32) * scale * gain_ref[at]).astype(jnp.bfloat16)

    def partner_tile(q, cut=0):
        w_copy(q, False).wait()
        core_out[q, :, cut:] = jnp.dot(x_ref[...], w_partner[q % PAIRS, :, cut:], preferred_element_type=jnp.float32)

        @pl.when(q + PAIRS < partner_count + tiles)
        def _():
            w_copy(q + PAIRS, False).start()

        core_copy(q, cut).start()

    def own_tile(q, total, cut=0):
        w_copy(q, True).wait()
        total[...] = jnp.dot(x_ref[...], w_own[q % PAIRS, :, cut:], preferred_element_type=jnp.float32)

        @pl.when(q + PAIRS < own_count + tiles)
        def _():
            w_copy(q + PAIRS, True).start()

        core_copy(q, cut).wait_recv()
        total[...] += core_in[q, :, cut:]

    def columns(i):
        return pl.ds(pl.multiple_of(i * TILE, TILE), TILE)

    def send_tile(s):
        own_tile(s, chip_out.at[s])

    def keep_tile(s):
        own_tile(s, z_ref.at[:, columns(s - own_count)])

    edge_fetch(0).wait()
    edge_fetch(1).wait()
    edge = jnp.dot(x_ref[...], w_edge[...], preferred_element_type=jnp.float32)
    for k in range(2):
        edge_out[k] = edge[:, k * EDGE:(k + 1) * EDGE]
        edge_copy(k).start()
    partner_tile(0, EDGE)
    partner_tile(1)
    own_tile(0, chip_out.at[0, :, pl.ds(EDGE, TILE - EDGE)], EDGE)
    chip_copy(0, 0, 1, EDGE).start()

    @pl.loop(1, 3)
    def _(s):
        partner_tile(s + 1)
        send_tile(s)

    chip_copy(1, 1, 2).start()

    @pl.loop(2, last_group)
    def _(group):
        @pl.loop(0, GROUP)
        def _(t):
            s = group_start(group) + t
            partner_tile(s + 1)
            send_tile(s)

        chip_copy(group, group_start(group), GROUP).start()

    @pl.loop(tiles - SHIFT, tiles + SHIFT)
    def _(s):
        partner_tile(s + 1)
        pl.when(core == 1)(lambda: send_tile(s))
        pl.when(core == 0)(lambda: keep_tile(s))

    pl.when(core == 1)(lambda: chip_copy(last_group, tiles - SHIFT, 2 * SHIFT).start())

    @pl.loop(tiles + SHIFT, 2 * tiles + SHIFT)
    def _(s):
        pl.when(s + 1 < partner_count + tiles)(lambda: partner_tile(s + 1))
        pl.when(s < own_count + tiles)(lambda: keep_tile(s))

    lane_peak[...] = jnp.full((batch, LANES), -jnp.inf, jnp.float32)
    lane_mass[...] = jnp.zeros((batch, LANES), jnp.float32)

    def finish(place, first, count, edges=None):
        if edges is None:
            chip_arrival(place, first, count).wait_recv()
        else:
            for k in range(2):
                edge_copy(k, arrival=edges + k).wait_recv()
            chip_in[first, :, :EDGE] = edge_in[edges] + edge_in[edges + 1]
            chip_arrival(place, first, count, EDGE).wait_recv()

        @pl.loop(first, first + count)
        def _(i):
            z = z_ref[:, columns(i)] + chip_in[i]
            z_ref[:, columns(i)] = z
            parts = [z[:, k * LANES:(k + 1) * LANES] for k in range(TILE // LANES)]
            peak = lane_peak[...]
            new_peak = functools.reduce(jnp.maximum, parts, peak)
            mass = lane_mass[...] * jnp.exp(peak - new_peak)
            for part in parts:
                mass = mass + jnp.exp(part - new_peak)
            lane_peak[...] = new_peak
            lane_mass[...] = mass

    @pl.when(core == 0)
    def _():
        finish(0, 0, 1, edges=0)
        finish(tail, tiles - 1, 1, edges=2)

    finish(1, 1 - core, 2)

    @pl.loop(2, last_group)
    def _(group):
        finish(group, group_start(group) - core, GROUP)

    pl.when(core == 1)(lambda: finish(last_group, tiles - 2 * SHIFT, 2 * SHIFT))

    peaks_by_lane, mass_by_lane = lane_peak[...].T, lane_mass[...].T
    peak = jnp.max(peaks_by_lane, axis=0, keepdims=True)
    mass = jnp.sum(mass_by_lane * jnp.exp(peaks_by_lane - peak), axis=0, keepdims=True)
    first = lax.broadcasted_iota(jnp.int32, (2, batch), 0) == 0
    message = jnp.where(first, peak, mass)
    mass_out[...] = message
    mass_in[me] = message

    def mass_copy(k, arrival=False):
        peer, place = peers[k]
        slot = place if arrival else me
        return pltpu.make_async_remote_copy(
            mass_out, mass_in.at[slot], mass_send.at[k], mass_recv.at[slot],
            device_id=peer, device_id_type=MESH,
        )

    everyone = cols * rows
    for k in range(everyone - 1):
        mass_copy(k).start()

    for k in range(rows - 1):
        sq_copy(k).wait_send()

    core_copy(0, EDGE).wait_send()

    @pl.loop(1, partner_count + tiles)
    def _(s):
        core_copy(s).wait_send()

    for k in range(2):
        edge_copy(k).wait_send()
    chip_copy(0, 0, 1, EDGE).wait_send()
    chip_copy(1, 1, 2).wait_send()

    @pl.loop(2, last_group)
    def _(group):
        chip_copy(group, group_start(group), GROUP).wait_send()

    pl.when(core == 1)(lambda: chip_copy(last_group, tiles - SHIFT, 2 * SHIFT).wait_send())

    for k in reversed(range(everyone - 1)):
        mass_copy(k, arrival=True).wait_recv()
    peaks = [mass_in[d, 0:1] for d in range(everyone)]
    top = functools.reduce(jnp.maximum, peaks)
    total = jnp.zeros_like(top)
    for d in range(everyone):
        total = total + mass_in[d, 1:2] * jnp.exp(peaks[d] - top)
    log_norm = top + jnp.log(total)
    lse_row_ref[...] = log_norm
    lse_col_ref[...] = jnp.broadcast_to(row_to_column(log_norm), (batch, LANES))

    for k in range(everyone - 1):
        mass_copy(k).wait_send()


def subtract_kernel(z_ref, lse_col_ref, lse_row_ref, out_hbm, log_norm_hbm, out_ref, log_norm_ref, sem, log_norm_sem):
    batch, block = z_ref.shape
    log_norm_ref[...] = lse_row_ref[0]
    copies = [pltpu.make_async_copy(log_norm_ref, log_norm_hbm, log_norm_sem)]
    copies[0].start()
    for n in range(batch // SUBLANES):
        at = slice(n * SUBLANES, (n + 1) * SUBLANES)
        lse = lse_col_ref[at]
        for k in range(0, block, LANES):
            out_ref[at, k:k + LANES] = z_ref[at, k:k + LANES] - lse
        rows = pl.ds(n * SUBLANES, SUBLANES)
        copies.append(pltpu.make_async_copy(out_ref.at[rows], out_hbm.at[rows], sem.at[n]))
        copies[-1].start()
    for copy in copies:
        copy.wait()


def solution(mesh):
    cols, rows = mesh.shape["col"], mesh.shape["row"]

    def local_head(hidden, norm_gain, w_head):
        batch, width = hidden.shape
        block = w_head.shape[1] // rows
        tiles = block // TILE
        sizes = (cols, rows, width, block, tiles, width * rows)
        f32 = jnp.float32
        dma = pltpu.SemaphoreType.DMA
        vmem = pl.BlockSpec(memory_space=pltpu.VMEM)
        hbm = pl.BlockSpec(memory_space=pl.ANY)
        z, lse_col, lse_row = pl.pallas_call(
            functools.partial(head_kernel, sizes),
            name="head",
            out_shape=(
                pltpu.VMEM((batch, block), f32),
                pltpu.VMEM((batch, LANES), f32),
                pltpu.VMEM((1, batch), f32),
            ),
            in_specs=[pl.BlockSpec(memory_space=pltpu.HBM)] * 3,
            out_specs=[vmem] * 3,
            scratch_shapes=[
                pltpu.VMEM((batch, width), jnp.bfloat16),
                pltpu.VMEM((width,), f32),
                pltpu.VMEM((batch, width), jnp.bfloat16),
                pltpu.VMEM((PAIRS, width, TILE), jnp.bfloat16),
                pltpu.VMEM((PAIRS, width, TILE), jnp.bfloat16),
                pltpu.VMEM((2 * tiles + SHIFT, batch, TILE), f32),
                pltpu.VMEM((2 * tiles + SHIFT, batch, TILE), f32),
                pltpu.VMEM((tiles + SHIFT, batch, TILE), f32),
                pltpu.VMEM((tiles, batch, TILE), f32),
                pltpu.VMEM((1, batch), f32),
                pltpu.VMEM((rows, 1, batch), f32),
                pltpu.VMEM((2, batch), f32),
                pltpu.VMEM((cols * rows, 2, batch), f32),
                pltpu.VMEM((batch, LANES), f32),
                pltpu.VMEM((batch, LANES), f32),
                pltpu.VMEM((width, 2 * EDGE), jnp.bfloat16),
                pltpu.VMEM((2, batch, EDGE), f32),
                pltpu.VMEM((4, batch, EDGE), f32),
                dma((2,)),
                dma((2,)),
                dma((4,)),
                dma,
                dma,
                dma((PAIRS,)),
                dma((PAIRS,)),
                dma((2 * tiles + SHIFT,)),
                dma((2 * tiles + SHIFT,)),
                dma((tiles + SHIFT,)),
                dma((tiles,)),
                dma((rows,)),
                dma((rows,)),
                dma((cols * rows,)),
                dma((cols * rows,)),
            ],
            compiler_params=pltpu.CompilerParams(
                collective_id=0, has_side_effects=True, vmem_limit_bytes=VMEM_LIMIT
            ),
        )(*(pltpu.with_memory_space_constraint(a, pltpu.HBM) for a in (hidden, norm_gain, w_head)))
        return pl.pallas_call(
            subtract_kernel,
            name="subtract",
            out_shape=(
                jax.ShapeDtypeStruct((batch, block), f32),
                jax.ShapeDtypeStruct((batch,), f32),
            ),
            in_specs=[vmem] * 3,
            out_specs=[hbm] * 2,
            scratch_shapes=[pltpu.VMEM((batch, block), f32), pltpu.VMEM((batch,), f32), dma((batch // SUBLANES,)), dma],
            compiler_params=pltpu.CompilerParams(vmem_limit_bytes=16 * 1024 * 1024),
        )(z, lse_col, lse_row)

    return jax.shard_map(
        local_head,
        mesh=mesh,
        in_specs=(P("dp", "row"), P("row"), P("row", "col")),
        out_specs=(P("dp", ("col", "row")), P("dp")),
        check_vma=False,
    )
```

```python
import functools

import jax
import jax.numpy as jnp
from jax import lax
from jax.experimental import pallas as pl
from jax.experimental.pallas import tpu as pltpu
from jax.sharding import PartitionSpec as P

EPS = 1e-5
MESH = pl.DeviceIdType.MESH
LANES = 128
TILE = 512
PAIRS = 6
GROUP = 4
EARLY = 2
EDGE = 128
SHIFT = 1
SUBLANES = 8
VMEM_LIMIT = 48 * 1024 * 1024


def diagonal(batch):
    shape = (batch, batch)
    return lax.broadcasted_iota(jnp.int32, shape, 0) == lax.broadcasted_iota(jnp.int32, shape, 1)


def column_to_row(column):
    batch = column.shape[0]
    return jnp.sum(jnp.where(diagonal(batch), column, 0.0), axis=0, keepdims=True)


def row_to_column(row):
    return jnp.sum(jnp.where(diagonal(row.shape[1]), row, 0.0), axis=1, keepdims=True)


def head_kernel(
    sizes,
    hidden_hbm,
    gain_hbm,
    w_hbm,
    z_ref,
    lse_col_ref,
    lse_row_ref,
    h_ref,
    gain_ref,
    x_ref,
    w_own,
    w_partner,
    core_out,
    core_in,
    chip_out,
    chip_in,
    sq_out,
    sq_in,
    mass_out,
    mass_in,
    lane_peak,
    lane_mass,
    w_edge,
    edge_out,
    edge_in,
    edge_sem,
    edge_send,
    edge_recv,
    h_sem,
    gain_sem,
    w_own_sem,
    w_partner_sem,
    core_send,
    core_recv,
    chip_send,
    chip_recv,
    sq_send,
    sq_recv,
    mass_send,
    mass_recv,
):
    cols, rows, width, block, tiles, features = sizes
    dp, col, row = lax.axis_index("dp"), lax.axis_index("col"), lax.axis_index("row")
    chip, core = row // 2, row % 2
    batch = h_ref.shape[0]

    def device(flip_col, flip_chip, flip_core):
        c = 1 - col if flip_col else col
        r = (1 - chip if flip_chip else chip) * 2 + (1 - core if flip_core else core)
        return (dp, c, r), c * rows + r

    me = device(0, 0, 0)[1]
    row_peers = [device(0, 1, 1), device(0, 1, 0), device(0, 0, 1)]
    mirror = device(1, 0, 0)
    peers = [device(1, 1, 1), device(1, 1, 0), device(1, 0, 1), mirror, *row_peers]
    partner = row_peers[2][0]

    own_count = tiles - SHIFT + core * 2 * SHIFT
    partner_count = 2 * tiles - own_count

    def w_copy(s, own):
        count = own_count if own else partner_count
        side = core if own else 1 - core
        late = jnp.where(s < count, 0, 1)
        tile = (1 - late) * (side * (tiles - SHIFT) + s) + late * (side * tiles + s - count)
        start = (late * chip + (1 - late) * (1 - chip)) * 2 * block + tile * TILE
        buf, sem = (w_own, w_own_sem) if own else (w_partner, w_partner_sem)
        slot = s % PAIRS
        return pltpu.make_async_copy(
            w_hbm.at[:, pl.ds(pl.multiple_of(start, TILE), TILE)], buf.at[slot], sem.at[slot]
        )

    def core_copy(s, cut=0):
        at = pl.ds(cut, TILE - cut)
        return pltpu.make_async_remote_copy(
            core_out.at[s, :, at], core_in.at[s, :, at], core_send.at[s], core_recv.at[s],
            device_id=partner, device_id_type=MESH,
        )

    def chip_copy(group, s, count, cut=0):
        at = pl.ds(cut, TILE - cut)
        tile = core * (tiles - SHIFT) + s
        place = core * tail if isinstance(group, int) and group == 0 else group
        return pltpu.make_async_remote_copy(
            chip_out.at[pl.ds(s, count), :, at], chip_in.at[pl.ds(tile % tiles, count), :, at],
            chip_send.at[group], chip_recv.at[place],
            device_id=(dp, col, (1 - chip) * 2 + tile // tiles), device_id_type=MESH,
        )

    def chip_arrival(place, first, count, cut=0):
        at = pl.ds(cut, TILE - cut)
        return pltpu.make_async_remote_copy(
            chip_out.at[pl.ds(0, count), :, at], chip_in.at[pl.ds(first, count), :, at],
            chip_send.at[0], chip_recv.at[place],
            device_id=row_peers[1][0], device_id_type=MESH,
        )

    def edge_start(own):
        side = core if own else 1 - core
        start = (1 - chip) * 2 * block + side * (tiles - SHIFT) * TILE
        return pl.ds(pl.multiple_of(start, TILE), EDGE)

    def edge_fetch(k):
        return pltpu.make_async_copy(
            w_hbm.at[:, edge_start(k == 0)], w_edge.at[:, pl.ds(k * EDGE, EDGE)], edge_sem.at[k]
        )

    def edge_copy(k, arrival=None):
        place = arrival if arrival is not None else 2 * core if k == 0 else 3 - 2 * core
        return pltpu.make_async_remote_copy(
            edge_out.at[k], edge_in.at[place], edge_send.at[k], edge_recv.at[place],
            device_id=(dp, col, (1 - chip) * 2), device_id_type=MESH,
        )

    def group_start(group):
        return (group - 2) * GROUP + 3

    last_group = 2 + (tiles - SHIFT - 3) // GROUP
    tail = last_group + 1

    h_copy = pltpu.make_async_copy(hidden_hbm, h_ref, h_sem)
    gain_copy = pltpu.make_async_copy(gain_hbm, gain_ref, gain_sem)
    h_copy.start()
    gain_copy.start()

    barrier = pltpu.get_barrier_semaphore()
    for peer, _ in [mirror, *row_peers]:
        pl.semaphore_signal(barrier, inc=1, device_id=peer, device_id_type=MESH)

    def fetch(first, last):
        @pl.loop(first, last)
        def _(q):
            w_copy(q, False).start()
            w_copy(q, True).start()

    edge_fetch(0).start()
    edge_fetch(1).start()
    fetch(0, EARLY)

    h_copy.wait()
    gain_copy.wait()
    squares = jnp.zeros((batch, LANES), jnp.float32)
    for k in range(width // LANES):
        part = h_ref[:, k * LANES:(k + 1) * LANES].astype(jnp.float32)
        squares = squares + part * part
    local_sq = column_to_row(jnp.sum(squares, axis=1, keepdims=True))
    sq_out[...] = local_sq
    sq_in[row] = local_sq
    pl.semaphore_wait(barrier, rows)

    def sq_copy(k, arrival=False):
        peer, _ = row_peers[k]
        slot = peer[2] if arrival else row
        return pltpu.make_async_remote_copy(
            sq_out, sq_in.at[slot], sq_send.at[k], sq_recv.at[slot],
            device_id=peer, device_id_type=MESH,
        )

    for k in range(rows - 1):
        sq_copy(k).start()
    fetch(EARLY, PAIRS)
    for k in reversed(range(rows - 1)):
        sq_copy(k, arrival=True).wait_recv()
    total_sq = sq_in[0]
    for k in range(1, rows):
        total_sq = total_sq + sq_in[k]
    scale_row = lax.rsqrt(total_sq / features + EPS)
    scale = row_to_column(scale_row)
    for k in range(width // LANES):
        at = slice(k * LANES, (k + 1) * LANES)
        x_ref[:, at] = (h_ref[:, at].astype(jnp.float32) * scale * gain_ref[at]).astype(jnp.bfloat16)

    def partner_tile(q, cut=0):
        w_copy(q, False).wait()
        core_out[q, :, cut:] = jnp.dot(x_ref[...], w_partner[q % PAIRS, :, cut:], preferred_element_type=jnp.float32)

        @pl.when(q + PAIRS < partner_count + tiles)
        def _():
            w_copy(q + PAIRS, False).start()

        core_copy(q, cut).start()

    def own_tile(q, total, cut=0):
        w_copy(q, True).wait()
        total[...] = jnp.dot(x_ref[...], w_own[q % PAIRS, :, cut:], preferred_element_type=jnp.float32)

        @pl.when(q + PAIRS < own_count + tiles)
        def _():
            w_copy(q + PAIRS, True).start()

        core_copy(q, cut).wait_recv()
        total[...] += core_in[q, :, cut:]

    def columns(i):
        return pl.ds(pl.multiple_of(i * TILE, TILE), TILE)

    def send_tile(s):
        own_tile(s, chip_out.at[s])

    def keep_tile(s):
        own_tile(s, z_ref.at[:, columns(s - own_count)])

    edge_fetch(0).wait()
    edge_fetch(1).wait()
    half = width // 2
    edge = jnp.dot(x_ref[:, :half], w_edge[:half], preferred_element_type=jnp.float32)
    edge += jnp.dot(x_ref[:, half:], w_edge[half:], preferred_element_type=jnp.float32)
    for k in range(2):
        edge_out[k] = edge[:, k * EDGE:(k + 1) * EDGE]
        edge_copy(k).start()
    partner_tile(0, EDGE)
    partner_tile(1)
    own_tile(0, chip_out.at[0, :, pl.ds(EDGE, TILE - EDGE)], EDGE)
    chip_copy(0, 0, 1, EDGE).start()

    @pl.loop(1, 3)
    def _(s):
        partner_tile(s + 1)
        send_tile(s)

    chip_copy(1, 1, 2).start()

    def pace(group):
        chip_arrival(group, group_start(group) - core, GROUP).wait_recv()

    @pl.loop(2, last_group)
    def _(group):
        pl.when(group == 4)(lambda: chip_arrival(1, 1 - core, 2).wait_recv())
        pl.when((group > 4) & (group % 2 == 0))(lambda: pace(group // 2 - 1))

        @pl.loop(0, GROUP)
        def _(t):
            s = group_start(group) + t
            partner_tile(s + 1)
            send_tile(s)

        chip_copy(group, group_start(group), GROUP).start()

    @pl.loop(tiles - SHIFT, tiles + SHIFT)
    def _(s):
        partner_tile(s + 1)
        pl.when(core == 1)(lambda: send_tile(s))
        pl.when(core == 0)(lambda: keep_tile(s))

    pl.when(core == 1)(lambda: chip_copy(last_group, tiles - SHIFT, 2 * SHIFT).start())

    @pl.loop(tiles + SHIFT, 2 * tiles + SHIFT)
    def _(s):
        step = s - tiles - SHIFT
        pl.when(step % (2 * GROUP) == GROUP)(lambda: pace(last_group // 2 + step // (2 * GROUP)))
        pl.when(s + 1 < partner_count + tiles)(lambda: partner_tile(s + 1))
        pl.when(s < own_count + tiles)(lambda: keep_tile(s))

    lane_peak[...] = jnp.full((batch, LANES), -jnp.inf, jnp.float32)
    lane_mass[...] = jnp.zeros((batch, LANES), jnp.float32)

    def finish(place, first, count, edges=None, wait=True):
        if wait and edges is None:
            chip_arrival(place, first, count).wait_recv()
        if edges is not None:
            for k in range(2):
                edge_copy(k, arrival=edges + k).wait_recv()
            chip_in[first, :, :EDGE] = edge_in[edges] + edge_in[edges + 1]
            chip_arrival(place, first, count, EDGE).wait_recv()

        @pl.loop(first, first + count)
        def _(i):
            z = z_ref[:, columns(i)] + chip_in[i]
            z_ref[:, columns(i)] = z
            parts = [z[:, k * LANES:(k + 1) * LANES] for k in range(TILE // LANES)]
            peak = lane_peak[...]
            new_peak = functools.reduce(jnp.maximum, parts, peak)
            mass = lane_mass[...] * jnp.exp(peak - new_peak)
            for part in parts:
                mass = mass + jnp.exp(part - new_peak)
            lane_peak[...] = new_peak
            lane_mass[...] = mass

    @pl.when(core == 0)
    def _():
        finish(0, 0, 1, edges=0)
        finish(tail, tiles - 1, 1, edges=2)

    finish(1, 1 - core, 2, wait=False)

    @pl.loop(2, last_group - 1)
    def _(group):
        finish(group, group_start(group) - core, GROUP, wait=False)

    finish(last_group - 1, group_start(last_group - 1) - core, GROUP)

    pl.when(core == 1)(lambda: finish(last_group, tiles - 2 * SHIFT, 2 * SHIFT))

    peaks_by_lane, mass_by_lane = lane_peak[...].T, lane_mass[...].T
    peak = jnp.max(peaks_by_lane, axis=0, keepdims=True)
    mass = jnp.sum(mass_by_lane * jnp.exp(peaks_by_lane - peak), axis=0, keepdims=True)
    first = lax.broadcasted_iota(jnp.int32, (2, batch), 0) == 0
    message = jnp.where(first, peak, mass)
    mass_out[...] = message
    mass_in[me] = message

    def mass_copy(k, arrival=False):
        peer, place = peers[k]
        slot = place if arrival else me
        return pltpu.make_async_remote_copy(
            mass_out, mass_in.at[slot], mass_send.at[k], mass_recv.at[slot],
            device_id=peer, device_id_type=MESH,
        )

    everyone = cols * rows
    for k in range(everyone - 1):
        mass_copy(k).start()

    for k in range(rows - 1):
        sq_copy(k).wait_send()

    core_copy(0, EDGE).wait_send()

    @pl.loop(1, partner_count + tiles)
    def _(s):
        core_copy(s).wait_send()

    for k in range(2):
        edge_copy(k).wait_send()
    chip_copy(0, 0, 1, EDGE).wait_send()
    chip_copy(1, 1, 2).wait_send()

    @pl.loop(2, last_group)
    def _(group):
        chip_copy(group, group_start(group), GROUP).wait_send()

    pl.when(core == 1)(lambda: chip_copy(last_group, tiles - SHIFT, 2 * SHIFT).wait_send())

    for k in reversed(range(everyone - 1)):
        mass_copy(k, arrival=True).wait_recv()
    peaks = [mass_in[d, 0:1] for d in range(everyone)]
    top = functools.reduce(jnp.maximum, peaks)
    total = jnp.zeros_like(top)
    for d in range(everyone):
        total = total + mass_in[d, 1:2] * jnp.exp(peaks[d] - top)
    log_norm = top + jnp.log(total)
    lse_row_ref[...] = log_norm
    lse_col_ref[...] = jnp.broadcast_to(row_to_column(log_norm), (batch, LANES))

    for k in range(everyone - 1):
        mass_copy(k).wait_send()


def subtract_kernel(z_ref, lse_col_ref, lse_row_ref, out_hbm, log_norm_hbm, out_ref, log_norm_ref, sem, log_norm_sem):
    batch, block = z_ref.shape
    log_norm_ref[...] = lse_row_ref[0]
    copies = [pltpu.make_async_copy(log_norm_ref, log_norm_hbm, log_norm_sem)]
    copies[0].start()
    for n in range(batch // SUBLANES):
        at = slice(n * SUBLANES, (n + 1) * SUBLANES)
        lse = lse_col_ref[at]
        for k in range(0, block, LANES):
            out_ref[at, k:k + LANES] = z_ref[at, k:k + LANES] - lse
        rows = pl.ds(n * SUBLANES, SUBLANES)
        copies.append(pltpu.make_async_copy(out_ref.at[rows], out_hbm.at[rows], sem.at[n]))
        copies[-1].start()
    for copy in copies:
        copy.wait()


def solution(mesh):
    cols, rows = mesh.shape["col"], mesh.shape["row"]

    def local_head(hidden, norm_gain, w_head):
        batch, width = hidden.shape
        block = w_head.shape[1] // rows
        tiles = block // TILE
        sizes = (cols, rows, width, block, tiles, width * rows)
        f32 = jnp.float32
        dma = pltpu.SemaphoreType.DMA
        vmem = pl.BlockSpec(memory_space=pltpu.VMEM)
        hbm = pl.BlockSpec(memory_space=pl.ANY)
        z, lse_col, lse_row = pl.pallas_call(
            functools.partial(head_kernel, sizes),
            name="head",
            out_shape=(
                pltpu.VMEM((batch, block), f32),
                pltpu.VMEM((batch, LANES), f32),
                pltpu.VMEM((1, batch), f32),
            ),
            in_specs=[pl.BlockSpec(memory_space=pltpu.HBM)] * 3,
            out_specs=[vmem] * 3,
            scratch_shapes=[
                pltpu.VMEM((batch, width), jnp.bfloat16),
                pltpu.VMEM((width,), f32),
                pltpu.VMEM((batch, width), jnp.bfloat16),
                pltpu.VMEM((PAIRS, width, TILE), jnp.bfloat16),
                pltpu.VMEM((PAIRS, width, TILE), jnp.bfloat16),
                pltpu.VMEM((2 * tiles + SHIFT, batch, TILE), f32),
                pltpu.VMEM((2 * tiles + SHIFT, batch, TILE), f32),
                pltpu.VMEM((tiles + SHIFT, batch, TILE), f32),
                pltpu.VMEM((tiles, batch, TILE), f32),
                pltpu.VMEM((1, batch), f32),
                pltpu.VMEM((rows, 1, batch), f32),
                pltpu.VMEM((2, batch), f32),
                pltpu.VMEM((cols * rows, 2, batch), f32),
                pltpu.VMEM((batch, LANES), f32),
                pltpu.VMEM((batch, LANES), f32),
                pltpu.VMEM((width, 2 * EDGE), jnp.bfloat16),
                pltpu.VMEM((2, batch, EDGE), f32),
                pltpu.VMEM((4, batch, EDGE), f32),
                dma((2,)),
                dma((2,)),
                dma((4,)),
                dma,
                dma,
                dma((PAIRS,)),
                dma((PAIRS,)),
                dma((2 * tiles + SHIFT,)),
                dma((2 * tiles + SHIFT,)),
                dma((tiles + SHIFT,)),
                dma((tiles,)),
                dma((rows,)),
                dma((rows,)),
                dma((cols * rows,)),
                dma((cols * rows,)),
            ],
            compiler_params=pltpu.CompilerParams(
                collective_id=0, has_side_effects=True, vmem_limit_bytes=VMEM_LIMIT
            ),
        )(*(pltpu.with_memory_space_constraint(a, pltpu.HBM) for a in (hidden, norm_gain, w_head)))
        return pl.pallas_call(
            subtract_kernel,
            name="subtract",
            out_shape=(
                jax.ShapeDtypeStruct((batch, block), f32),
                jax.ShapeDtypeStruct((batch,), f32),
            ),
            in_specs=[vmem] * 3,
            out_specs=[hbm] * 2,
            scratch_shapes=[pltpu.VMEM((batch, block), f32), pltpu.VMEM((batch,), f32), dma((batch // SUBLANES,)), dma],
            compiler_params=pltpu.CompilerParams(vmem_limit_bytes=16 * 1024 * 1024),
        )(z, lse_col, lse_row)

    return jax.shard_map(
        local_head,
        mesh=mesh,
        in_specs=(P("dp", "row"), P("row"), P("row", "col")),
        out_specs=(P("dp", ("col", "row")), P("dp")),
        check_vma=False,
    )
```

```python
import functools

import jax
import jax.numpy as jnp
from jax import lax
from jax.experimental import pallas as pl
from jax.experimental.pallas import tpu as pltpu
from jax.sharding import PartitionSpec as P

EPS = 1e-5
MESH = pl.DeviceIdType.MESH
LANES = 128
TILE = 512
PAIRS = 6
GROUP = 4
EDGE = 128
SHIFT = 1
SUBLANES = 8
VMEM_LIMIT = 48 * 1024 * 1024


def diagonal(batch):
    shape = (batch, batch)
    return lax.broadcasted_iota(jnp.int32, shape, 0) == lax.broadcasted_iota(jnp.int32, shape, 1)


def column_to_row(column):
    batch = column.shape[0]
    return jnp.sum(jnp.where(diagonal(batch), column, 0.0), axis=0, keepdims=True)


def row_to_column(row):
    return jnp.sum(jnp.where(diagonal(row.shape[1]), row, 0.0), axis=1, keepdims=True)


def head_kernel(
    sizes,
    hidden_hbm,
    gain_hbm,
    w_hbm,
    z_ref,
    lse_col_ref,
    lse_row_ref,
    h_ref,
    gain_ref,
    x_ref,
    w_own,
    w_partner,
    core_out,
    core_in,
    chip_out,
    chip_in,
    sq_out,
    sq_in,
    mass_out,
    mass_in,
    lane_peak,
    lane_mass,
    w_edge,
    edge_out,
    edge_in,
    edge_sem,
    edge_send,
    edge_recv,
    h_sem,
    gain_sem,
    w_own_sem,
    w_partner_sem,
    core_send,
    core_recv,
    chip_send,
    chip_recv,
    sq_send,
    sq_recv,
    mass_send,
    mass_recv,
):
    cols, rows, width, block, tiles, features = sizes
    dp, col, row = lax.axis_index("dp"), lax.axis_index("col"), lax.axis_index("row")
    chip, core = row // 2, row % 2
    batch = h_ref.shape[0]

    def device(flip_col, flip_chip, flip_core):
        c = 1 - col if flip_col else col
        r = (1 - chip if flip_chip else chip) * 2 + (1 - core if flip_core else core)
        return (dp, c, r), c * rows + r

    me = device(0, 0, 0)[1]
    row_peers = [device(0, 1, 1), device(0, 1, 0), device(0, 0, 1)]
    mirror = device(1, 0, 0)
    peers = [device(1, 1, 1), device(1, 1, 0), device(1, 0, 1), mirror, *row_peers]
    partner = row_peers[2][0]

    own_count = tiles - SHIFT + core * 2 * SHIFT
    partner_count = 2 * tiles - own_count

    def w_copy(s, own):
        count = own_count if own else partner_count
        side = core if own else 1 - core
        late = jnp.where(s < count, 0, 1)
        tile = (1 - late) * (side * (tiles - SHIFT) + s) + late * (side * tiles + s - count)
        start = (late * chip + (1 - late) * (1 - chip)) * 2 * block + tile * TILE
        buf, sem = (w_own, w_own_sem) if own else (w_partner, w_partner_sem)
        slot = s % PAIRS
        return pltpu.make_async_copy(
            w_hbm.at[:, pl.ds(pl.multiple_of(start, TILE), TILE)], buf.at[slot], sem.at[slot]
        )

    def core_copy(s, cut=0):
        at = pl.ds(cut, TILE - cut)
        return pltpu.make_async_remote_copy(
            core_out.at[s, :, at], core_in.at[s, :, at], core_send.at[s], core_recv.at[s],
            device_id=partner, device_id_type=MESH,
        )

    def chip_copy(group, s, count, cut=0):
        at = pl.ds(cut, TILE - cut)
        tile = core * (tiles - SHIFT) + s
        place = core * tail if isinstance(group, int) and group == 0 else group
        return pltpu.make_async_remote_copy(
            chip_out.at[pl.ds(s, count), :, at], chip_in.at[pl.ds(tile % tiles, count), :, at],
            chip_send.at[group], chip_recv.at[place],
            device_id=(dp, col, (1 - chip) * 2 + tile // tiles), device_id_type=MESH,
        )

    def chip_arrival(place, first, count, cut=0):
        at = pl.ds(cut, TILE - cut)
        return pltpu.make_async_remote_copy(
            chip_out.at[pl.ds(0, count), :, at], chip_in.at[pl.ds(first, count), :, at],
            chip_send.at[0], chip_recv.at[place],
            device_id=row_peers[1][0], device_id_type=MESH,
        )

    def edge_start(own):
        side = core if own else 1 - core
        start = (1 - chip) * 2 * block + side * (tiles - SHIFT) * TILE
        return pl.ds(pl.multiple_of(start, TILE), EDGE)

    def edge_fetch(k):
        return pltpu.make_async_copy(
            w_hbm.at[:, edge_start(k == 0)], w_edge.at[:, pl.ds(k * EDGE, EDGE)], edge_sem.at[k]
        )

    def edge_copy(k, arrival=None):
        place = arrival if arrival is not None else 2 * core if k == 0 else 3 - 2 * core
        return pltpu.make_async_remote_copy(
            edge_out.at[k], edge_in.at[place], edge_send.at[k], edge_recv.at[place],
            device_id=(dp, col, (1 - chip) * 2), device_id_type=MESH,
        )

    def group_start(group):
        return (group - 2) * GROUP + 3

    last_group = 2 + (tiles - SHIFT - 3) // GROUP
    tail = last_group + 1

    h_copy = pltpu.make_async_copy(hidden_hbm, h_ref, h_sem)
    gain_copy = pltpu.make_async_copy(gain_hbm, gain_ref, gain_sem)
    h_copy.start()
    gain_copy.start()

    barrier = pltpu.get_barrier_semaphore()
    for peer, _ in [mirror, *row_peers]:
        pl.semaphore_signal(barrier, inc=1, device_id=peer, device_id_type=MESH)

    def fetch(first, last):
        @pl.loop(first, last)
        def _(q):
            w_copy(q, False).start()
            w_copy(q, True).start()


    h_copy.wait()
    squares = jnp.zeros((batch, LANES), jnp.float32)
    for k in range(width // LANES):
        part = h_ref[:, k * LANES:(k + 1) * LANES].astype(jnp.float32)
        squares = squares + part * part
    local_sq = column_to_row(jnp.sum(squares, axis=1, keepdims=True))
    sq_out[...] = local_sq
    sq_in[row] = local_sq
    pl.semaphore_wait(barrier, rows)

    def sq_copy(k, arrival=False):
        peer, _ = row_peers[k]
        slot = peer[2] if arrival else row
        return pltpu.make_async_remote_copy(
            sq_out, sq_in.at[slot], sq_send.at[k], sq_recv.at[slot],
            device_id=peer, device_id_type=MESH,
        )

    for k in range(rows - 1):
        sq_copy(k).start()
    edge_fetch(0).start()
    edge_fetch(1).start()
    fetch(0, 1)
    gain_copy.wait()
    for k in reversed(range(rows - 1)):
        sq_copy(k, arrival=True).wait_recv()
    fetch(1, 2)
    total_sq = sq_in[0]
    for k in range(1, rows):
        total_sq = total_sq + sq_in[k]
    scale_row = lax.rsqrt(total_sq / features + EPS)
    scale = row_to_column(scale_row)
    for k in range(width // LANES):
        at = slice(k * LANES, (k + 1) * LANES)
        x_ref[:, at] = (h_ref[:, at].astype(jnp.float32) * scale * gain_ref[at]).astype(jnp.bfloat16)

    def partner_tile(q, cut=0):
        w_copy(q, False).wait()
        core_out[q, :, cut:] = jnp.dot(x_ref[...], w_partner[q % PAIRS, :, cut:], preferred_element_type=jnp.float32)

        @pl.when(q + PAIRS < partner_count + tiles)
        def _():
            w_copy(q + PAIRS, False).start()

        core_copy(q, cut).start()

    def own_tile(q, total, cut=0):
        w_copy(q, True).wait()
        total[...] = jnp.dot(x_ref[...], w_own[q % PAIRS, :, cut:], preferred_element_type=jnp.float32)

        @pl.when(q + PAIRS < own_count + tiles)
        def _():
            w_copy(q + PAIRS, True).start()

        core_copy(q, cut).wait_recv()
        total[...] += core_in[q, :, cut:]

    def columns(i):
        return pl.ds(pl.multiple_of(i * TILE, TILE), TILE)

    def send_tile(s):
        own_tile(s, chip_out.at[s])

    def keep_tile(s):
        own_tile(s, z_ref.at[:, columns(s - own_count)])

    edge_fetch(0).wait()
    edge_fetch(1).wait()
    for k in range(2):
        at = slice(k * EDGE, (k + 1) * EDGE)
        edge_out[k] = jnp.dot(x_ref[...], w_edge[:, at], preferred_element_type=jnp.float32)
    for k in range(2):
        edge_copy(k).start()
    fetch(2, 4)
    partner_tile(0, EDGE)
    fetch(4, PAIRS)
    partner_tile(1)
    own_tile(0, chip_out.at[0, :, pl.ds(EDGE, TILE - EDGE)], EDGE)
    chip_copy(0, 0, 1, EDGE).start()

    @pl.loop(1, 3)
    def _(s):
        partner_tile(s + 1)
        send_tile(s)

    chip_copy(1, 1, 2).start()

    @pl.loop(2, last_group)
    def _(group):
        @pl.loop(0, GROUP)
        def _(t):
            s = group_start(group) + t
            partner_tile(s + 1)
            send_tile(s)

        chip_copy(group, group_start(group), GROUP).start()

    @pl.loop(tiles - SHIFT, tiles + SHIFT)
    def _(s):
        partner_tile(s + 1)
        pl.when(core == 1)(lambda: send_tile(s))
        pl.when(core == 0)(lambda: keep_tile(s))

    pl.when(core == 1)(lambda: chip_copy(last_group, tiles - SHIFT, 2 * SHIFT).start())

    @pl.loop(tiles + SHIFT, 2 * tiles + SHIFT)
    def _(s):
        pl.when(s + 1 < partner_count + tiles)(lambda: partner_tile(s + 1))
        pl.when(s < own_count + tiles)(lambda: keep_tile(s))

    lane_peak[...] = jnp.full((batch, LANES), -jnp.inf, jnp.float32)
    lane_mass[...] = jnp.zeros((batch, LANES), jnp.float32)

    def finish(place, first, count, edges=None):
        if edges is None:
            chip_arrival(place, first, count).wait_recv()
        else:
            for k in range(2):
                edge_copy(k, arrival=edges + k).wait_recv()
            chip_in[first, :, :EDGE] = edge_in[edges] + edge_in[edges + 1]
            chip_arrival(place, first, count, EDGE).wait_recv()

        @pl.loop(first, first + count)
        def _(i):
            z = z_ref[:, columns(i)] + chip_in[i]
            z_ref[:, columns(i)] = z
            parts = [z[:, k * LANES:(k + 1) * LANES] for k in range(TILE // LANES)]
            peak = lane_peak[...]
            new_peak = functools.reduce(jnp.maximum, parts, peak)
            mass = lane_mass[...] * jnp.exp(peak - new_peak)
            for part in parts:
                mass = mass + jnp.exp(part - new_peak)
            lane_peak[...] = new_peak
            lane_mass[...] = mass

    @pl.when(core == 0)
    def _():
        finish(0, 0, 1, edges=0)
        finish(tail, tiles - 1, 1, edges=2)

    finish(1, 1 - core, 2)

    @pl.loop(2, last_group)
    def _(group):
        finish(group, group_start(group) - core, GROUP)

    pl.when(core == 1)(lambda: finish(last_group, tiles - 2 * SHIFT, 2 * SHIFT))

    peaks_by_lane, mass_by_lane = lane_peak[...].T, lane_mass[...].T
    peak = jnp.max(peaks_by_lane, axis=0, keepdims=True)
    mass = jnp.sum(mass_by_lane * jnp.exp(peaks_by_lane - peak), axis=0, keepdims=True)
    first = lax.broadcasted_iota(jnp.int32, (2, batch), 0) == 0
    message = jnp.where(first, peak, mass)
    mass_out[...] = message
    mass_in[me] = message

    def mass_copy(k, arrival=False):
        peer, place = peers[k]
        slot = place if arrival else me
        return pltpu.make_async_remote_copy(
            mass_out, mass_in.at[slot], mass_send.at[k], mass_recv.at[slot],
            device_id=peer, device_id_type=MESH,
        )

    everyone = cols * rows
    for k in range(everyone - 1):
        mass_copy(k).start()

    for k in range(rows - 1):
        sq_copy(k).wait_send()

    core_copy(0, EDGE).wait_send()

    @pl.loop(1, partner_count + tiles)
    def _(s):
        core_copy(s).wait_send()

    for k in range(2):
        edge_copy(k).wait_send()
    chip_copy(0, 0, 1, EDGE).wait_send()
    chip_copy(1, 1, 2).wait_send()

    @pl.loop(2, last_group)
    def _(group):
        chip_copy(group, group_start(group), GROUP).wait_send()

    pl.when(core == 1)(lambda: chip_copy(last_group, tiles - SHIFT, 2 * SHIFT).wait_send())

    for k in reversed(range(everyone - 1)):
        mass_copy(k, arrival=True).wait_recv()
    peaks = [mass_in[d, 0:1] for d in range(everyone)]
    top = functools.reduce(jnp.maximum, peaks)
    total = jnp.zeros_like(top)
    for d in range(everyone):
        total = total + mass_in[d, 1:2] * jnp.exp(peaks[d] - top)
    log_norm = top + jnp.log(total)
    lse_row_ref[...] = log_norm
    lse_col_ref[...] = jnp.broadcast_to(row_to_column(log_norm), (batch, LANES))

    for k in range(everyone - 1):
        mass_copy(k).wait_send()


def subtract_kernel(z_ref, lse_col_ref, lse_row_ref, out_hbm, log_norm_hbm, out_ref, log_norm_ref, sem, log_norm_sem):
    batch, block = z_ref.shape
    log_norm_ref[...] = lse_row_ref[0]
    copies = [pltpu.make_async_copy(log_norm_ref, log_norm_hbm, log_norm_sem)]
    copies[0].start()
    for n in range(batch // SUBLANES):
        at = slice(n * SUBLANES, (n + 1) * SUBLANES)
        lse = lse_col_ref[at]
        for k in range(0, block, LANES):
            out_ref[at, k:k + LANES] = z_ref[at, k:k + LANES] - lse
        rows = pl.ds(n * SUBLANES, SUBLANES)
        copies.append(pltpu.make_async_copy(out_ref.at[rows], out_hbm.at[rows], sem.at[n]))
        copies[-1].start()
    for copy in copies:
        copy.wait()


def solution(mesh):
    cols, rows = mesh.shape["col"], mesh.shape["row"]

    def local_head(hidden, norm_gain, w_head):
        batch, width = hidden.shape
        block = w_head.shape[1] // rows
        tiles = block // TILE
        sizes = (cols, rows, width, block, tiles, width * rows)
        f32 = jnp.float32
        dma = pltpu.SemaphoreType.DMA
        vmem = pl.BlockSpec(memory_space=pltpu.VMEM)
        hbm = pl.BlockSpec(memory_space=pl.ANY)
        z, lse_col, lse_row = pl.pallas_call(
            functools.partial(head_kernel, sizes),
            name="head",
            out_shape=(
                pltpu.VMEM((batch, block), f32),
                pltpu.VMEM((batch, LANES), f32),
                pltpu.VMEM((1, batch), f32),
            ),
            in_specs=[pl.BlockSpec(memory_space=pltpu.HBM)] * 3,
            out_specs=[vmem] * 3,
            scratch_shapes=[
                pltpu.VMEM((batch, width), jnp.bfloat16),
                pltpu.VMEM((width,), f32),
                pltpu.VMEM((batch, width), jnp.bfloat16),
                pltpu.VMEM((PAIRS, width, TILE), jnp.bfloat16),
                pltpu.VMEM((PAIRS, width, TILE), jnp.bfloat16),
                pltpu.VMEM((2 * tiles + SHIFT, batch, TILE), f32),
                pltpu.VMEM((2 * tiles + SHIFT, batch, TILE), f32),
                pltpu.VMEM((tiles + SHIFT, batch, TILE), f32),
                pltpu.VMEM((tiles, batch, TILE), f32),
                pltpu.VMEM((1, batch), f32),
                pltpu.VMEM((rows, 1, batch), f32),
                pltpu.VMEM((2, batch), f32),
                pltpu.VMEM((cols * rows, 2, batch), f32),
                pltpu.VMEM((batch, LANES), f32),
                pltpu.VMEM((batch, LANES), f32),
                pltpu.VMEM((width, 2 * EDGE), jnp.bfloat16),
                pltpu.VMEM((2, batch, EDGE), f32),
                pltpu.VMEM((4, batch, EDGE), f32),
                dma((2,)),
                dma((2,)),
                dma((4,)),
                dma,
                dma,
                dma((PAIRS,)),
                dma((PAIRS,)),
                dma((2 * tiles + SHIFT,)),
                dma((2 * tiles + SHIFT,)),
                dma((tiles + SHIFT,)),
                dma((tiles,)),
                dma((rows,)),
                dma((rows,)),
                dma((cols * rows,)),
                dma((cols * rows,)),
            ],
            compiler_params=pltpu.CompilerParams(
                collective_id=0, has_side_effects=True, vmem_limit_bytes=VMEM_LIMIT
            ),
        )(*(pltpu.with_memory_space_constraint(a, pltpu.HBM) for a in (hidden, norm_gain, w_head)))
        return pl.pallas_call(
            subtract_kernel,
            name="subtract",
            out_shape=(
                jax.ShapeDtypeStruct((batch, block), f32),
                jax.ShapeDtypeStruct((batch,), f32),
            ),
            in_specs=[vmem] * 3,
            out_specs=[hbm] * 2,
            scratch_shapes=[pltpu.VMEM((batch, block), f32), pltpu.VMEM((batch,), f32), dma((batch // SUBLANES,)), dma],
            compiler_params=pltpu.CompilerParams(vmem_limit_bytes=16 * 1024 * 1024),
        )(z, lse_col, lse_row)

    return jax.shard_map(
        local_head,
        mesh=mesh,
        in_specs=(P("dp", "row"), P("row"), P("row", "col")),
        out_specs=(P("dp", ("col", "row")), P("dp")),
        check_vma=False,
    )
```

```python
import functools

import jax
import jax.numpy as jnp
from jax import lax
from jax.experimental import pallas as pl
from jax.experimental.pallas import tpu as pltpu
from jax.sharding import PartitionSpec as P

EPS = 1e-5
MESH = pl.DeviceIdType.MESH
LANES = 128
TILE = 512
PAIRS = 6
GROUP = 4
EDGE = 128
SHIFT = 1
SUBLANES = 8
VMEM_LIMIT = 48 * 1024 * 1024


def diagonal(batch):
    shape = (batch, batch)
    return lax.broadcasted_iota(jnp.int32, shape, 0) == lax.broadcasted_iota(jnp.int32, shape, 1)


def column_to_row(column):
    batch = column.shape[0]
    return jnp.sum(jnp.where(diagonal(batch), column, 0.0), axis=0, keepdims=True)


def row_to_column(row):
    return jnp.sum(jnp.where(diagonal(row.shape[1]), row, 0.0), axis=1, keepdims=True)


def head_kernel(
    sizes,
    hidden_hbm,
    gain_hbm,
    w_hbm,
    z_ref,
    lse_col_ref,
    lse_row_ref,
    h_ref,
    gain_ref,
    x_ref,
    w_own,
    w_partner,
    core_out,
    core_in,
    chip_out,
    chip_in,
    sq_out,
    sq_in,
    mass_out,
    mass_in,
    lane_peak,
    lane_mass,
    w_edge,
    edge_out,
    edge_in,
    edge_sem,
    edge_send,
    edge_recv,
    h_sem,
    gain_sem,
    w_own_sem,
    w_partner_sem,
    core_send,
    core_recv,
    chip_send,
    chip_recv,
    sq_send,
    sq_recv,
    mass_send,
    mass_recv,
):
    cols, rows, width, block, tiles, features = sizes
    dp, col, row = lax.axis_index("dp"), lax.axis_index("col"), lax.axis_index("row")
    chip, core = row // 2, row % 2
    batch = h_ref.shape[0]

    def device(flip_col, flip_chip, flip_core):
        c = 1 - col if flip_col else col
        r = (1 - chip if flip_chip else chip) * 2 + (1 - core if flip_core else core)
        return (dp, c, r), c * rows + r

    me = device(0, 0, 0)[1]
    row_peers = [device(0, 1, 1), device(0, 1, 0), device(0, 0, 1)]
    mirror = device(1, 0, 0)
    peers = [device(1, 1, 1), device(1, 1, 0), device(1, 0, 1), mirror, *row_peers]
    partner = row_peers[2][0]

    own_count = tiles - SHIFT + core * 2 * SHIFT
    partner_count = 2 * tiles - own_count

    def w_copy(s, own):
        count = own_count if own else partner_count
        side = core if own else 1 - core
        late = jnp.where(s < count, 0, 1)
        tile = (1 - late) * (side * (tiles - SHIFT) + s) + late * (side * tiles + s - count)
        start = (late * chip + (1 - late) * (1 - chip)) * 2 * block + tile * TILE
        buf, sem = (w_own, w_own_sem) if own else (w_partner, w_partner_sem)
        slot = s % PAIRS
        return pltpu.make_async_copy(
            w_hbm.at[:, pl.ds(pl.multiple_of(start, TILE), TILE)], buf.at[slot], sem.at[slot]
        )

    def core_copy(s, cut=0):
        at = pl.ds(cut, TILE - cut)
        return pltpu.make_async_remote_copy(
            core_out.at[s, :, at], core_in.at[s, :, at], core_send.at[s], core_recv.at[s],
            device_id=partner, device_id_type=MESH,
        )

    def chip_copy(group, s, count, cut=0):
        at = pl.ds(cut, TILE - cut)
        tile = core * (tiles - SHIFT) + s
        place = core * tail if isinstance(group, int) and group == 0 else group
        return pltpu.make_async_remote_copy(
            chip_out.at[pl.ds(s, count), :, at], chip_in.at[pl.ds(tile % tiles, count), :, at],
            chip_send.at[group], chip_recv.at[place],
            device_id=(dp, col, (1 - chip) * 2 + tile // tiles), device_id_type=MESH,
        )

    def chip_arrival(place, first, count, cut=0):
        at = pl.ds(cut, TILE - cut)
        return pltpu.make_async_remote_copy(
            chip_out.at[pl.ds(0, count), :, at], chip_in.at[pl.ds(first, count), :, at],
            chip_send.at[0], chip_recv.at[place],
            device_id=row_peers[1][0], device_id_type=MESH,
        )

    def edge_start(own):
        side = core if own else 1 - core
        start = (1 - chip) * 2 * block + side * (tiles - SHIFT) * TILE
        return pl.ds(pl.multiple_of(start, TILE), EDGE)

    def edge_fetch(k):
        return pltpu.make_async_copy(
            w_hbm.at[:, edge_start(k == 0)], w_edge.at[:, pl.ds(k * EDGE, EDGE)], edge_sem.at[k]
        )

    def edge_copy(k, arrival=None):
        place = arrival if arrival is not None else 2 * core if k == 0 else 3 - 2 * core
        return pltpu.make_async_remote_copy(
            edge_out.at[k], edge_in.at[place], edge_send.at[k], edge_recv.at[place],
            device_id=(dp, col, (1 - chip) * 2), device_id_type=MESH,
        )

    def group_start(group):
        return (group - 2) * GROUP + 3

    last_group = 2 + (tiles - SHIFT - 3) // GROUP
    tail = last_group + 1

    h_copy = pltpu.make_async_copy(hidden_hbm, h_ref, h_sem)
    gain_copy = pltpu.make_async_copy(gain_hbm, gain_ref, gain_sem)
    h_copy.start()
    gain_copy.start()

    barrier = pltpu.get_barrier_semaphore()
    for peer, _ in [mirror, *row_peers]:
        pl.semaphore_signal(barrier, inc=1, device_id=peer, device_id_type=MESH)

    def fetch(first, last):
        @pl.loop(first, last)
        def _(q):
            w_copy(q, False).start()
            w_copy(q, True).start()


    edge_fetch(0).start()
    edge_fetch(1).start()
    fetch(0, 1)

    h_copy.wait()
    squares = jnp.zeros((batch, LANES), jnp.float32)
    for k in range(width // LANES):
        part = h_ref[:, k * LANES:(k + 1) * LANES].astype(jnp.float32)
        squares = squares + part * part
    local_sq = column_to_row(jnp.sum(squares, axis=1, keepdims=True))
    sq_out[...] = local_sq
    sq_in[row] = local_sq
    pl.semaphore_wait(barrier, rows)

    def sq_copy(k, arrival=False):
        peer, _ = row_peers[k]
        slot = peer[2] if arrival else row
        return pltpu.make_async_remote_copy(
            sq_out, sq_in.at[slot], sq_send.at[k], sq_recv.at[slot],
            device_id=peer, device_id_type=MESH,
        )

    for k in range(rows - 1):
        sq_copy(k).start()
    fetch(1, 2)
    gain_copy.wait()
    for k in reversed(range(rows - 1)):
        sq_copy(k, arrival=True).wait_recv()
    total_sq = sq_in[0]
    for k in range(1, rows):
        total_sq = total_sq + sq_in[k]
    scale_row = lax.rsqrt(total_sq / features + EPS)
    scale = row_to_column(scale_row)
    for k in range(width // LANES):
        at = slice(k * LANES, (k + 1) * LANES)
        x_ref[:, at] = (h_ref[:, at].astype(jnp.float32) * scale * gain_ref[at]).astype(jnp.bfloat16)

    def partner_tile(q, cut=0):
        w_copy(q, False).wait()
        core_out[q, :, cut:] = jnp.dot(x_ref[...], w_partner[q % PAIRS, :, cut:], preferred_element_type=jnp.float32)

        @pl.when(q + PAIRS < partner_count + tiles)
        def _():
            w_copy(q + PAIRS, False).start()

        core_copy(q, cut).start()

    def own_tile(q, total, cut=0):
        w_copy(q, True).wait()
        total[...] = jnp.dot(x_ref[...], w_own[q % PAIRS, :, cut:], preferred_element_type=jnp.float32)

        @pl.when(q + PAIRS < own_count + tiles)
        def _():
            w_copy(q + PAIRS, True).start()

        core_copy(q, cut).wait_recv()
        total[...] += core_in[q, :, cut:]

    def columns(i):
        return pl.ds(pl.multiple_of(i * TILE, TILE), TILE)

    def send_tile(s):
        own_tile(s, chip_out.at[s])

    def keep_tile(s):
        own_tile(s, z_ref.at[:, columns(s - own_count)])

    edge_fetch(0).wait()
    edge_fetch(1).wait()
    for k in range(2):
        at = slice(k * EDGE, (k + 1) * EDGE)
        edge_out[k] = jnp.dot(x_ref[...], w_edge[:, at], preferred_element_type=jnp.float32)
    for k in range(2):
        edge_copy(k).start()
    fetch(2, 4)
    partner_tile(0, EDGE)
    fetch(4, PAIRS)
    partner_tile(1)
    own_tile(0, chip_out.at[0, :, pl.ds(EDGE, TILE - EDGE)], EDGE)
    chip_copy(0, 0, 1, EDGE).start()

    @pl.loop(1, 3)
    def _(s):
        partner_tile(s + 1)
        send_tile(s)

    chip_copy(1, 1, 2).start()

    @pl.loop(2, last_group)
    def _(group):
        @pl.loop(0, GROUP)
        def _(t):
            s = group_start(group) + t
            partner_tile(s + 1)
            send_tile(s)

        chip_copy(group, group_start(group), GROUP).start()

    @pl.loop(tiles - SHIFT, tiles + SHIFT)
    def _(s):
        partner_tile(s + 1)

        @pl.when(core == 1)
        def _():
            send_tile(s)
            chip_copy(last_group + s - tiles + SHIFT, s, 1).start()

        pl.when(core == 0)(lambda: keep_tile(s))

    @pl.loop(tiles + SHIFT, 2 * tiles + SHIFT)
    def _(s):
        pl.when(s + 1 < partner_count + tiles)(lambda: partner_tile(s + 1))
        pl.when(s < own_count + tiles)(lambda: keep_tile(s))

    lane_peak[...] = jnp.full((batch, LANES), -jnp.inf, jnp.float32)
    lane_mass[...] = jnp.zeros((batch, LANES), jnp.float32)

    def finish(place, first, count, edges=None):
        if edges is None:
            chip_arrival(place, first, count).wait_recv()
        else:
            for k in range(2):
                edge_copy(k, arrival=edges + k).wait_recv()
            chip_in[first, :, :EDGE] = edge_in[edges] + edge_in[edges + 1]
            chip_arrival(place, first, count, EDGE).wait_recv()

        @pl.loop(first, first + count)
        def _(i):
            z = z_ref[:, columns(i)] + chip_in[i]
            z_ref[:, columns(i)] = z
            parts = [z[:, k * LANES:(k + 1) * LANES] for k in range(TILE // LANES)]
            peak = lane_peak[...]
            new_peak = functools.reduce(jnp.maximum, parts, peak)
            mass = lane_mass[...] * jnp.exp(peak - new_peak)
            for part in parts:
                mass = mass + jnp.exp(part - new_peak)
            lane_peak[...] = new_peak
            lane_mass[...] = mass

    @pl.when(core == 0)
    def _():
        finish(0, 0, 1, edges=0)
        finish(tail, tiles - 1, 1, edges=2)

    finish(1, 1 - core, 2)

    @pl.loop(2, last_group)
    def _(group):
        finish(group, group_start(group) - core, GROUP)

    @pl.when(core == 1)
    def _():
        for k in range(2 * SHIFT):
            finish(last_group + k, tiles - 2 * SHIFT + k, 1)

    peaks_by_lane, mass_by_lane = lane_peak[...].T, lane_mass[...].T
    peak = jnp.max(peaks_by_lane, axis=0, keepdims=True)
    mass = jnp.sum(mass_by_lane * jnp.exp(peaks_by_lane - peak), axis=0, keepdims=True)
    first = lax.broadcasted_iota(jnp.int32, (2, batch), 0) == 0
    message = jnp.where(first, peak, mass)
    mass_out[...] = message
    mass_in[me] = message

    def mass_copy(k, arrival=False):
        peer, place = peers[k]
        slot = place if arrival else me
        return pltpu.make_async_remote_copy(
            mass_out, mass_in.at[slot], mass_send.at[k], mass_recv.at[slot],
            device_id=peer, device_id_type=MESH,
        )

    everyone = cols * rows
    for k in range(everyone - 1):
        mass_copy(k).start()

    for k in range(rows - 1):
        sq_copy(k).wait_send()

    core_copy(0, EDGE).wait_send()

    @pl.loop(1, partner_count + tiles)
    def _(s):
        core_copy(s).wait_send()

    for k in range(2):
        edge_copy(k).wait_send()
    chip_copy(0, 0, 1, EDGE).wait_send()
    chip_copy(1, 1, 2).wait_send()

    @pl.loop(2, last_group)
    def _(group):
        chip_copy(group, group_start(group), GROUP).wait_send()

    @pl.when(core == 1)
    def _():
        for k in range(2 * SHIFT):
            chip_copy(last_group + k, tiles - SHIFT + k, 1).wait_send()

    for k in reversed(range(everyone - 1)):
        mass_copy(k, arrival=True).wait_recv()
    peaks = [mass_in[d, 0:1] for d in range(everyone)]
    top = functools.reduce(jnp.maximum, peaks)
    total = jnp.zeros_like(top)
    for d in range(everyone):
        total = total + mass_in[d, 1:2] * jnp.exp(peaks[d] - top)
    log_norm = top + jnp.log(total)
    lse_row_ref[...] = log_norm
    lse_col_ref[...] = jnp.broadcast_to(row_to_column(log_norm), (batch, LANES))

    for k in range(everyone - 1):
        mass_copy(k).wait_send()


def subtract_kernel(z_ref, lse_col_ref, lse_row_ref, out_hbm, log_norm_hbm, out_ref, log_norm_ref, sem, log_norm_sem):
    batch, block = z_ref.shape
    log_norm_ref[...] = lse_row_ref[0]
    copies = [pltpu.make_async_copy(log_norm_ref, log_norm_hbm, log_norm_sem)]
    copies[0].start()
    for n in range(batch // SUBLANES):
        at = slice(n * SUBLANES, (n + 1) * SUBLANES)
        lse = lse_col_ref[at]
        for k in range(0, block, LANES):
            out_ref[at, k:k + LANES] = z_ref[at, k:k + LANES] - lse
        rows = pl.ds(n * SUBLANES, SUBLANES)
        copies.append(pltpu.make_async_copy(out_ref.at[rows], out_hbm.at[rows], sem.at[n]))
        copies[-1].start()
    for copy in copies:
        copy.wait()


def solution(mesh):
    cols, rows = mesh.shape["col"], mesh.shape["row"]

    def local_head(hidden, norm_gain, w_head):
        batch, width = hidden.shape
        block = w_head.shape[1] // rows
        tiles = block // TILE
        sizes = (cols, rows, width, block, tiles, width * rows)
        f32 = jnp.float32
        dma = pltpu.SemaphoreType.DMA
        vmem = pl.BlockSpec(memory_space=pltpu.VMEM)
        hbm = pl.BlockSpec(memory_space=pl.ANY)
        z, lse_col, lse_row = pl.pallas_call(
            functools.partial(head_kernel, sizes),
            name="head",
            out_shape=(
                pltpu.VMEM((batch, block), f32),
                pltpu.VMEM((batch, LANES), f32),
                pltpu.VMEM((1, batch), f32),
            ),
            in_specs=[pl.BlockSpec(memory_space=pltpu.HBM)] * 3,
            out_specs=[vmem] * 3,
            scratch_shapes=[
                pltpu.VMEM((batch, width), jnp.bfloat16),
                pltpu.VMEM((width,), f32),
                pltpu.VMEM((batch, width), jnp.bfloat16),
                pltpu.VMEM((PAIRS, width, TILE), jnp.bfloat16),
                pltpu.VMEM((PAIRS, width, TILE), jnp.bfloat16),
                pltpu.VMEM((2 * tiles + SHIFT, batch, TILE), f32),
                pltpu.VMEM((2 * tiles + SHIFT, batch, TILE), f32),
                pltpu.VMEM((tiles + SHIFT, batch, TILE), f32),
                pltpu.VMEM((tiles, batch, TILE), f32),
                pltpu.VMEM((1, batch), f32),
                pltpu.VMEM((rows, 1, batch), f32),
                pltpu.VMEM((2, batch), f32),
                pltpu.VMEM((cols * rows, 2, batch), f32),
                pltpu.VMEM((batch, LANES), f32),
                pltpu.VMEM((batch, LANES), f32),
                pltpu.VMEM((width, 2 * EDGE), jnp.bfloat16),
                pltpu.VMEM((2, batch, EDGE), f32),
                pltpu.VMEM((4, batch, EDGE), f32),
                dma((2,)),
                dma((2,)),
                dma((4,)),
                dma,
                dma,
                dma((PAIRS,)),
                dma((PAIRS,)),
                dma((2 * tiles + SHIFT,)),
                dma((2 * tiles + SHIFT,)),
                dma((tiles + SHIFT,)),
                dma((tiles,)),
                dma((rows,)),
                dma((rows,)),
                dma((cols * rows,)),
                dma((cols * rows,)),
            ],
            compiler_params=pltpu.CompilerParams(
                collective_id=0, has_side_effects=True, vmem_limit_bytes=VMEM_LIMIT
            ),
        )(*(pltpu.with_memory_space_constraint(a, pltpu.HBM) for a in (hidden, norm_gain, w_head)))
        return pl.pallas_call(
            subtract_kernel,
            name="subtract",
            out_shape=(
                jax.ShapeDtypeStruct((batch, block), f32),
                jax.ShapeDtypeStruct((batch,), f32),
            ),
            in_specs=[vmem] * 3,
            out_specs=[hbm] * 2,
            scratch_shapes=[pltpu.VMEM((batch, block), f32), pltpu.VMEM((batch,), f32), dma((batch // SUBLANES,)), dma],
            compiler_params=pltpu.CompilerParams(vmem_limit_bytes=16 * 1024 * 1024),
        )(z, lse_col, lse_row)

    return jax.shard_map(
        local_head,
        mesh=mesh,
        in_specs=(P("dp", "row"), P("row"), P("row", "col")),
        out_specs=(P("dp", ("col", "row")), P("dp")),
        check_vma=False,
    )
```

```python
import functools

import jax
import jax.numpy as jnp
from jax import lax
from jax.experimental import pallas as pl
from jax.experimental.pallas import tpu as pltpu
from jax.sharding import PartitionSpec as P

EPS = 1e-5
MESH = pl.DeviceIdType.MESH
LANES = 128
TILE = 512
PAIRS = 6
GROUP = 4
EDGE = 128
PARTS = 4
SHIFT = 1
SUBLANES = 8
VMEM_LIMIT = 48 * 1024 * 1024


def diagonal(batch):
    shape = (batch, batch)
    return lax.broadcasted_iota(jnp.int32, shape, 0) == lax.broadcasted_iota(jnp.int32, shape, 1)


def column_to_row(column):
    batch = column.shape[0]
    return jnp.sum(jnp.where(diagonal(batch), column, 0.0), axis=0, keepdims=True)


def row_to_column(row):
    return jnp.sum(jnp.where(diagonal(row.shape[1]), row, 0.0), axis=1, keepdims=True)


def head_kernel(
    sizes,
    hidden_hbm,
    gain_hbm,
    w_hbm,
    z_ref,
    lse_col_ref,
    lse_row_ref,
    h_ref,
    gain_ref,
    x_ref,
    w_own,
    w_partner,
    core_out,
    core_in,
    chip_out,
    chip_in,
    sq_out,
    sq_in,
    mass_out,
    mass_in,
    lane_peak,
    lane_mass,
    w_edge,
    edge_out,
    edge_in,
    edge_sem,
    edge_send,
    edge_recv,
    h_sem,
    gain_sem,
    w_own_sem,
    w_partner_sem,
    core_send,
    core_recv,
    chip_send,
    chip_recv,
    sq_send,
    sq_recv,
    mass_send,
    mass_recv,
):
    cols, rows, width, block, tiles, features = sizes
    dp, col, row = lax.axis_index("dp"), lax.axis_index("col"), lax.axis_index("row")
    chip, core = row // 2, row % 2
    batch = h_ref.shape[0]

    def device(flip_col, flip_chip, flip_core):
        c = 1 - col if flip_col else col
        r = (1 - chip if flip_chip else chip) * 2 + (1 - core if flip_core else core)
        return (dp, c, r), c * rows + r

    me = device(0, 0, 0)[1]
    row_peers = [device(0, 1, 1), device(0, 1, 0), device(0, 0, 1)]
    mirror = device(1, 0, 0)
    peers = [device(1, 1, 1), device(1, 1, 0), device(1, 0, 1), mirror, *row_peers]
    partner = row_peers[2][0]

    own_count = tiles - SHIFT + core * 2 * SHIFT
    partner_count = 2 * tiles - own_count

    def w_copy(s, own):
        count = own_count if own else partner_count
        side = core if own else 1 - core
        late = jnp.where(s < count, 0, 1)
        tile = (1 - late) * (side * (tiles - SHIFT) + s) + late * (side * tiles + s - count)
        start = (late * chip + (1 - late) * (1 - chip)) * 2 * block + tile * TILE
        buf, sem = (w_own, w_own_sem) if own else (w_partner, w_partner_sem)
        slot = s % PAIRS
        return pltpu.make_async_copy(
            w_hbm.at[:, pl.ds(pl.multiple_of(start, TILE), TILE)], buf.at[slot], sem.at[slot]
        )

    def core_copy(s, cut=0):
        at = pl.ds(cut, TILE - cut)
        return pltpu.make_async_remote_copy(
            core_out.at[s, :, at], core_in.at[s, :, at], core_send.at[s], core_recv.at[s],
            device_id=partner, device_id_type=MESH,
        )

    def chip_copy(group, s, count, cut=0):
        at = pl.ds(cut, TILE - cut)
        tile = core * (tiles - SHIFT) + s
        place = core * tail if isinstance(group, int) and group == 0 else group
        return pltpu.make_async_remote_copy(
            chip_out.at[pl.ds(s, count), :, at], chip_in.at[pl.ds(tile % tiles, count), :, at],
            chip_send.at[group], chip_recv.at[place],
            device_id=(dp, col, (1 - chip) * 2 + tile // tiles), device_id_type=MESH,
        )

    def chip_arrival(place, first, count, cut=0):
        at = pl.ds(cut, TILE - cut)
        return pltpu.make_async_remote_copy(
            chip_out.at[pl.ds(0, count), :, at], chip_in.at[pl.ds(first, count), :, at],
            chip_send.at[0], chip_recv.at[place],
            device_id=row_peers[1][0], device_id_type=MESH,
        )

    def edge_start(own):
        side = core if own else 1 - core
        start = (1 - chip) * 2 * block + side * (tiles - SHIFT) * TILE
        return pl.ds(pl.multiple_of(start, TILE), EDGE)

    def edge_fetch(k):
        return pltpu.make_async_copy(
            w_hbm.at[:, edge_start(k == 0)], w_edge.at[:, pl.ds(k * EDGE, EDGE)], edge_sem.at[k]
        )

    def edge_copy(k, arrival=None):
        place = arrival if arrival is not None else 2 * core if k == 0 else 3 - 2 * core
        return pltpu.make_async_remote_copy(
            edge_out.at[k], edge_in.at[place], edge_send.at[k], edge_recv.at[place],
            device_id=(dp, col, (1 - chip) * 2), device_id_type=MESH,
        )

    def group_start(group):
        return (group - 2) * GROUP + 3

    last_group = 2 + (tiles - SHIFT - 3) // GROUP
    tail = last_group + 1

    h_copies = []
    for k in range(PARTS):
        rows_k = pl.ds(k * batch // PARTS, batch // PARTS)
        h_copies.append(pltpu.make_async_copy(hidden_hbm.at[rows_k], h_ref.at[rows_k], h_sem.at[k]))
    gain_copy = pltpu.make_async_copy(gain_hbm, gain_ref, gain_sem)
    for copy in h_copies:
        copy.start()
    gain_copy.start()

    barrier = pltpu.get_barrier_semaphore()
    for peer, _ in [mirror, *row_peers]:
        pl.semaphore_signal(barrier, inc=1, device_id=peer, device_id_type=MESH)

    def fetch(first, last):
        @pl.loop(first, last)
        def _(q):
            w_copy(q, False).start()
            w_copy(q, True).start()


    edge_fetch(0).start()
    edge_fetch(1).start()
    fetch(0, 1)

    for copy in h_copies:
        copy.wait()
    squares = jnp.zeros((batch, LANES), jnp.float32)
    for k in range(width // LANES):
        part = h_ref[:, k * LANES:(k + 1) * LANES].astype(jnp.float32)
        squares = squares + part * part
    local_sq = column_to_row(jnp.sum(squares, axis=1, keepdims=True))
    sq_out[...] = local_sq
    sq_in[row] = local_sq
    pl.semaphore_wait(barrier, rows)

    def sq_copy(k, arrival=False):
        peer, _ = row_peers[k]
        slot = peer[2] if arrival else row
        return pltpu.make_async_remote_copy(
            sq_out, sq_in.at[slot], sq_send.at[k], sq_recv.at[slot],
            device_id=peer, device_id_type=MESH,
        )

    for k in range(rows - 1):
        sq_copy(k).start()
    fetch(1, 2)
    gain_copy.wait()
    for k in reversed(range(rows - 1)):
        sq_copy(k, arrival=True).wait_recv()
    total_sq = sq_in[0]
    for k in range(1, rows):
        total_sq = total_sq + sq_in[k]
    scale_row = lax.rsqrt(total_sq / features + EPS)
    scale = row_to_column(scale_row)
    for k in range(width // LANES):
        at = slice(k * LANES, (k + 1) * LANES)
        x_ref[:, at] = (h_ref[:, at].astype(jnp.float32) * scale * gain_ref[at]).astype(jnp.bfloat16)

    def partner_tile(q, cut=0):
        w_copy(q, False).wait()
        core_out[q, :, cut:] = jnp.dot(x_ref[...], w_partner[q % PAIRS, :, cut:], preferred_element_type=jnp.float32)

        @pl.when(q + PAIRS < partner_count + tiles)
        def _():
            w_copy(q + PAIRS, False).start()

        core_copy(q, cut).start()

    def own_tile(q, total, cut=0):
        w_copy(q, True).wait()
        total[...] = jnp.dot(x_ref[...], w_own[q % PAIRS, :, cut:], preferred_element_type=jnp.float32)

        @pl.when(q + PAIRS < own_count + tiles)
        def _():
            w_copy(q + PAIRS, True).start()

        core_copy(q, cut).wait_recv()
        total[...] += core_in[q, :, cut:]

    def columns(i):
        return pl.ds(pl.multiple_of(i * TILE, TILE), TILE)

    def send_tile(s):
        own_tile(s, chip_out.at[s])

    def keep_tile(s):
        own_tile(s, z_ref.at[:, columns(s - own_count)])

    edge_fetch(0).wait()
    edge_fetch(1).wait()
    for k in range(2):
        at = slice(k * EDGE, (k + 1) * EDGE)
        edge_out[k] = jnp.dot(x_ref[...], w_edge[:, at], preferred_element_type=jnp.float32)
    for k in range(2):
        edge_copy(k).start()
    partner_tile(0, EDGE)
    fetch(2, PAIRS)
    partner_tile(1)
    own_tile(0, chip_out.at[0, :, pl.ds(EDGE, TILE - EDGE)], EDGE)
    chip_copy(0, 0, 1, EDGE).start()

    @pl.loop(1, 3)
    def _(s):
        partner_tile(s + 1)
        send_tile(s)

    chip_copy(1, 1, 2).start()

    @pl.loop(2, last_group)
    def _(group):
        @pl.loop(0, GROUP)
        def _(t):
            s = group_start(group) + t
            partner_tile(s + 1)
            send_tile(s)

        chip_copy(group, group_start(group), GROUP).start()

    @pl.loop(tiles - SHIFT, tiles + SHIFT)
    def _(s):
        partner_tile(s + 1)

        @pl.when(core == 1)
        def _():
            send_tile(s)
            chip_copy(last_group + s - tiles + SHIFT, s, 1).start()

        pl.when(core == 0)(lambda: keep_tile(s))

    @pl.loop(tiles + SHIFT, 2 * tiles + SHIFT)
    def _(s):
        pl.when(s + 1 < partner_count + tiles)(lambda: partner_tile(s + 1))
        pl.when(s < own_count + tiles)(lambda: keep_tile(s))

    lane_peak[...] = jnp.full((batch, LANES), -jnp.inf, jnp.float32)
    lane_mass[...] = jnp.zeros((batch, LANES), jnp.float32)

    def finish(place, first, count, edges=None):
        if edges is None:
            chip_arrival(place, first, count).wait_recv()
        else:
            for k in range(2):
                edge_copy(k, arrival=edges + k).wait_recv()
            chip_in[first, :, :EDGE] = edge_in[edges] + edge_in[edges + 1]
            chip_arrival(place, first, count, EDGE).wait_recv()

        @pl.loop(first, first + count)
        def _(i):
            z = z_ref[:, columns(i)] + chip_in[i]
            z_ref[:, columns(i)] = z
            parts = [z[:, k * LANES:(k + 1) * LANES] for k in range(TILE // LANES)]
            peak = lane_peak[...]
            new_peak = functools.reduce(jnp.maximum, parts, peak)
            mass = lane_mass[...] * jnp.exp(peak - new_peak)
            for part in parts:
                mass = mass + jnp.exp(part - new_peak)
            lane_peak[...] = new_peak
            lane_mass[...] = mass

    @pl.when(core == 0)
    def _():
        finish(0, 0, 1, edges=0)
        finish(tail, tiles - 1, 1, edges=2)

    finish(1, 1 - core, 2)

    @pl.loop(2, last_group)
    def _(group):
        finish(group, group_start(group) - core, GROUP)

    @pl.when(core == 1)
    def _():
        for k in range(2 * SHIFT):
            finish(last_group + k, tiles - 2 * SHIFT + k, 1)

    peaks_by_lane, mass_by_lane = lane_peak[...].T, lane_mass[...].T
    peak = jnp.max(peaks_by_lane, axis=0, keepdims=True)
    mass = jnp.sum(mass_by_lane * jnp.exp(peaks_by_lane - peak), axis=0, keepdims=True)
    first = lax.broadcasted_iota(jnp.int32, (2, batch), 0) == 0
    message = jnp.where(first, peak, mass)
    mass_out[...] = message
    mass_in[me] = message

    def mass_copy(k, arrival=False):
        peer, place = peers[k]
        slot = place if arrival else me
        return pltpu.make_async_remote_copy(
            mass_out, mass_in.at[slot], mass_send.at[k], mass_recv.at[slot],
            device_id=peer, device_id_type=MESH,
        )

    everyone = cols * rows
    for k in range(everyone - 1):
        mass_copy(k).start()

    for k in range(rows - 1):
        sq_copy(k).wait_send()

    core_copy(0, EDGE).wait_send()

    @pl.loop(1, partner_count + tiles)
    def _(s):
        core_copy(s).wait_send()

    for k in range(2):
        edge_copy(k).wait_send()
    chip_copy(0, 0, 1, EDGE).wait_send()
    chip_copy(1, 1, 2).wait_send()

    @pl.loop(2, last_group)
    def _(group):
        chip_copy(group, group_start(group), GROUP).wait_send()

    @pl.when(core == 1)
    def _():
        for k in range(2 * SHIFT):
            chip_copy(last_group + k, tiles - SHIFT + k, 1).wait_send()

    for k in reversed(range(everyone - 1)):
        mass_copy(k, arrival=True).wait_recv()
    peaks = [mass_in[d, 0:1] for d in range(everyone)]
    top = functools.reduce(jnp.maximum, peaks)
    total = jnp.zeros_like(top)
    for d in range(everyone):
        total = total + mass_in[d, 1:2] * jnp.exp(peaks[d] - top)
    log_norm = top + jnp.log(total)
    lse_row_ref[...] = log_norm
    lse_col_ref[...] = jnp.broadcast_to(row_to_column(log_norm), (batch, LANES))

    for k in range(everyone - 1):
        mass_copy(k).wait_send()


def subtract_kernel(z_ref, lse_col_ref, lse_row_ref, out_hbm, log_norm_hbm, out_ref, log_norm_ref, sem, log_norm_sem):
    batch, block = z_ref.shape
    log_norm_ref[...] = lse_row_ref[0]
    copies = [pltpu.make_async_copy(log_norm_ref, log_norm_hbm, log_norm_sem)]
    copies[0].start()
    for n in range(batch // SUBLANES):
        at = slice(n * SUBLANES, (n + 1) * SUBLANES)
        lse = lse_col_ref[at]
        for k in range(0, block, LANES):
            out_ref[at, k:k + LANES] = z_ref[at, k:k + LANES] - lse
        rows = pl.ds(n * SUBLANES, SUBLANES)
        copies.append(pltpu.make_async_copy(out_ref.at[rows], out_hbm.at[rows], sem.at[n]))
        copies[-1].start()
    for copy in copies:
        copy.wait()


def solution(mesh):
    cols, rows = mesh.shape["col"], mesh.shape["row"]

    def local_head(hidden, norm_gain, w_head):
        batch, width = hidden.shape
        block = w_head.shape[1] // rows
        tiles = block // TILE
        sizes = (cols, rows, width, block, tiles, width * rows)
        f32 = jnp.float32
        dma = pltpu.SemaphoreType.DMA
        vmem = pl.BlockSpec(memory_space=pltpu.VMEM)
        hbm = pl.BlockSpec(memory_space=pl.ANY)
        z, lse_col, lse_row = pl.pallas_call(
            functools.partial(head_kernel, sizes),
            name="head",
            out_shape=(
                pltpu.VMEM((batch, block), f32),
                pltpu.VMEM((batch, LANES), f32),
                pltpu.VMEM((1, batch), f32),
            ),
            in_specs=[pl.BlockSpec(memory_space=pltpu.HBM)] * 3,
            out_specs=[vmem] * 3,
            scratch_shapes=[
                pltpu.VMEM((batch, width), jnp.bfloat16),
                pltpu.VMEM((width,), f32),
                pltpu.VMEM((batch, width), jnp.bfloat16),
                pltpu.VMEM((PAIRS, width, TILE), jnp.bfloat16),
                pltpu.VMEM((PAIRS, width, TILE), jnp.bfloat16),
                pltpu.VMEM((2 * tiles + SHIFT, batch, TILE), f32),
                pltpu.VMEM((2 * tiles + SHIFT, batch, TILE), f32),
                pltpu.VMEM((tiles + SHIFT, batch, TILE), f32),
                pltpu.VMEM((tiles, batch, TILE), f32),
                pltpu.VMEM((1, batch), f32),
                pltpu.VMEM((rows, 1, batch), f32),
                pltpu.VMEM((2, batch), f32),
                pltpu.VMEM((cols * rows, 2, batch), f32),
                pltpu.VMEM((batch, LANES), f32),
                pltpu.VMEM((batch, LANES), f32),
                pltpu.VMEM((width, 2 * EDGE), jnp.bfloat16),
                pltpu.VMEM((2, batch, EDGE), f32),
                pltpu.VMEM((4, batch, EDGE), f32),
                dma((2,)),
                dma((2,)),
                dma((4,)),
                dma((PARTS,)),
                dma,
                dma((PAIRS,)),
                dma((PAIRS,)),
                dma((2 * tiles + SHIFT,)),
                dma((2 * tiles + SHIFT,)),
                dma((tiles + SHIFT,)),
                dma((tiles,)),
                dma((rows,)),
                dma((rows,)),
                dma((cols * rows,)),
                dma((cols * rows,)),
            ],
            compiler_params=pltpu.CompilerParams(
                collective_id=0, has_side_effects=True, vmem_limit_bytes=VMEM_LIMIT
            ),
        )(*(pltpu.with_memory_space_constraint(a, pltpu.HBM) for a in (hidden, norm_gain, w_head)))
        return pl.pallas_call(
            subtract_kernel,
            name="subtract",
            out_shape=(
                jax.ShapeDtypeStruct((batch, block), f32),
                jax.ShapeDtypeStruct((batch,), f32),
            ),
            in_specs=[vmem] * 3,
            out_specs=[hbm] * 2,
            scratch_shapes=[pltpu.VMEM((batch, block), f32), pltpu.VMEM((batch,), f32), dma((batch // SUBLANES,)), dma],
            compiler_params=pltpu.CompilerParams(vmem_limit_bytes=16 * 1024 * 1024),
        )(z, lse_col, lse_row)

    return jax.shard_map(
        local_head,
        mesh=mesh,
        in_specs=(P("dp", "row"), P("row"), P("row", "col")),
        out_specs=(P("dp", ("col", "row")), P("dp")),
        check_vma=False,
    )
```

```python
import functools

import jax
import jax.numpy as jnp
from jax import lax
from jax.experimental import pallas as pl
from jax.experimental.pallas import tpu as pltpu
from jax.sharding import PartitionSpec as P

EPS = 1e-5
MESH = pl.DeviceIdType.MESH
LANES = 128
TILE = 512
PAIRS = 6
GROUP = 4
EDGE = 128
PARTS = 4
SHIFT = 1
SUBLANES = 8
VMEM_LIMIT = 48 * 1024 * 1024


def diagonal(batch):
    shape = (batch, batch)
    return lax.broadcasted_iota(jnp.int32, shape, 0) == lax.broadcasted_iota(jnp.int32, shape, 1)


def column_to_row(column):
    batch = column.shape[0]
    return jnp.sum(jnp.where(diagonal(batch), column, 0.0), axis=0, keepdims=True)


def row_to_column(row):
    return jnp.sum(jnp.where(diagonal(row.shape[1]), row, 0.0), axis=1, keepdims=True)


def head_kernel(
    sizes,
    hidden_hbm,
    gain_hbm,
    w_hbm,
    z_ref,
    lse_col_ref,
    lse_row_ref,
    h_ref,
    gain_ref,
    x_ref,
    w_own,
    w_partner,
    core_out,
    core_in,
    chip_out,
    chip_in,
    sq_out,
    sq_in,
    mass_out,
    mass_in,
    lane_peak,
    lane_mass,
    w_edge,
    edge_out,
    edge_in,
    edge_sem,
    edge_send,
    edge_recv,
    h_sem,
    gain_sem,
    w_own_sem,
    w_partner_sem,
    core_send,
    core_recv,
    chip_send,
    chip_recv,
    sq_send,
    sq_recv,
    mass_send,
    mass_recv,
):
    cols, rows, width, block, tiles, features = sizes
    dp, col, row = lax.axis_index("dp"), lax.axis_index("col"), lax.axis_index("row")
    chip, core = row // 2, row % 2
    batch = h_ref.shape[0]

    def device(flip_col, flip_chip, flip_core):
        c = 1 - col if flip_col else col
        r = (1 - chip if flip_chip else chip) * 2 + (1 - core if flip_core else core)
        return (dp, c, r), c * rows + r

    me = device(0, 0, 0)[1]
    row_peers = [device(0, 1, 1), device(0, 1, 0), device(0, 0, 1)]
    mirror = device(1, 0, 0)
    peers = [device(1, 1, 1), device(1, 1, 0), device(1, 0, 1), mirror, *row_peers]
    partner = row_peers[2][0]

    own_count = tiles - SHIFT + core * 2 * SHIFT
    partner_count = 2 * tiles - own_count

    def w_copy(s, own, part=None):
        count = own_count if own else partner_count
        side = core if own else 1 - core
        late = jnp.where(s < count, 0, 1)
        tile = (1 - late) * (side * (tiles - SHIFT) + s) + late * (side * tiles + s - count)
        start = (late * chip + (1 - late) * (1 - chip)) * 2 * block + tile * TILE
        buf, sem = (w_own, w_own_sem) if own else (w_partner, w_partner_sem)
        slot = s % PAIRS
        at = pl.ds(0, width) if part is None else pl.ds(part * width // PARTS, width // PARTS)
        return pltpu.make_async_copy(
            w_hbm.at[at, pl.ds(pl.multiple_of(start, TILE), TILE)], buf.at[slot, at], sem.at[slot]
        )

    def w_fetch(s, own):
        for part in range(PARTS):
            w_copy(s, own, part).start()

    def core_copy(s, cut=0):
        at = pl.ds(cut, TILE - cut)
        return pltpu.make_async_remote_copy(
            core_out.at[s, :, at], core_in.at[s, :, at], core_send.at[s], core_recv.at[s],
            device_id=partner, device_id_type=MESH,
        )

    def chip_copy(group, s, count, cut=0):
        at = pl.ds(cut, TILE - cut)
        tile = core * (tiles - SHIFT) + s
        place = core * tail if isinstance(group, int) and group == 0 else group
        return pltpu.make_async_remote_copy(
            chip_out.at[pl.ds(s, count), :, at], chip_in.at[pl.ds(tile % tiles, count), :, at],
            chip_send.at[group], chip_recv.at[place],
            device_id=(dp, col, (1 - chip) * 2 + tile // tiles), device_id_type=MESH,
        )

    def chip_arrival(place, first, count, cut=0):
        at = pl.ds(cut, TILE - cut)
        return pltpu.make_async_remote_copy(
            chip_out.at[pl.ds(0, count), :, at], chip_in.at[pl.ds(first, count), :, at],
            chip_send.at[0], chip_recv.at[place],
            device_id=row_peers[1][0], device_id_type=MESH,
        )

    def edge_start(own):
        side = core if own else 1 - core
        start = (1 - chip) * 2 * block + side * (tiles - SHIFT) * TILE
        return pl.ds(pl.multiple_of(start, TILE), EDGE)

    def edge_fetch(k):
        return pltpu.make_async_copy(
            w_hbm.at[:, edge_start(k == 0)], w_edge.at[:, pl.ds(k * EDGE, EDGE)], edge_sem.at[k]
        )

    def edge_copy(k, arrival=None):
        place = arrival if arrival is not None else 2 * core if k == 0 else 3 - 2 * core
        return pltpu.make_async_remote_copy(
            edge_out.at[k], edge_in.at[place], edge_send.at[k], edge_recv.at[place],
            device_id=(dp, col, (1 - chip) * 2), device_id_type=MESH,
        )

    def group_start(group):
        return (group - 2) * GROUP + 3

    last_group = 2 + (tiles - SHIFT - 3) // GROUP
    tail = last_group + 1

    h_copies = []
    for k in range(PARTS):
        rows_k = pl.ds(k * batch // PARTS, batch // PARTS)
        h_copies.append(pltpu.make_async_copy(hidden_hbm.at[rows_k], h_ref.at[rows_k], h_sem.at[k]))
    gain_copy = pltpu.make_async_copy(gain_hbm, gain_ref, gain_sem)
    for copy in h_copies:
        copy.start()
    gain_copy.start()

    barrier = pltpu.get_barrier_semaphore()
    for peer, _ in [mirror, *row_peers]:
        pl.semaphore_signal(barrier, inc=1, device_id=peer, device_id_type=MESH)

    def fetch(first, last):
        @pl.loop(first, last)
        def _(q):
            w_fetch(q, False)
            w_fetch(q, True)


    edge_fetch(0).start()
    edge_fetch(1).start()
    fetch(0, 1)

    for copy in h_copies:
        copy.wait()
    squares = jnp.zeros((batch, LANES), jnp.float32)
    for k in range(width // LANES):
        part = h_ref[:, k * LANES:(k + 1) * LANES].astype(jnp.float32)
        squares = squares + part * part
    local_sq = column_to_row(jnp.sum(squares, axis=1, keepdims=True))
    sq_out[...] = local_sq
    sq_in[row] = local_sq
    pl.semaphore_wait(barrier, rows)

    def sq_copy(k, arrival=False):
        peer, _ = row_peers[k]
        slot = peer[2] if arrival else row
        return pltpu.make_async_remote_copy(
            sq_out, sq_in.at[slot], sq_send.at[k], sq_recv.at[slot],
            device_id=peer, device_id_type=MESH,
        )

    for k in range(rows - 1):
        sq_copy(k).start()
    fetch(1, 3)
    gain_copy.wait()
    for k in reversed(range(rows - 1)):
        sq_copy(k, arrival=True).wait_recv()
    total_sq = sq_in[0]
    for k in range(1, rows):
        total_sq = total_sq + sq_in[k]
    scale_row = lax.rsqrt(total_sq / features + EPS)
    scale = row_to_column(scale_row)
    for k in range(width // LANES):
        at = slice(k * LANES, (k + 1) * LANES)
        x_ref[:, at] = (h_ref[:, at].astype(jnp.float32) * scale * gain_ref[at]).astype(jnp.bfloat16)

    def partner_tile(q, cut=0):
        w_copy(q, False).wait()
        core_out[q, :, cut:] = jnp.dot(x_ref[...], w_partner[q % PAIRS, :, cut:], preferred_element_type=jnp.float32)

        @pl.when(q + PAIRS < partner_count + tiles)
        def _():
            w_fetch(q + PAIRS, False)

        core_copy(q, cut).start()

    def own_tile(q, total, cut=0):
        w_copy(q, True).wait()
        total[...] = jnp.dot(x_ref[...], w_own[q % PAIRS, :, cut:], preferred_element_type=jnp.float32)

        @pl.when(q + PAIRS < own_count + tiles)
        def _():
            w_fetch(q + PAIRS, True)

        core_copy(q, cut).wait_recv()
        total[...] += core_in[q, :, cut:]

    def columns(i):
        return pl.ds(pl.multiple_of(i * TILE, TILE), TILE)

    def send_tile(s):
        own_tile(s, chip_out.at[s])

    def keep_tile(s):
        own_tile(s, z_ref.at[:, columns(s - own_count)])

    edge_fetch(0).wait()
    edge_fetch(1).wait()
    for k in range(2):
        at = slice(k * EDGE, (k + 1) * EDGE)
        edge_out[k] = jnp.dot(x_ref[...], w_edge[:, at], preferred_element_type=jnp.float32)
    for k in range(2):
        edge_copy(k).start()
    partner_tile(0, EDGE)
    fetch(3, PAIRS)
    partner_tile(1)
    own_tile(0, chip_out.at[0, :, pl.ds(EDGE, TILE - EDGE)], EDGE)
    chip_copy(0, 0, 1, EDGE).start()

    @pl.loop(1, 3)
    def _(s):
        partner_tile(s + 1)
        send_tile(s)

    chip_copy(1, 1, 2).start()

    @pl.loop(2, last_group)
    def _(group):
        @pl.loop(0, GROUP)
        def _(t):
            s = group_start(group) + t
            partner_tile(s + 1)
            send_tile(s)

        chip_copy(group, group_start(group), GROUP).start()

    @pl.loop(tiles - SHIFT, tiles + SHIFT)
    def _(s):
        partner_tile(s + 1)

        @pl.when(core == 1)
        def _():
            send_tile(s)
            chip_copy(last_group + s - tiles + SHIFT, s, 1).start()

        pl.when(core == 0)(lambda: keep_tile(s))

    @pl.loop(tiles + SHIFT, 2 * tiles + SHIFT)
    def _(s):
        pl.when(s + 1 < partner_count + tiles)(lambda: partner_tile(s + 1))
        pl.when(s < own_count + tiles)(lambda: keep_tile(s))

    lane_peak[...] = jnp.full((batch, LANES), -jnp.inf, jnp.float32)
    lane_mass[...] = jnp.zeros((batch, LANES), jnp.float32)

    def finish(place, first, count, edges=None):
        if edges is None:
            chip_arrival(place, first, count).wait_recv()
        else:
            for k in range(2):
                edge_copy(k, arrival=edges + k).wait_recv()
            chip_in[first, :, :EDGE] = edge_in[edges] + edge_in[edges + 1]
            chip_arrival(place, first, count, EDGE).wait_recv()

        @pl.loop(first, first + count)
        def _(i):
            z = z_ref[:, columns(i)] + chip_in[i]
            z_ref[:, columns(i)] = z
            parts = [z[:, k * LANES:(k + 1) * LANES] for k in range(TILE // LANES)]
            peak = lane_peak[...]
            new_peak = functools.reduce(jnp.maximum, parts, peak)
            mass = lane_mass[...] * jnp.exp(peak - new_peak)
            for part in parts:
                mass = mass + jnp.exp(part - new_peak)
            lane_peak[...] = new_peak
            lane_mass[...] = mass

    @pl.when(core == 0)
    def _():
        finish(0, 0, 1, edges=0)
        finish(tail, tiles - 1, 1, edges=2)

    finish(1, 1 - core, 2)

    @pl.loop(2, last_group)
    def _(group):
        finish(group, group_start(group) - core, GROUP)

    @pl.when(core == 1)
    def _():
        for k in range(2 * SHIFT):
            finish(last_group + k, tiles - 2 * SHIFT + k, 1)

    peaks_by_lane, mass_by_lane = lane_peak[...].T, lane_mass[...].T
    peak = jnp.max(peaks_by_lane, axis=0, keepdims=True)
    mass = jnp.sum(mass_by_lane * jnp.exp(peaks_by_lane - peak), axis=0, keepdims=True)
    first = lax.broadcasted_iota(jnp.int32, (2, batch), 0) == 0
    message = jnp.where(first, peak, mass)
    mass_out[...] = message
    mass_in[me] = message

    def mass_copy(k, arrival=False):
        peer, place = peers[k]
        slot = place if arrival else me
        return pltpu.make_async_remote_copy(
            mass_out, mass_in.at[slot], mass_send.at[k], mass_recv.at[slot],
            device_id=peer, device_id_type=MESH,
        )

    everyone = cols * rows
    for k in range(everyone - 1):
        mass_copy(k).start()

    for k in range(rows - 1):
        sq_copy(k).wait_send()

    core_copy(0, EDGE).wait_send()

    @pl.loop(1, partner_count + tiles)
    def _(s):
        core_copy(s).wait_send()

    for k in range(2):
        edge_copy(k).wait_send()
    chip_copy(0, 0, 1, EDGE).wait_send()
    chip_copy(1, 1, 2).wait_send()

    @pl.loop(2, last_group)
    def _(group):
        chip_copy(group, group_start(group), GROUP).wait_send()

    @pl.when(core == 1)
    def _():
        for k in range(2 * SHIFT):
            chip_copy(last_group + k, tiles - SHIFT + k, 1).wait_send()

    for k in reversed(range(everyone - 1)):
        mass_copy(k, arrival=True).wait_recv()
    peaks = [mass_in[d, 0:1] for d in range(everyone)]
    top = functools.reduce(jnp.maximum, peaks)
    total = jnp.zeros_like(top)
    for d in range(everyone):
        total = total + mass_in[d, 1:2] * jnp.exp(peaks[d] - top)
    log_norm = top + jnp.log(total)
    lse_row_ref[...] = log_norm
    lse_col_ref[...] = jnp.broadcast_to(row_to_column(log_norm), (batch, LANES))

    for k in range(everyone - 1):
        mass_copy(k).wait_send()


def subtract_kernel(z_ref, lse_col_ref, lse_row_ref, out_hbm, log_norm_hbm, out_ref, log_norm_ref, sem, log_norm_sem):
    batch, block = z_ref.shape
    log_norm_ref[...] = lse_row_ref[0]
    copies = [pltpu.make_async_copy(log_norm_ref, log_norm_hbm, log_norm_sem)]
    copies[0].start()
    for n in range(batch // SUBLANES):
        at = slice(n * SUBLANES, (n + 1) * SUBLANES)
        lse = lse_col_ref[at]
        for half in range(2):
            first = half * block // 2
            for k in range(first, first + block // 2, LANES):
                out_ref[at, k:k + LANES] = z_ref[at, k:k + LANES] - lse
            place = (pl.ds(n * SUBLANES, SUBLANES), pl.ds(first, block // 2))
            copies.append(pltpu.make_async_copy(out_ref.at[place], out_hbm.at[place], sem.at[2 * n + half]))
            copies[-1].start()
    for copy in copies:
        copy.wait()


def solution(mesh):
    cols, rows = mesh.shape["col"], mesh.shape["row"]

    def local_head(hidden, norm_gain, w_head):
        batch, width = hidden.shape
        block = w_head.shape[1] // rows
        tiles = block // TILE
        sizes = (cols, rows, width, block, tiles, width * rows)
        f32 = jnp.float32
        dma = pltpu.SemaphoreType.DMA
        vmem = pl.BlockSpec(memory_space=pltpu.VMEM)
        hbm = pl.BlockSpec(memory_space=pl.ANY)
        z, lse_col, lse_row = pl.pallas_call(
            functools.partial(head_kernel, sizes),
            name="head",
            out_shape=(
                pltpu.VMEM((batch, block), f32),
                pltpu.VMEM((batch, LANES), f32),
                pltpu.VMEM((1, batch), f32),
            ),
            in_specs=[pl.BlockSpec(memory_space=pltpu.HBM)] * 3,
            out_specs=[vmem] * 3,
            scratch_shapes=[
                pltpu.VMEM((batch, width), jnp.bfloat16),
                pltpu.VMEM((width,), f32),
                pltpu.VMEM((batch, width), jnp.bfloat16),
                pltpu.VMEM((PAIRS, width, TILE), jnp.bfloat16),
                pltpu.VMEM((PAIRS, width, TILE), jnp.bfloat16),
                pltpu.VMEM((2 * tiles + SHIFT, batch, TILE), f32),
                pltpu.VMEM((2 * tiles + SHIFT, batch, TILE), f32),
                pltpu.VMEM((tiles + SHIFT, batch, TILE), f32),
                pltpu.VMEM((tiles, batch, TILE), f32),
                pltpu.VMEM((1, batch), f32),
                pltpu.VMEM((rows, 1, batch), f32),
                pltpu.VMEM((2, batch), f32),
                pltpu.VMEM((cols * rows, 2, batch), f32),
                pltpu.VMEM((batch, LANES), f32),
                pltpu.VMEM((batch, LANES), f32),
                pltpu.VMEM((width, 2 * EDGE), jnp.bfloat16),
                pltpu.VMEM((2, batch, EDGE), f32),
                pltpu.VMEM((4, batch, EDGE), f32),
                dma((2,)),
                dma((2,)),
                dma((4,)),
                dma((PARTS,)),
                dma,
                dma((PAIRS,)),
                dma((PAIRS,)),
                dma((2 * tiles + SHIFT,)),
                dma((2 * tiles + SHIFT,)),
                dma((tiles + SHIFT,)),
                dma((tiles,)),
                dma((rows,)),
                dma((rows,)),
                dma((cols * rows,)),
                dma((cols * rows,)),
            ],
            compiler_params=pltpu.CompilerParams(
                collective_id=0, has_side_effects=True, vmem_limit_bytes=VMEM_LIMIT
            ),
        )(*(pltpu.with_memory_space_constraint(a, pltpu.HBM) for a in (hidden, norm_gain, w_head)))
        return pl.pallas_call(
            subtract_kernel,
            name="subtract",
            out_shape=(
                jax.ShapeDtypeStruct((batch, block), f32),
                jax.ShapeDtypeStruct((batch,), f32),
            ),
            in_specs=[vmem] * 3,
            out_specs=[hbm] * 2,
            scratch_shapes=[pltpu.VMEM((batch, block), f32), pltpu.VMEM((batch,), f32), dma((2 * batch // SUBLANES,)), dma],
            compiler_params=pltpu.CompilerParams(vmem_limit_bytes=16 * 1024 * 1024),
        )(z, lse_col, lse_row)

    return jax.shard_map(
        local_head,
        mesh=mesh,
        in_specs=(P("dp", "row"), P("row"), P("row", "col")),
        out_specs=(P("dp", ("col", "row")), P("dp")),
        check_vma=False,
    )
```

```python
import functools

import jax
import jax.numpy as jnp
from jax import lax
from jax.experimental import pallas as pl
from jax.experimental.pallas import tpu as pltpu
from jax.sharding import PartitionSpec as P

EPS = 1e-5
MESH = pl.DeviceIdType.MESH
LANES = 128
TILE = 512
PAIRS = 6
GROUP = 4
EDGE = 128
PARTS = 8
SHIFT = 1
SUBLANES = 8
VMEM_LIMIT = 48 * 1024 * 1024


def diagonal(batch):
    shape = (batch, batch)
    return lax.broadcasted_iota(jnp.int32, shape, 0) == lax.broadcasted_iota(jnp.int32, shape, 1)


def column_to_row(column):
    batch = column.shape[0]
    return jnp.sum(jnp.where(diagonal(batch), column, 0.0), axis=0, keepdims=True)


def row_to_column(row):
    return jnp.sum(jnp.where(diagonal(row.shape[1]), row, 0.0), axis=1, keepdims=True)


def head_kernel(
    sizes,
    hidden_hbm,
    gain_hbm,
    w_hbm,
    z_ref,
    lse_col_ref,
    lse_row_ref,
    h_ref,
    gain_ref,
    x_ref,
    w_own,
    w_partner,
    core_out,
    core_in,
    chip_out,
    chip_in,
    sq_out,
    sq_in,
    mass_out,
    mass_in,
    lane_peak,
    lane_mass,
    w_edge,
    edge_out,
    edge_in,
    edge_sem,
    edge_send,
    edge_recv,
    h_sem,
    gain_sem,
    w_own_sem,
    w_partner_sem,
    core_send,
    core_recv,
    chip_send,
    chip_recv,
    sq_send,
    sq_recv,
    mass_send,
    mass_recv,
):
    cols, rows, width, block, tiles, features = sizes
    dp, col, row = lax.axis_index("dp"), lax.axis_index("col"), lax.axis_index("row")
    chip, core = row // 2, row % 2
    batch = h_ref.shape[0]

    def device(flip_col, flip_chip, flip_core):
        c = 1 - col if flip_col else col
        r = (1 - chip if flip_chip else chip) * 2 + (1 - core if flip_core else core)
        return (dp, c, r), c * rows + r

    me = device(0, 0, 0)[1]
    row_peers = [device(0, 1, 1), device(0, 1, 0), device(0, 0, 1)]
    mirror = device(1, 0, 0)
    peers = [device(1, 1, 1), device(1, 1, 0), device(1, 0, 1), mirror, *row_peers]
    partner = row_peers[2][0]

    own_count = tiles - SHIFT + core * 2 * SHIFT
    partner_count = 2 * tiles - own_count

    def w_copy(s, own):
        count = own_count if own else partner_count
        side = core if own else 1 - core
        late = jnp.where(s < count, 0, 1)
        tile = (1 - late) * (side * (tiles - SHIFT) + s) + late * (side * tiles + s - count)
        start = (late * chip + (1 - late) * (1 - chip)) * 2 * block + tile * TILE
        buf, sem = (w_own, w_own_sem) if own else (w_partner, w_partner_sem)
        slot = s % PAIRS
        return pltpu.make_async_copy(
            w_hbm.at[:, pl.ds(pl.multiple_of(start, TILE), TILE)], buf.at[slot], sem.at[slot]
        )

    def core_copy(s, cut=0):
        at = pl.ds(cut, TILE - cut)
        return pltpu.make_async_remote_copy(
            core_out.at[s, :, at], core_in.at[s, :, at], core_send.at[s], core_recv.at[s],
            device_id=partner, device_id_type=MESH,
        )

    def chip_copy(group, s, count, cut=0):
        at = pl.ds(cut, TILE - cut)
        tile = core * (tiles - SHIFT) + s
        place = core * tail if isinstance(group, int) and group == 0 else group
        return pltpu.make_async_remote_copy(
            chip_out.at[pl.ds(s, count), :, at], chip_in.at[pl.ds(tile % tiles, count), :, at],
            chip_send.at[group], chip_recv.at[place],
            device_id=(dp, col, (1 - chip) * 2 + tile // tiles), device_id_type=MESH,
        )

    def chip_arrival(place, first, count, cut=0):
        at = pl.ds(cut, TILE - cut)
        return pltpu.make_async_remote_copy(
            chip_out.at[pl.ds(0, count), :, at], chip_in.at[pl.ds(first, count), :, at],
            chip_send.at[0], chip_recv.at[place],
            device_id=row_peers[1][0], device_id_type=MESH,
        )

    def edge_start(own):
        side = core if own else 1 - core
        start = (1 - chip) * 2 * block + side * (tiles - SHIFT) * TILE
        return pl.ds(pl.multiple_of(start, TILE), EDGE)

    def edge_fetch(k):
        return pltpu.make_async_copy(
            w_hbm.at[:, edge_start(k == 0)], w_edge.at[:, pl.ds(k * EDGE, EDGE)], edge_sem.at[k]
        )

    def edge_copy(k, arrival=None):
        place = arrival if arrival is not None else 2 * core if k == 0 else 3 - 2 * core
        return pltpu.make_async_remote_copy(
            edge_out.at[k], edge_in.at[place], edge_send.at[k], edge_recv.at[place],
            device_id=(dp, col, (1 - chip) * 2), device_id_type=MESH,
        )

    def group_start(group):
        return (group - 2) * GROUP + 3

    last_group = 2 + (tiles - SHIFT - 3) // GROUP
    tail = last_group + 1

    h_copies = []
    for k in range(PARTS):
        rows_k = pl.ds(k * batch // PARTS, batch // PARTS)
        h_copies.append(pltpu.make_async_copy(hidden_hbm.at[rows_k], h_ref.at[rows_k], h_sem.at[k]))
    gain_copy = pltpu.make_async_copy(gain_hbm, gain_ref, gain_sem)
    for copy in h_copies:
        copy.start()
    gain_copy.start()

    barrier = pltpu.get_barrier_semaphore()
    for peer, _ in [mirror, *row_peers]:
        pl.semaphore_signal(barrier, inc=1, device_id=peer, device_id_type=MESH)

    def fetch(first, last):
        @pl.loop(first, last)
        def _(q):
            w_copy(q, False).start()
            w_copy(q, True).start()


    edge_fetch(0).start()
    edge_fetch(1).start()
    fetch(0, 1)

    for copy in h_copies:
        copy.wait()
    squares = jnp.zeros((batch, LANES), jnp.float32)
    for k in range(width // LANES):
        part = h_ref[:, k * LANES:(k + 1) * LANES].astype(jnp.float32)
        squares = squares + part * part
    local_sq = column_to_row(jnp.sum(squares, axis=1, keepdims=True))
    sq_out[...] = local_sq
    sq_in[row] = local_sq
    pl.semaphore_wait(barrier, rows)

    def sq_copy(k, arrival=False):
        peer, _ = row_peers[k]
        slot = peer[2] if arrival else row
        return pltpu.make_async_remote_copy(
            sq_out, sq_in.at[slot], sq_send.at[k], sq_recv.at[slot],
            device_id=peer, device_id_type=MESH,
        )

    for k in range(rows - 1):
        sq_copy(k).start()
    fetch(1, 2)
    gain_copy.wait()
    for k in reversed(range(rows - 1)):
        sq_copy(k, arrival=True).wait_recv()
    total_sq = sq_in[0]
    for k in range(1, rows):
        total_sq = total_sq + sq_in[k]
    scale_row = lax.rsqrt(total_sq / features + EPS)
    scale = row_to_column(scale_row)
    for k in range(width // LANES):
        at = slice(k * LANES, (k + 1) * LANES)
        x_ref[:, at] = (h_ref[:, at].astype(jnp.float32) * scale * gain_ref[at]).astype(jnp.bfloat16)

    def partner_tile(q, cut=0):
        w_copy(q, False).wait()
        core_out[q, :, cut:] = jnp.dot(x_ref[...], w_partner[q % PAIRS, :, cut:], preferred_element_type=jnp.float32)

        @pl.when(q + PAIRS < partner_count + tiles)
        def _():
            w_copy(q + PAIRS, False).start()

        core_copy(q, cut).start()

    def own_tile(q, total, cut=0):
        w_copy(q, True).wait()
        total[...] = jnp.dot(x_ref[...], w_own[q % PAIRS, :, cut:], preferred_element_type=jnp.float32)

        @pl.when(q + PAIRS < own_count + tiles)
        def _():
            w_copy(q + PAIRS, True).start()

        core_copy(q, cut).wait_recv()
        total[...] += core_in[q, :, cut:]

    def columns(i):
        return pl.ds(pl.multiple_of(i * TILE, TILE), TILE)

    def send_tile(s):
        own_tile(s, chip_out.at[s])

    def keep_tile(s):
        own_tile(s, z_ref.at[:, columns(s - own_count)])

    edge_fetch(0).wait()
    edge_fetch(1).wait()
    for k in range(2):
        at = slice(k * EDGE, (k + 1) * EDGE)
        edge_out[k] = jnp.dot(x_ref[...], w_edge[:, at], preferred_element_type=jnp.float32)
    for k in range(2):
        edge_copy(k).start()
    partner_tile(0, EDGE)
    fetch(2, PAIRS)
    partner_tile(1)
    own_tile(0, chip_out.at[0, :, pl.ds(EDGE, TILE - EDGE)], EDGE)
    chip_copy(0, 0, 1, EDGE).start()

    @pl.loop(1, 3)
    def _(s):
        partner_tile(s + 1)
        send_tile(s)

    chip_copy(1, 1, 2).start()

    @pl.loop(2, last_group)
    def _(group):
        @pl.loop(0, GROUP)
        def _(t):
            s = group_start(group) + t
            partner_tile(s + 1)
            send_tile(s)

        chip_copy(group, group_start(group), GROUP).start()

    @pl.loop(tiles - SHIFT, tiles + SHIFT)
    def _(s):
        partner_tile(s + 1)

        @pl.when(core == 1)
        def _():
            send_tile(s)
            chip_copy(last_group + s - tiles + SHIFT, s, 1).start()

        pl.when(core == 0)(lambda: keep_tile(s))

    @pl.loop(tiles + SHIFT, 2 * tiles + SHIFT)
    def _(s):
        pl.when(s + 1 < partner_count + tiles)(lambda: partner_tile(s + 1))
        pl.when(s < own_count + tiles)(lambda: keep_tile(s))

    lane_peak[...] = jnp.full((batch, LANES), -jnp.inf, jnp.float32)
    lane_mass[...] = jnp.zeros((batch, LANES), jnp.float32)

    def finish(place, first, count, edges=None):
        if edges is None:
            chip_arrival(place, first, count).wait_recv()
        else:
            for k in range(2):
                edge_copy(k, arrival=edges + k).wait_recv()
            chip_in[first, :, :EDGE] = edge_in[edges] + edge_in[edges + 1]
            chip_arrival(place, first, count, EDGE).wait_recv()

        @pl.loop(first, first + count)
        def _(i):
            z = z_ref[:, columns(i)] + chip_in[i]
            z_ref[:, columns(i)] = z
            parts = [z[:, k * LANES:(k + 1) * LANES] for k in range(TILE // LANES)]
            peak = lane_peak[...]
            new_peak = functools.reduce(jnp.maximum, parts, peak)
            mass = lane_mass[...] * jnp.exp(peak - new_peak)
            for part in parts:
                mass = mass + jnp.exp(part - new_peak)
            lane_peak[...] = new_peak
            lane_mass[...] = mass

    @pl.when(core == 0)
    def _():
        finish(0, 0, 1, edges=0)
        finish(tail, tiles - 1, 1, edges=2)

    finish(1, 1 - core, 2)

    @pl.loop(2, last_group)
    def _(group):
        finish(group, group_start(group) - core, GROUP)

    @pl.when(core == 1)
    def _():
        for k in range(2 * SHIFT):
            finish(last_group + k, tiles - 2 * SHIFT + k, 1)

    peaks_by_lane, mass_by_lane = lane_peak[...].T, lane_mass[...].T
    peak = jnp.max(peaks_by_lane, axis=0, keepdims=True)
    mass = jnp.sum(mass_by_lane * jnp.exp(peaks_by_lane - peak), axis=0, keepdims=True)
    first = lax.broadcasted_iota(jnp.int32, (2, batch), 0) == 0
    message = jnp.where(first, peak, mass)
    mass_out[...] = message
    mass_in[me] = message

    def mass_copy(k, arrival=False):
        peer, place = peers[k]
        slot = place if arrival else me
        return pltpu.make_async_remote_copy(
            mass_out, mass_in.at[slot], mass_send.at[k], mass_recv.at[slot],
            device_id=peer, device_id_type=MESH,
        )

    everyone = cols * rows
    for k in range(everyone - 1):
        mass_copy(k).start()

    for k in range(rows - 1):
        sq_copy(k).wait_send()

    core_copy(0, EDGE).wait_send()

    @pl.loop(1, partner_count + tiles)
    def _(s):
        core_copy(s).wait_send()

    for k in range(2):
        edge_copy(k).wait_send()
    chip_copy(0, 0, 1, EDGE).wait_send()
    chip_copy(1, 1, 2).wait_send()

    @pl.loop(2, last_group)
    def _(group):
        chip_copy(group, group_start(group), GROUP).wait_send()

    @pl.when(core == 1)
    def _():
        for k in range(2 * SHIFT):
            chip_copy(last_group + k, tiles - SHIFT + k, 1).wait_send()

    for k in reversed(range(everyone - 1)):
        mass_copy(k, arrival=True).wait_recv()
    peaks = [mass_in[d, 0:1] for d in range(everyone)]
    top = functools.reduce(jnp.maximum, peaks)
    total = jnp.zeros_like(top)
    for d in range(everyone):
        total = total + mass_in[d, 1:2] * jnp.exp(peaks[d] - top)
    log_norm = top + jnp.log(total)
    lse_row_ref[...] = log_norm
    lse_col_ref[...] = jnp.broadcast_to(row_to_column(log_norm), (batch, LANES))

    for k in range(everyone - 1):
        mass_copy(k).wait_send()


def subtract_kernel(z_ref, lse_col_ref, lse_row_ref, out_hbm, log_norm_hbm, out_ref, log_norm_ref, sem, log_norm_sem):
    batch, block = z_ref.shape
    log_norm_ref[...] = lse_row_ref[0]
    copies = [pltpu.make_async_copy(log_norm_ref, log_norm_hbm, log_norm_sem)]
    copies[0].start()
    for n in range(batch // SUBLANES):
        at = slice(n * SUBLANES, (n + 1) * SUBLANES)
        lse = lse_col_ref[at]
        for k in range(0, block, LANES):
            out_ref[at, k:k + LANES] = z_ref[at, k:k + LANES] - lse
        rows = pl.ds(n * SUBLANES, SUBLANES)
        copies.append(pltpu.make_async_copy(out_ref.at[rows], out_hbm.at[rows], sem.at[n]))
        copies[-1].start()
    for copy in copies:
        copy.wait()


def solution(mesh):
    cols, rows = mesh.shape["col"], mesh.shape["row"]

    def local_head(hidden, norm_gain, w_head):
        batch, width = hidden.shape
        block = w_head.shape[1] // rows
        tiles = block // TILE
        sizes = (cols, rows, width, block, tiles, width * rows)
        f32 = jnp.float32
        dma = pltpu.SemaphoreType.DMA
        vmem = pl.BlockSpec(memory_space=pltpu.VMEM)
        hbm = pl.BlockSpec(memory_space=pl.ANY)
        z, lse_col, lse_row = pl.pallas_call(
            functools.partial(head_kernel, sizes),
            name="head",
            out_shape=(
                pltpu.VMEM((batch, block), f32),
                pltpu.VMEM((batch, LANES), f32),
                pltpu.VMEM((1, batch), f32),
            ),
            in_specs=[pl.BlockSpec(memory_space=pltpu.HBM)] * 3,
            out_specs=[vmem] * 3,
            scratch_shapes=[
                pltpu.VMEM((batch, width), jnp.bfloat16),
                pltpu.VMEM((width,), f32),
                pltpu.VMEM((batch, width), jnp.bfloat16),
                pltpu.VMEM((PAIRS, width, TILE), jnp.bfloat16),
                pltpu.VMEM((PAIRS, width, TILE), jnp.bfloat16),
                pltpu.VMEM((2 * tiles + SHIFT, batch, TILE), f32),
                pltpu.VMEM((2 * tiles + SHIFT, batch, TILE), f32),
                pltpu.VMEM((tiles + SHIFT, batch, TILE), f32),
                pltpu.VMEM((tiles, batch, TILE), f32),
                pltpu.VMEM((1, batch), f32),
                pltpu.VMEM((rows, 1, batch), f32),
                pltpu.VMEM((2, batch), f32),
                pltpu.VMEM((cols * rows, 2, batch), f32),
                pltpu.VMEM((batch, LANES), f32),
                pltpu.VMEM((batch, LANES), f32),
                pltpu.VMEM((width, 2 * EDGE), jnp.bfloat16),
                pltpu.VMEM((2, batch, EDGE), f32),
                pltpu.VMEM((4, batch, EDGE), f32),
                dma((2,)),
                dma((2,)),
                dma((4,)),
                dma((PARTS,)),
                dma,
                dma((PAIRS,)),
                dma((PAIRS,)),
                dma((2 * tiles + SHIFT,)),
                dma((2 * tiles + SHIFT,)),
                dma((tiles + SHIFT,)),
                dma((tiles,)),
                dma((rows,)),
                dma((rows,)),
                dma((cols * rows,)),
                dma((cols * rows,)),
            ],
            compiler_params=pltpu.CompilerParams(
                collective_id=0, has_side_effects=True, vmem_limit_bytes=VMEM_LIMIT
            ),
        )(*(pltpu.with_memory_space_constraint(a, pltpu.HBM) for a in (hidden, norm_gain, w_head)))
        return pl.pallas_call(
            subtract_kernel,
            name="subtract",
            out_shape=(
                jax.ShapeDtypeStruct((batch, block), f32),
                jax.ShapeDtypeStruct((batch,), f32),
            ),
            in_specs=[vmem] * 3,
            out_specs=[hbm] * 2,
            scratch_shapes=[pltpu.VMEM((batch, block), f32), pltpu.VMEM((batch,), f32), dma((batch // SUBLANES,)), dma],
            compiler_params=pltpu.CompilerParams(vmem_limit_bytes=16 * 1024 * 1024),
        )(z, lse_col, lse_row)

    return jax.shard_map(
        local_head,
        mesh=mesh,
        in_specs=(P("dp", "row"), P("row"), P("row", "col")),
        out_specs=(P("dp", ("col", "row")), P("dp")),
        check_vma=False,
    )
```
